32 devices in a mesh: seq: 8 (over z, y), tp: 4 (over x, core).
Axes of the slice: x: 2, y: 2, z: 4, core: 2. Of those that a mesh axis runs over, the one named last changes fastest.
Arguments:
- tokens: bfloat16 [8192, 1024], P(('seq', 'tp')), may hold values from -6 to 6
- fine_gain: float32 [1024], replicated, may hold values from 0.1 to 1.9
- fine_query: bfloat16 [1024, 1024], replicated, may hold values from -2.0625 to 2.0625
- fine_keyval: bfloat16 [1024, 2048], replicated, may hold values from -0.125 to 0.125
- fine_out: bfloat16 [1024, 1024], replicated, may hold values from -0.1875 to 0.1875
- down_weight: bfloat16 [1024, 4096], P(None, 'tp'), may hold values from -0.1875 to 0.1875
- coarse_gain: float32 [4096], replicated, may hold values from 0.1 to 1.9
- coarse_query: bfloat16 [4096, 4096], P('seq', 'tp'), may hold values from -1.03125 to 1.03125
- coarse_keyval: bfloat16 [4096, 2, 4096], P('seq', None, 'tp'), may hold values from -0.0625 to 0.0625
- coarse_out: bfloat16 [4096, 4096], P('tp'), may hold values from -0.09375 to 0.09375
- up_weight: bfloat16 [4096, 1024], P('tp'), may hold values from -0.09375 to 0.09375
Outputs:
- result: bfloat16 [8192, 1024], P(('seq', 'tp'))
The draws below stay inside these ranges and needn't reach their ends.
All inputs are finite; a program needn't handle non-finite values.
Results may differ from the reference program's by a relative error of at most 0.02.
Values may be sent and summed in bfloat16 or wider, within the bound.
A program may use at most 192 MiB of HBM per device.

```python
import math
import jax
import jax.numpy as jnp
from jax import lax

D_FINE = 1024
D_COARSE = 4096
HEAD = 128
WINDOW = 256
SHORT = 8
TOKENS = 8192


def paired_weights(key, marker, rows, cols, spread):
    base = jax.random.fold_in(key, marker)
    first, second, third = jax.random.split(base, 3)
    root = jnp.sqrt(jnp.float32(rows))
    key_part = jax.random.truncated_normal(first, -4.0, 4.0, (rows, cols), jnp.float32) / root
    value_part = jax.random.truncated_normal(second, -4.0, 4.0, (rows, cols), jnp.float32) / root
    query_part = jax.random.truncated_normal(third, -4.0, 4.0, (rows, cols), jnp.float32) / root
    query_part = spread * query_part
    return (query_part, key_part, value_part)


def draw_fine_query(key, part):
    return paired_weights(key, 11, D_FINE, D_FINE, 1.0)[0].astype(jnp.bfloat16)


def draw_fine_keyval(key, part):
    drawn = paired_weights(key, 11, D_FINE, D_FINE, 1.0)
    return jnp.concatenate([drawn[1], drawn[2]], 1).astype(jnp.bfloat16)


def draw_coarse_query(key, part):
    return paired_weights(key, 23, D_COARSE, D_COARSE, 3.0)[0].astype(jnp.bfloat16)


def draw_coarse_keyval(key, part):
    drawn = paired_weights(key, 23, D_COARSE, D_COARSE, 3.0)
    return jnp.stack([drawn[1], drawn[2]], 1).astype(jnp.bfloat16)


def level_of(key, extent, cuts, smallest, high):
    gain, own = 1.0, jax.random.fold_in(key, 6)
    for dim, parts in cuts:
        draws = jnp.exp(jax.random.uniform(jax.random.fold_in(own, dim), (parts,), jnp.float32, smallest / len(cuts), high / len(cuts)))
        gain = gain * jnp.repeat(draws, extent[dim] // parts).reshape([-1 if axis == dim else 1 for axis in range(len(extent))])
    return gain


def noise(rng, dims, deviation, bound, cuts=(), kind=jnp.bfloat16):
    factor_of = level_of(rng, dims, cuts, -0.22, 0.18) if cuts else 1.0
    values = jax.random.normal(rng, dims, jnp.float32) * deviation * factor_of
    return jnp.minimum(jnp.maximum(values, -bound), bound).astype(kind)


def setup_inputs(seed: int = 0) -> dict:
    key_list = jax.random.split(jax.random.key(seed), 12)
    tokens = noise(key_list[0], (TOKENS, D_FINE), 1.0, 6.0, ((0, 32),))
    fine_gain = jnp.clip(1.0 + 0.18 * jax.random.normal(key_list[1], (D_FINE,), jnp.float32), 0.1, 1.9)
    fine_query = draw_fine_query(jax.random.fold_in(key_list[11], 71), 0)
    fine_keyval = draw_fine_keyval(jax.random.fold_in(key_list[11], 71), 0)
    fine_out = noise(key_list[4], (D_FINE, D_FINE), D_FINE ** -0.5, 0.1875)
    down_weight = noise(key_list[5], (D_FINE, D_COARSE), D_FINE ** -0.5, 0.1875, ((1, 4),))
    coarse_gain = jnp.clip(1.0 + 0.18 * jax.random.normal(key_list[6], (D_COARSE,), jnp.float32), 0.1, 1.9)
    coarse_query = draw_coarse_query(jax.random.fold_in(key_list[11], 71), 0)
    coarse_keyval = draw_coarse_keyval(jax.random.fold_in(key_list[11], 71), 0)
    coarse_out = noise(key_list[9], (D_COARSE, D_COARSE), D_COARSE ** -0.5, 0.09375, ((0, 4),))
    up_weight = noise(key_list[10], (D_COARSE, D_FINE), D_COARSE ** -0.5, 0.09375, ((0, 4),))
    return dict(tokens=tokens, fine_gain=fine_gain, fine_query=fine_query, fine_keyval=fine_keyval, fine_out=fine_out, down_weight=down_weight, coarse_gain=coarse_gain, coarse_query=coarse_query, coarse_keyval=coarse_keyval, coarse_out=coarse_out, up_weight=up_weight)


epsilon = 1e-06
big_negative = -1e+30

def normalize(values, scale_gain):
    mean_square = lax.optimization_barrier(jnp.mean(values * values, axis=-1, keepdims=True))
    return values * lax.rsqrt(mean_square + epsilon) * scale_gain

def fine_attention(queries, keyvals):
    total_rows = queries.shape[0]
    heads = D_FINE // HEAD
    scale = 1.0 / math.sqrt(HEAD)
    query_heads = queries.reshape(total_rows, heads, HEAD)
    padded = jnp.concatenate([jnp.zeros((WINDOW, 2 * D_FINE), jnp.bfloat16), keyvals], 0)

    def block_step(block):
        first = block * WINDOW
        query_block = lax.dynamic_slice_in_dim(query_heads, first, WINDOW, 0)
        key_block = lax.dynamic_slice_in_dim(padded, first, 2 * WINDOW, 0)
        key_heads = key_block[:, :D_FINE].reshape(2 * WINDOW, heads, HEAD)
        value_heads = key_block[:, D_FINE:].reshape(2 * WINDOW, heads, HEAD)
        scores = jnp.einsum('qhd,khd->hqk', query_block.astype(jnp.float32), key_heads.astype(jnp.float32)) * scale
        row_index = jnp.arange(WINDOW, dtype=jnp.int32)[:, None]
        col_index = jnp.arange(2 * WINDOW, dtype=jnp.int32)[None, :]
        offset = row_index + WINDOW - col_index
        allowed = (offset >= 0) & (offset < WINDOW) & (first - WINDOW + col_index >= 0)
        scores = jnp.where(allowed[None], scores, big_negative)
        peak = lax.optimization_barrier(jnp.max(scores, axis=-1, keepdims=True))
        terms = jnp.where(allowed[None], jnp.exp(scores - peak), 0.0)
        denom = lax.optimization_barrier(jnp.sum(terms, axis=-1))
        weights = terms.astype(jnp.bfloat16).astype(jnp.float32)
        mixed = jnp.einsum('hqk,khd->hqd', weights, value_heads.astype(jnp.float32)) / denom[..., None]
        return jnp.transpose(mixed, (1, 0, 2)).reshape(WINDOW, D_FINE).astype(jnp.bfloat16)
    blocks = lax.map(block_step, jnp.arange(total_rows // WINDOW, dtype=jnp.int32))
    return blocks.reshape(total_rows, D_FINE)

def coarse_attention(queries, keyvals):
    count = queries.shape[0]
    heads = D_COARSE // HEAD
    scale = 1.0 / math.sqrt(HEAD)
    block = 1024 if count % 1024 == 0 else count

    def head_step(head):
        query_head = lax.dynamic_slice_in_dim(queries, head * HEAD, HEAD, 1).astype(jnp.float32)
        key_head = lax.dynamic_slice_in_dim(keyvals, head * HEAD, HEAD, 1).astype(jnp.float32)
        value_head = lax.dynamic_slice_in_dim(keyvals, D_COARSE + head * HEAD, HEAD, 1).astype(jnp.float32)

        def query_step(index):
            first = index * block
            query_block = lax.dynamic_slice_in_dim(query_head, first, block, 0)
            scores = jnp.dot(query_block, key_head.T) * scale
            row_index = first + jnp.arange(block, dtype=jnp.int32)[:, None]
            col_index = jnp.arange(count, dtype=jnp.int32)[None, :]
            allowed = col_index <= row_index
            scores = jnp.where(allowed, scores, big_negative)
            peak = lax.optimization_barrier(jnp.max(scores, axis=-1, keepdims=True))
            terms = jnp.where(allowed, jnp.exp(scores - peak), 0.0)
            denom = lax.optimization_barrier(jnp.sum(terms, axis=-1, keepdims=True))
            weights = terms.astype(jnp.bfloat16).astype(jnp.float32)
            return (jnp.dot(weights, value_head) / denom).astype(jnp.bfloat16)
        outputs = lax.map(query_step, jnp.arange(count // block, dtype=jnp.int32))
        return outputs.reshape(count, HEAD)
    per_head = lax.map(head_step, jnp.arange(heads, dtype=jnp.int32))
    return jnp.transpose(per_head, (1, 0, 2)).reshape(count, D_COARSE)

def reference(tokens, fine_gain, fine_query, fine_keyval, fine_out, down_weight, coarse_gain, coarse_query, coarse_keyval, coarse_out, up_weight):
    inputs = tokens.astype(jnp.float32)
    normed = normalize(inputs, fine_gain).astype(jnp.bfloat16)
    queries = jnp.dot(normed, fine_query, preferred_element_type=jnp.float32).astype(jnp.bfloat16)
    keyvals = jnp.dot(normed, fine_keyval, preferred_element_type=jnp.float32).astype(jnp.bfloat16)
    local = fine_attention(queries, keyvals)
    fine_state = (inputs + jnp.dot(local, fine_out, preferred_element_type=jnp.float32)).astype(jnp.bfloat16)
    count = fine_state.shape[0] // SHORT
    pooled = lax.optimization_barrier(jnp.mean(fine_state.astype(jnp.float32).reshape(count, SHORT, D_FINE), axis=1)).astype(jnp.bfloat16)
    shortened = jnp.dot(pooled, down_weight, preferred_element_type=jnp.float32).astype(jnp.bfloat16)
    coarse_normed = normalize(shortened.astype(jnp.float32), coarse_gain).astype(jnp.bfloat16)
    coarse_queries = jnp.dot(coarse_normed, coarse_query, preferred_element_type=jnp.float32).astype(jnp.bfloat16)
    coarse_kv = jnp.dot(coarse_normed, coarse_keyval.reshape(D_COARSE, 2 * D_COARSE), preferred_element_type=jnp.float32).astype(jnp.bfloat16)
    coarse_heads = coarse_attention(coarse_queries, coarse_kv)
    coarse_state = (shortened.astype(jnp.float32) + jnp.dot(coarse_heads, coarse_out, preferred_element_type=jnp.float32)).astype(jnp.bfloat16)
    delayed = jnp.concatenate([jnp.zeros((1, D_COARSE), jnp.bfloat16), coarse_state[:-1]], 0)
    lifted = jnp.dot(delayed, up_weight, preferred_element_type=jnp.float32)
    result = fine_state.astype(jnp.float32) + jnp.repeat(lifted, SHORT, axis=0)
    return result.astype(jnp.bfloat16)
```

```python
import functools
import math

import jax
import jax.numpy as jnp
from jax import lax
from jax.experimental import pallas as pl
from jax.experimental.pallas import tpu as pltpu
from jax.sharding import PartitionSpec as P

HEAD = 128
WINDOW = 256
SHORT = 8


epsilon = 1e-06
big_negative = -1e30


def from_behind(array, axis, by):
    size = lax.axis_size(axis)
    pairs = [(i, i + by) for i in range(size) if 0 <= i + by < size]
    return lax.ppermute(array, axis, pairs)


def normalize(values, scale_gain):
    mean_square = jnp.mean(values * values, axis=-1, keepdims=True)
    return values * lax.rsqrt(mean_square + epsilon) * scale_gain


def online_update(state, query_heads, key_piece, value_piece, query_index):
    running_max, running_sum, accumulate = state
    scale = 1.0 / math.sqrt(HEAD)
    scores = (
        jnp.einsum("qhd,khd->hqk", query_heads, key_piece, preferred_element_type=jnp.float32)
        * scale
    )
    key_index = jnp.arange(key_piece.shape[0], dtype=jnp.int32)
    allowed = key_index[None, :] <= query_index[:, None]
    scores = jnp.where(allowed[None], scores, big_negative)
    new_max = jnp.maximum(running_max, jnp.max(scores, axis=-1))
    terms = jnp.where(allowed[None], jnp.exp(scores - new_max[..., None]), 0.0)
    new_sum = jnp.sum(terms, axis=-1)
    product = jnp.einsum(
        "hqk,khd->hqd", terms.astype(jnp.bfloat16), value_piece, preferred_element_type=jnp.float32
    )
    return (new_max, new_sum, product)


def body(
    tokens,
    fine_gain,
    fine_query,
    fine_keyval,
    fine_out,
    down_weight,
    coarse_gain,
    coarse_query,
    coarse_keyval,
    coarse_out,
    up_weight,
):
    tok_rows = tokens.shape[0]
    width = tokens.shape[1]
    fine_heads = width // HEAD
    scale = 1.0 / math.sqrt(HEAD)
    start_row = lax.axis_index(("seq", "tp")) * tok_rows
    inputs = tokens.astype(jnp.float32)
    normed = normalize(inputs, fine_gain).astype(jnp.bfloat16)
    queries = jnp.dot(normed, fine_query, preferred_element_type=jnp.float32).astype(jnp.bfloat16)
    keyvals = jnp.dot(normed, fine_keyval, preferred_element_type=jnp.float32).astype(jnp.bfloat16)
    earlier = from_behind(keyvals, ("seq", "tp"), 1)
    key_rows = jnp.concatenate([earlier, keyvals], 0)
    span = key_rows.shape[0]
    key_heads = key_rows[:, :width].reshape(span, fine_heads, HEAD)
    value_heads = key_rows[:, width:].reshape(span, fine_heads, HEAD)
    query_heads = queries.reshape(tok_rows, fine_heads, HEAD)
    scores = (
        jnp.einsum("qhd,khd->hqk", query_heads, key_heads, preferred_element_type=jnp.float32)
        * scale
    )
    row_index = jnp.arange(tok_rows, dtype=jnp.int32)[:, None]
    col_index = jnp.arange(span, dtype=jnp.int32)[None, :]
    offset = row_index + WINDOW - col_index
    allowed = (offset >= 0) & (offset < WINDOW) & (start_row - WINDOW + col_index >= 0)
    scores = jnp.where(allowed[None], scores, big_negative)
    peak = jnp.max(scores, axis=-1, keepdims=True)
    terms = jnp.where(allowed[None], jnp.exp(scores - peak), 0.0)
    denom = jnp.sum(terms, axis=-1)
    mixed = jnp.einsum(
        "hqk,khd->qhd", terms.astype(jnp.bfloat16), value_heads, preferred_element_type=jnp.float32
    )
    local = (mixed / jnp.transpose(denom)[..., None]).reshape(tok_rows, width).astype(jnp.bfloat16)
    fine_state = (inputs + jnp.dot(local, fine_out, preferred_element_type=jnp.float32)).astype(
        jnp.bfloat16
    )
    pooled = jnp.mean(
        fine_state.astype(jnp.float32).reshape(tok_rows // SHORT, SHORT, width), axis=1
    ).astype(jnp.bfloat16)
    pooled_all = lax.all_gather(pooled, "tp", axis=0, tiled=True)
    short_cols = jnp.dot(pooled_all, down_weight, preferred_element_type=jnp.float32).astype(
        jnp.bfloat16
    )
    shortened = lax.all_gather(short_cols, "tp", axis=1, tiled=True)
    coarse_normed = normalize(shortened.astype(jnp.float32), coarse_gain).astype(jnp.bfloat16)
    coarse_rows = coarse_normed.shape[0]
    local_cols = coarse_query.shape[1]
    local_heads = local_cols // HEAD
    query_rows = lax.all_gather(coarse_query, "seq", axis=0, tiled=True)
    keyval_rows = lax.all_gather(coarse_keyval, "seq", axis=0, tiled=True)
    count = query_rows.shape[0]
    query_sum = jnp.dot(coarse_normed, query_rows, preferred_element_type=jnp.float32)
    keyval_sum = jnp.dot(
        coarse_normed,
        keyval_rows.reshape(count, 2 * local_cols),
        preferred_element_type=jnp.float32,
    )
    coarse_queries = query_sum.astype(jnp.bfloat16).reshape(coarse_rows, local_heads, HEAD)
    coarse_kv = keyval_sum.astype(jnp.bfloat16).reshape(coarse_rows, 2, local_cols)
    my_first = lax.axis_index("seq") * coarse_rows
    query_index = my_first + jnp.arange(coarse_rows, dtype=jnp.int32)
    initial = (
        jnp.full((local_heads, coarse_rows), big_negative, jnp.float32),
        jnp.zeros((local_heads, coarse_rows), jnp.float32),
        jnp.zeros((local_heads, coarse_rows, HEAD), jnp.float32),
    )
    piece = lax.all_gather(coarse_kv, "seq", axis=0, tiled=True)
    count = piece.shape[0]
    key_piece = piece[:, 0].reshape(count, local_heads, HEAD)
    value_piece = piece[:, 1].reshape(count, local_heads, HEAD)
    final = lax.cond(
        jnp.int32(0) < my_first + coarse_rows,
        lambda: online_update(initial, coarse_queries, key_piece, value_piece, query_index),
        lambda: initial,
    )
    head_out = final[2] / final[1][..., None]
    coarse_heads = (
        jnp.transpose(head_out, (1, 0, 2)).reshape(coarse_rows, local_cols).astype(jnp.bfloat16)
    )
    partials = jnp.dot(coarse_heads, coarse_out, preferred_element_type=jnp.float32)
    attended = lax.psum_scatter(
        partials.astype(jnp.bfloat16), "tp", scatter_dimension=1, tiled=True
    ).astype(jnp.float32)
    coarse_state = (short_cols.astype(jnp.float32) + attended).astype(jnp.bfloat16)
    prior_row = from_behind(coarse_state[coarse_rows - 1 :], "seq", 1)
    delayed = jnp.concatenate([prior_row, coarse_state[: coarse_rows - 1]], 0)
    lifted = lax.psum_scatter(
        jnp.dot(delayed, up_weight, preferred_element_type=jnp.float32).astype(jnp.bfloat16),
        "tp",
        scatter_dimension=0,
        tiled=True,
    ).astype(jnp.float32)
    result = fine_state.astype(jnp.float32) + jnp.repeat(lifted, SHORT, axis=0)
    return result.astype(jnp.bfloat16)


def flip(index, bit):
    return index + bit - 2 * bit * lax.rem(lax.div(index, jnp.int32(bit)), jnp.int32(2))


def bits_of(size):
    out, bit = [], size // 2
    while bit:
        out.append(bit)
        bit //= 2
    return out


def dot32(left, right):
    return jnp.dot(left, right, preferred_element_type=jnp.float32)


def dot_t(left, right):
    return lax.dot_general(
        left, right, (((1,), (1,)), ((), ())), preferred_element_type=jnp.float32
    )


def section_kernel(
    seq, tp,
    tokens, fine_gain, fine_query, fine_keyval, fine_out, down_weight, coarse_gain, coarse_query,
    coarse_kv, coarse_out, up_weight,
    result,
    both, wq, wkv, wo, down_own, down_g, wqk, wv, wout, wup,
    normed, queries, key_rows, local, fine_state, pooled_all, mqk, mv, pv_out, pv_in, mixed_qk,
    mixed_v, qkv, factors, terms, denoms, shifted, heads_out, heads_in, coarse_heads, short_cols,
    ss_tp, ss_seq, send1, recv1, state, send2, recv2,
    load_sem, halo_s, halo_r, qk_s, qk_r, v_s, v_r, d_s, d_r, pa_s, pa_r, pb_s, pb_r, pc_s, pc_r,
    ssa_s, ssa_r, ssb_s, ssb_r, pv_s, pv_r, h_s, h_r, r1_s, r1_r, r2_s, r2_r,
):
    me_s = lax.axis_index("seq")
    me_t = lax.axis_index("tp")
    rows, width = tokens.shape
    scale = 1.0 / math.sqrt(HEAD)
    total = seq * tp
    lin = me_s * tp + me_t
    after = lax.rem(lin + 1, total)
    before = lax.rem(lin + total - 1, total)
    bf, f32 = jnp.bfloat16, jnp.float32

    def around(index, step, size):
        return lax.rem(index + step, size)

    def toggle(index, mask):
        bit = 1
        while bit <= mask:
            if mask & bit:
                index = flip(index, bit)
            bit *= 2
        return index

    def remote(src, dst, send, recv, device):
        copy = pltpu.make_async_remote_copy(
            src_ref=src, dst_ref=dst, send_sem=send, recv_sem=recv,
            device_id=device, device_id_type=pl.DeviceIdType.MESH,
        )
        copy.start()
        return copy

    def load(src, dst, sem):
        copy = pltpu.make_async_copy(src, dst, sem)
        copy.start()
        return copy

    def arrived(dst, sem):
        pltpu.make_async_copy(dst, dst, sem).wait()

    def linear(index):
        return {"seq": lax.div(index, tp), "tp": lax.rem(index, tp)}

    depth = coarse_query.shape[0]
    own = coarse_query.shape[1] // seq
    fcols = down_own.shape[1]
    per = fcols // depth
    half = seq // 2
    zh = lax.div(me_s, half)
    in_half = lax.rem(me_s, half)
    partner = flip(me_s, half)
    pool_rows = rows // SHORT
    crows = pool_rows * tp
    count = crows * seq
    tile = 2 * HEAD

    def head_cols(dest):
        return pl.ds(pl.multiple_of(dest * own, own), own)

    barrier = pltpu.get_barrier_semaphore()
    peers = [{"seq": around(me_s, d, seq)} for d in range(1, seq)]
    peers += [{"tp": around(me_t, d, tp)} for d in range(1, tp)]
    peers += [linear(after), linear(before)]
    in_tokens = load(tokens, both.at[pl.ds(rows, rows)], load_sem.at[0])
    in_down = load(down_weight, down_own, load_sem.at[4])
    in_wq = load(fine_query, wq, load_sem.at[2])
    in_wkv = load(fine_keyval, wkv, load_sem.at[1])
    in_wo = load(fine_out, wo, load_sem.at[3])
    for pl_part, source in ((0, coarse_query), (1, coarse_kv.at[0])):
        load(source.at[:, head_cols(me_s)], wqk.at[me_s, :, pl.ds(pl_part * own, own)],
             qk_r.at[me_s])
    for k, head in enumerate((partner, me_s)):
        load(coarse_kv.at[1, :, head_cols(head)], wv.at[in_half, :, pl.ds(k * own, own)],
             v_r.at[in_half])
    in_wout = load(coarse_out, wout, load_sem.at[5])
    in_wup = load(up_weight, wup, load_sem.at[6])
    for peer in peers:
        pl.semaphore_signal(barrier, inc=1, device_id=peer, device_id_type=pl.DeviceIdType.MESH)
    pl.semaphore_wait(barrier, len(peers))

    sent = []
    halo = remote(tokens, both.at[pl.ds(0, rows)], halo_s, halo_r, linear(after))

    def send_qk(offsets):
        for d in offsets:
            dest = toggle(me_s, d)
            for k, source in enumerate((coarse_query, coarse_kv.at[0])):
                sent.append(
                    remote(
                        source.at[:, head_cols(dest)], wqk.at[me_s, :, pl.ds(k * own, own)],
                        qk_s.at[2 * (d - 1) + k], qk_r.at[me_s], {"seq": dest},
                    )
                )

    def send_v():
        for d in range(1, half):
            dest = toggle(me_s, d)
            for k, head in enumerate((flip(dest, half), dest)):
                sent.append(
                    remote(
                        coarse_kv.at[1, :, head_cols(head)],
                        wv.at[in_half, :, pl.ds(k * own, own)],
                        v_s.at[2 * (d - 1) + k], v_r.at[in_half], {"seq": dest},
                    )
                )

    tp_bits = bits_of(tp)
    send_qk(range(half, seq))

    in_down.wait()
    cgain = coarse_gain[:, pl.ds(pl.multiple_of(me_t * fcols, fcols), fcols)]
    for j in range(per):
        cols = slice(j * depth, (j + 1) * depth)
        down_g[me_t * per + j] = (down_own[:, cols].astype(f32) * cgain[:, cols]).astype(bf)

    def send_down(slot, bit, number):
        copies = []
        for j in range(per):
            block = down_g.at[slot * per + j]
            at = number * per + j
            copies.append(remote(block, block, d_s.at[at], d_r.at[at], {"tp": flip(me_t, bit)}))
        return copies

    down_copies = {bit: send_down(me_t, bit, bit - 1) for bit in tp_bits}
    send_v()
    send_qk(range(1, half))

    gain = fine_gain[...]

    def norm_rows(first):
        values = both[pl.ds(first, rows), :].astype(f32)
        normed[pl.ds(first, rows), :] = normalize(values, gain).astype(bf)

    in_tokens.wait()
    norm_rows(rows)
    in_wq.wait()

    @pl.loop(0, width // tile)
    def _(i):
        cols = pl.ds(pl.multiple_of(i * tile, tile), tile)
        queries[:, cols] = dot32(normed[rows:, :], wq[:, cols]).astype(bf)

    in_wkv.wait()

    def project_rows(first):
        @pl.loop(0, 2 * width // tile)
        def _(i):
            cols = pl.ds(pl.multiple_of(i * tile, tile), tile)
            key_rows[pl.ds(first, rows), cols] = dot32(
                normed[pl.ds(first, rows), :], wkv[:, cols]
            ).astype(bf)

    project_rows(rows)
    halo.wait()
    norm_rows(0)
    project_rows(0)

    row_index = lax.broadcasted_iota(jnp.int32, (rows, 2 * rows), 0)
    col_index = lax.broadcasted_iota(jnp.int32, (rows, 2 * rows), 1)
    offset = row_index + rows - col_index
    allowed = (offset >= 0) & (offset < WINDOW) & (lin * rows - rows + col_index >= 0)

    def weigh(query, key, mask):
        scores = jnp.where(mask, dot_t(query, key) * scale, big_negative)
        peak = jnp.max(scores, axis=-1, keepdims=True)
        weights = jnp.where(mask, jnp.exp(scores - peak), 0.0)
        return weights.astype(bf), jnp.sum(weights, axis=-1, keepdims=True)

    @pl.loop(0, width // HEAD)
    def _(h):
        cols = pl.ds(pl.multiple_of(h * HEAD, HEAD), HEAD)
        vcols = pl.ds(pl.multiple_of(width + h * HEAD, HEAD), HEAD)
        weights, denom = weigh(queries[:, cols], key_rows[:, cols], allowed)
        local[:, cols] = (dot32(weights, key_rows[:, vcols]) / denom).astype(bf)

    in_wo.wait()

    @pl.loop(0, width // tile)
    def _(i):
        cols = pl.ds(pl.multiple_of(i * tile, tile), tile)
        value = both[rows:, cols].astype(f32) + dot32(local[...], wo[:, cols])
        value = value.astype(bf)
        fine_state[:, cols] = value
        mean = jnp.mean(value.astype(f32).reshape(pool_rows, SHORT, tile), axis=1)
        pooled_all[lin, :, cols] = mean.astype(bf)

    group = []
    for d in range(1, tp):
        slot = pooled_all.at[lin]
        group.append(remote(slot, slot, pa_s.at[d - 1], pa_r.at[d - 1], {"tp": toggle(me_t, d)}))
    for copy in group:
        copy.wait_recv()
    sent.extend(group)

    core_bit = tp_bits[-1]
    share = tp // 2
    mine_first = lax.rem(me_t, 2) * share

    def blocks(first_s, offset_t):
        return pooled_all.at[pl.ds(first_s * tp + offset_t, share)]

    held = [me_s]
    number = 0
    pending = []

    def exchange(bit):
        nonlocal number, held
        copies = []
        for index in held:
            part = blocks(index, mine_first)
            copies.append(
                remote(part, part, pb_s.at[number], pb_r.at[number], {"seq": flip(me_s, bit)})
            )
            number += 1
        held = held + [flip(index, bit) for index in held]
        return copies

    seq_bits = bits_of(seq)
    pending = exchange(seq_bits[0])

    mine = pooled_all[pl.ds(me_s * tp, tp)].reshape(crows, width)
    square_sum = jnp.zeros((8, crows), f32)
    for u in range(2):
        cols = slice(u * fcols // 2, (u + 1) * fcols // 2)
        wide = dot32(mine, down_own[:, cols]).astype(bf).astype(f32)
        short_cols[pl.ds(0, crows), cols] = wide
        square_sum += lax.dot_general(
            jnp.ones((8, fcols // 2), f32), wide * wide, (((1,), (1,)), ((), ())),
            preferred_element_type=f32, precision=lax.Precision.HIGHEST,
        )
    ss_tp[me_t] = square_sum
    group = []
    for d in range(1, tp):
        slot = ss_tp.at[me_t]
        group.append(remote(slot, slot, ssa_s.at[d - 1], ssa_r.at[d - 1], {"tp": toggle(me_t, d)}))
    for copy in group:
        copy.wait_recv()
    sent.extend(group)
    whole_sum = ss_tp[0]
    for t in range(1, tp):
        whole_sum += ss_tp[t]
    ss_seq[me_s] = whole_sum
    ss_copies = []
    for d in range(1, seq):
        slot = ss_seq.at[me_s]
        ss_copies.append(
            remote(slot, slot, ssb_s.at[d - 1], ssb_r.at[d - 1], {"seq": toggle(me_s, d)})
        )
    sent.extend(ss_copies)

    for bit in seq_bits[1:] + [None]:
        for copy in pending:
            copy.wait_recv()
        sent.extend(pending)
        if bit is not None:
            pending = exchange(bit)
    pending = []
    for k, index in enumerate(held[1:]):
        part = blocks(index, mine_first)
        pending.append(
            remote(part, part, pc_s.at[k], pc_r.at[k], {"tp": flip(me_t, core_bit)})
        )
    for copy in pending:
        copy.wait_recv()
    sent.extend(pending)

    chunk = width // 4

    def add_qk(source, first):
        arrived(wqk.at[source], qk_r.at[source])

        @pl.loop(0, width // chunk)
        def _(i):
            at = pl.ds(pl.multiple_of(i * chunk, chunk), chunk)
            product = dot32(down_g[source, at, :], wqk[source])
            if first:
                mqk[at, :] = product
            else:
                mqk[at, :] += product

    started = False
    have = [0]
    for k, bit in enumerate(tp_bits):
        for copy in down_copies[bit]:
            copy.wait_recv()
        sent.extend(down_copies[bit])
        now = []
        if k + 1 < len(tp_bits):
            pass
        have.append(bit)
    for k, bit in enumerate(tp_bits[1:]):
        subs = [m for m in range(1, tp) if m % (2 * bit) == 0]
        now = []
        for sub in subs:
            now += send_down(toggle(me_t, sub), bit, bit + sub - 1)
        for copy in now:
            copy.wait_recv()
        sent.extend(now)

    for hs in range(half):
        source = zh * half + hs
        arrived(wv.at[hs], v_r.at[hs])

        @pl.loop(0, width // chunk)
        def _(i, hs=hs, source=source):
            at = pl.ds(pl.multiple_of(i * chunk, chunk), chunk)
            product = dot32(down_g[source, at, :], wv[hs])
            if hs:
                product += mv[at, :]
            mv[at, :] = product
            if hs == half - 1:
                pv_out[at, :] = product[:, :own].astype(bf)

    pv_copy = remote(pv_out, pv_in, pv_s, pv_r, {"seq": partner})
    sent.append(pv_copy)
    for e in range(tp):
        for j in range(per):
            add_qk(toggle(me_t, e) * per + j, not started)
            started = True

    mixed_qk[...] = mqk[...].astype(bf)
    for copy in ss_copies:
        copy.wait_recv()
    sums = jnp.concatenate([ss_seq[s, 0:1, :] for s in range(seq)], 0)
    inverse = lax.rsqrt(sums / (tp * fcols) + epsilon)
    turned = jnp.transpose(jnp.concatenate([inverse] * (crows // seq), 0))
    for s in range(seq):
        factors[s * crows : (s + 1) * crows, :] = jnp.broadcast_to(
            turned[:, s : s + 1], (crows, HEAD)
        )
    block = 2 * crows

    def project(columns, mixed):
        @pl.loop(0, seq // 2)
        def _(i):
            at = pl.ds(pl.multiple_of(i * block, block), block)
            pooled = pooled_all[pl.ds(i * 2 * tp, 2 * tp)].reshape(block, width)
            product = dot32(pooled, mixed[...])
            for c in range(product.shape[1] // HEAD):
                part = product[:, c * HEAD : (c + 1) * HEAD] * factors[at, :]
                first = columns + c * HEAD
                qkv[at, first : first + HEAD] = part.astype(bf)

    project(0, mixed_qk)
    for i in range(seq // 2):
        extent = (i + 1) * block
        r = lax.broadcasted_iota(jnp.int32, (block, extent), 0) + i * block
        c = lax.broadcasted_iota(jnp.int32, (block, extent), 1)
        for h in range(own // HEAD):
            part = slice(h * HEAD, (h + 1) * HEAD)
            kpart = slice(own + h * HEAD, own + (h + 1) * HEAD)
            weights, denom = weigh(qkv[i * block : extent, part], qkv[:extent, kpart], c <= r)
            terms[h, i * block : extent, :extent] = weights
            denoms[h, i * block : extent, :] = jnp.broadcast_to(denom, (block, HEAD))

    earlier = pooled_all[before_slot(me_s, tp, total), pool_rows - 16 :, :]
    for u in range(2):
        cols = slice(u * fcols // 2, (u + 1) * fcols // 2)
        last = dot32(earlier, down_own[:, cols]).astype(bf).astype(f32)[15:16, :]
        last = jnp.where(me_s > 0, last, 0.0)
        rolled = pltpu.roll(short_cols[pl.ds(0, crows), cols], 1, 0)
        top = lax.broadcasted_iota(jnp.int32, rolled.shape, 0) == 0
        short_cols[pl.ds(0, crows), cols] = jnp.where(top, last, rolled)

    pv_copy.wait_recv()
    mixed_v[...] = (mv[:, own:] + pv_in[...].astype(f32)).astype(bf)
    project(2 * own, mixed_v)
    shifted[0:1, :] = jnp.zeros((1, own), f32)
    for i in range(seq // 2):
        extent = (i + 1) * block
        for h in range(own // HEAD):
            part = slice(h * HEAD, (h + 1) * HEAD)
            vpart = slice(2 * own + h * HEAD, 2 * own + (h + 1) * HEAD)
            out = dot32(terms[h, i * block : extent, :extent], qkv[:extent, vpart])
            shifted[i * block + 1 : extent + 1, part] = out / denoms[h, i * block : extent, :]
    heads_out[...] = shifted[:count, :].astype(bf).reshape(seq, crows, own)

    heads_in[me_s] = heads_out[me_s]
    h_copies = []
    order = sorted(range(1, seq), key=lambda d: -d)
    for d in order:
        dest = toggle(me_s, d)
        h_copies.append(
            remote(
                heads_out.at[dest], heads_in.at[me_s], h_s.at[d - 1], h_r.at[d - 1],
                {"seq": dest},
            )
        )
    sent.extend(h_copies)
    in_wout.wait()
    in_wup.wait()
    for copy in h_copies:
        copy.wait_recv()
    for j in range(seq):
        coarse_heads[:, j * own : (j + 1) * own] = heads_in[j]

    def partial(t, store):
        @pl.loop(0, fcols // tile)
        def _(i):
            cols = pl.ds(pl.multiple_of(i * tile, tile), tile)
            wcols = pl.ds(pl.multiple_of(t * fcols + i * tile, tile), tile)
            store(cols, dot32(coarse_heads[...], wout[:, wcols]))

    tp_order = sorted(range(1, tp), key=lambda d: abs(2 * d - tp))
    r1 = {}
    low_bits = tp_bits[::-1]
    for k, bit in enumerate(low_bits):
        for sub in range(tp - bit, 0, -2 * bit):
            dest = toggle(me_t, sub)
            for low in low_bits[:k]:
                r1[sub + low].wait_recv()

            def put(cols, value, sub=sub, k=k):
                for low in low_bits[:k]:
                    value += recv1[sub + low - 1, :, cols].astype(f32)
                send1[sub - 1, :, cols] = value.astype(bf)

            partial(dest, put)
            r1[sub] = remote(
                send1.at[sub - 1], recv1.at[sub - 1], r1_s.at[sub - 1], r1_r.at[sub - 1],
                {"tp": flip(me_t, bit)},
            )
    sent.extend(r1.values())

    def keep(cols, value):
        short_cols[:, cols] += value

    partial(me_t, keep)
    for bit in low_bits:
        r1[bit].wait_recv()
    whole = short_cols[...]
    for bit in low_bits:
        whole += recv1[bit - 1].astype(f32)
    top = lax.broadcasted_iota(jnp.int32, whole.shape, 0) == 0
    state[...] = jnp.where(top & (me_s == 0), 0.0, whole).astype(bf)

    @pl.loop(0, width // tile)
    def _(i):
        cols = pl.ds(pl.multiple_of(i * tile, tile), tile)
        short_cols[:, cols] = dot32(state[...], wup[:, cols])

    r2 = []
    for d in tp_order:
        dest = around(me_t, d, tp)
        part = short_cols[pl.ds(pl.multiple_of(dest * pool_rows, pool_rows), pool_rows), :]
        send2[d - 1] = part.astype(bf)
        r2.append(
            remote(
                send2.at[d - 1], recv2.at[d - 1], r2_s.at[d - 1], r2_r.at[d - 1], {"tp": dest}
            )
        )
    sent.extend(r2)
    lifted = short_cols[pl.ds(pl.multiple_of(me_t * pool_rows, pool_rows), pool_rows), :]
    for copy in r2:
        copy.wait_recv()
    for d in range(1, tp):
        lifted += recv2[d - 1].astype(f32)
    spread = jnp.broadcast_to(lifted[:, None, :], (pool_rows, SHORT, width)).reshape(rows, width)
    result[...] = (fine_state[...].astype(f32) + spread).astype(bf)
    for copy in sent:
        copy.wait_send()


def before_slot(me_s, tp, total):
    return lax.rem(me_s * tp + total - 1, total)


def head_body(
    tokens,
    fine_gain,
    fine_query,
    fine_keyval,
    fine_out,
    down_weight,
    coarse_gain,
    coarse_query,
    coarse_keyval,
    coarse_out,
    up_weight,
):
    seq, tp = lax.axis_size("seq"), lax.axis_size("tp")
    rows, width = tokens.shape
    depth, local_cols = coarse_query.shape
    own = local_cols // seq
    half = seq // 2
    pool_rows = rows // SHORT
    crows = pool_rows * tp
    count = crows * seq
    bf, f32 = jnp.bfloat16, jnp.float32
    V = pltpu.VMEM
    dma = lambda n: pltpu.SemaphoreType.DMA((n,))
    one = pltpu.SemaphoreType.DMA
    anywhere = pl.BlockSpec(memory_space=pl.ANY)
    vmem = pl.BlockSpec(memory_space=pltpu.VMEM)
    return pl.pallas_call(
        functools.partial(section_kernel, seq, tp),
        out_shape=jax.ShapeDtypeStruct((rows, width), bf),
        in_specs=[anywhere, vmem, anywhere, anywhere, anywhere, anywhere, vmem, anywhere,
                  anywhere, anywhere, anywhere],
        out_specs=vmem,
        scratch_shapes=[
            V((2 * rows, width), bf), V(fine_query.shape, bf), V(fine_keyval.shape, bf),
            V(fine_out.shape, bf), V(down_weight.shape, bf), V((seq, width, depth), bf),
            V((seq, depth, 2 * own), bf), V((half, depth, 2 * own), bf),
            V(coarse_out.shape, bf), V(up_weight.shape, bf),
            V((2 * rows, width), bf), V((rows, width), bf), V((2 * rows, 2 * width), bf),
            V((rows, width), bf), V((rows, width), bf), V((seq * tp, pool_rows, width), bf),
            V((width, 2 * own), f32), V((width, 2 * own), f32), V((width, own), bf),
            V((width, own), bf), V((width, 2 * own), bf), V((width, own), bf),
            V((count, 3 * own), bf), V((count, HEAD), f32),
            V((own // HEAD, count, count), bf), V((own // HEAD, count, HEAD), f32),
            V((count + 8, own), f32), V((seq, crows, own), bf), V((seq, crows, own), bf),
            V((crows, local_cols), bf), V((crows, local_cols), f32),
            V((tp, 8, crows), f32), V((seq, 8, crows), f32),
            V((tp - 1, crows, local_cols), bf), V((tp - 1, crows, local_cols), bf),
            V((crows, local_cols), bf),
            V((tp - 1, pool_rows, width), bf), V((tp - 1, pool_rows, width), bf),
            dma(7), one(()), one(()), dma(2 * (seq - 1)), dma(seq), dma(2 * (half - 1)), dma(half),
            dma(seq - seq // tp), dma(seq - seq // tp), dma(tp - 1), dma(tp - 1),
            dma(seq - 1), dma(seq - 1), dma(seq - 1), dma(seq - 1),
            dma(tp - 1), dma(tp - 1), dma(seq - 1), dma(seq - 1), one(()), one(()),
            dma(seq - 1), dma(seq - 1), dma(tp - 1), dma(tp - 1), dma(tp - 1), dma(tp - 1),
        ],
        compiler_params=pltpu.CompilerParams(
            collective_id=0, has_side_effects=True, vmem_limit_bytes=62 * 1024 * 1024
        ),
    )(tokens, fine_gain[None], fine_query, fine_keyval, fine_out, down_weight, coarse_gain[None],
      coarse_query, jnp.transpose(coarse_keyval, (1, 0, 2)), coarse_out, up_weight)


def chosen(*args):
    seq, tp = lax.axis_size("seq"), lax.axis_size("tp")
    local_heads = args[7].shape[1] // HEAD
    powers = seq & (seq - 1) == 0 and tp & (tp - 1) == 0 and seq > 1 and tp > 1
    square = args[10].shape[0] == args[10].shape[1] == args[7].shape[1]
    paired = seq % tp == 0 and seq > 2 and args[7].shape[0] * (seq // tp) == args[7].shape[1]
    paired = paired and args[0].shape[0] // SHORT * tp == HEAD
    if local_heads % seq == 0 and args[0].shape[0] == WINDOW and powers and square and paired:
        return head_body(*args)
    return body(*args)


def solution(mesh):
    return jax.shard_map(
        chosen,
        mesh=mesh,
        in_specs=(
            P(("seq", "tp"), None),
            P(),
            P(),
            P(),
            P(),
            P(None, "tp"),
            P(),
            P("seq", "tp"),
            P("seq", None, "tp"),
            P("tp", None),
            P("tp", None),
        ),
        out_specs=P(("seq", "tp"), None),
        check_vma=False,
    )
```

```python
import functools
import math

import jax
import jax.numpy as jnp
from jax import lax
from jax.experimental import pallas as pl
from jax.experimental.pallas import tpu as pltpu
from jax.sharding import PartitionSpec as P

HEAD = 128
WINDOW = 256
SHORT = 8


epsilon = 1e-06
big_negative = -1e30


def from_behind(array, axis, by):
    size = lax.axis_size(axis)
    pairs = [(i, i + by) for i in range(size) if 0 <= i + by < size]
    return lax.ppermute(array, axis, pairs)


def normalize(values, scale_gain):
    mean_square = jnp.mean(values * values, axis=-1, keepdims=True)
    return values * lax.rsqrt(mean_square + epsilon) * scale_gain


def online_update(state, query_heads, key_piece, value_piece, query_index):
    running_max, running_sum, accumulate = state
    scale = 1.0 / math.sqrt(HEAD)
    scores = (
        jnp.einsum("qhd,khd->hqk", query_heads, key_piece, preferred_element_type=jnp.float32)
        * scale
    )
    key_index = jnp.arange(key_piece.shape[0], dtype=jnp.int32)
    allowed = key_index[None, :] <= query_index[:, None]
    scores = jnp.where(allowed[None], scores, big_negative)
    new_max = jnp.maximum(running_max, jnp.max(scores, axis=-1))
    terms = jnp.where(allowed[None], jnp.exp(scores - new_max[..., None]), 0.0)
    new_sum = jnp.sum(terms, axis=-1)
    product = jnp.einsum(
        "hqk,khd->hqd", terms.astype(jnp.bfloat16), value_piece, preferred_element_type=jnp.float32
    )
    return (new_max, new_sum, product)


def body(
    tokens,
    fine_gain,
    fine_query,
    fine_keyval,
    fine_out,
    down_weight,
    coarse_gain,
    coarse_query,
    coarse_keyval,
    coarse_out,
    up_weight,
):
    tok_rows = tokens.shape[0]
    width = tokens.shape[1]
    fine_heads = width // HEAD
    scale = 1.0 / math.sqrt(HEAD)
    start_row = lax.axis_index(("seq", "tp")) * tok_rows
    inputs = tokens.astype(jnp.float32)
    normed = normalize(inputs, fine_gain).astype(jnp.bfloat16)
    queries = jnp.dot(normed, fine_query, preferred_element_type=jnp.float32).astype(jnp.bfloat16)
    keyvals = jnp.dot(normed, fine_keyval, preferred_element_type=jnp.float32).astype(jnp.bfloat16)
    earlier = from_behind(keyvals, ("seq", "tp"), 1)
    key_rows = jnp.concatenate([earlier, keyvals], 0)
    span = key_rows.shape[0]
    key_heads = key_rows[:, :width].reshape(span, fine_heads, HEAD)
    value_heads = key_rows[:, width:].reshape(span, fine_heads, HEAD)
    query_heads = queries.reshape(tok_rows, fine_heads, HEAD)
    scores = (
        jnp.einsum("qhd,khd->hqk", query_heads, key_heads, preferred_element_type=jnp.float32)
        * scale
    )
    row_index = jnp.arange(tok_rows, dtype=jnp.int32)[:, None]
    col_index = jnp.arange(span, dtype=jnp.int32)[None, :]
    offset = row_index + WINDOW - col_index
    allowed = (offset >= 0) & (offset < WINDOW) & (start_row - WINDOW + col_index >= 0)
    scores = jnp.where(allowed[None], scores, big_negative)
    peak = jnp.max(scores, axis=-1, keepdims=True)
    terms = jnp.where(allowed[None], jnp.exp(scores - peak), 0.0)
    denom = jnp.sum(terms, axis=-1)
    mixed = jnp.einsum(
        "hqk,khd->qhd", terms.astype(jnp.bfloat16), value_heads, preferred_element_type=jnp.float32
    )
    local = (mixed / jnp.transpose(denom)[..., None]).reshape(tok_rows, width).astype(jnp.bfloat16)
    fine_state = (inputs + jnp.dot(local, fine_out, preferred_element_type=jnp.float32)).astype(
        jnp.bfloat16
    )
    pooled = jnp.mean(
        fine_state.astype(jnp.float32).reshape(tok_rows // SHORT, SHORT, width), axis=1
    ).astype(jnp.bfloat16)
    pooled_all = lax.all_gather(pooled, "tp", axis=0, tiled=True)
    short_cols = jnp.dot(pooled_all, down_weight, preferred_element_type=jnp.float32).astype(
        jnp.bfloat16
    )
    shortened = lax.all_gather(short_cols, "tp", axis=1, tiled=True)
    coarse_normed = normalize(shortened.astype(jnp.float32), coarse_gain).astype(jnp.bfloat16)
    coarse_rows = coarse_normed.shape[0]
    local_cols = coarse_query.shape[1]
    local_heads = local_cols // HEAD
    query_rows = lax.all_gather(coarse_query, "seq", axis=0, tiled=True)
    keyval_rows = lax.all_gather(coarse_keyval, "seq", axis=0, tiled=True)
    count = query_rows.shape[0]
    query_sum = jnp.dot(coarse_normed, query_rows, preferred_element_type=jnp.float32)
    keyval_sum = jnp.dot(
        coarse_normed,
        keyval_rows.reshape(count, 2 * local_cols),
        preferred_element_type=jnp.float32,
    )
    coarse_queries = query_sum.astype(jnp.bfloat16).reshape(coarse_rows, local_heads, HEAD)
    coarse_kv = keyval_sum.astype(jnp.bfloat16).reshape(coarse_rows, 2, local_cols)
    my_first = lax.axis_index("seq") * coarse_rows
    query_index = my_first + jnp.arange(coarse_rows, dtype=jnp.int32)
    initial = (
        jnp.full((local_heads, coarse_rows), big_negative, jnp.float32),
        jnp.zeros((local_heads, coarse_rows), jnp.float32),
        jnp.zeros((local_heads, coarse_rows, HEAD), jnp.float32),
    )
    piece = lax.all_gather(coarse_kv, "seq", axis=0, tiled=True)
    count = piece.shape[0]
    key_piece = piece[:, 0].reshape(count, local_heads, HEAD)
    value_piece = piece[:, 1].reshape(count, local_heads, HEAD)
    final = lax.cond(
        jnp.int32(0) < my_first + coarse_rows,
        lambda: online_update(initial, coarse_queries, key_piece, value_piece, query_index),
        lambda: initial,
    )
    head_out = final[2] / final[1][..., None]
    coarse_heads = (
        jnp.transpose(head_out, (1, 0, 2)).reshape(coarse_rows, local_cols).astype(jnp.bfloat16)
    )
    partials = jnp.dot(coarse_heads, coarse_out, preferred_element_type=jnp.float32)
    attended = lax.psum_scatter(
        partials.astype(jnp.bfloat16), "tp", scatter_dimension=1, tiled=True
    ).astype(jnp.float32)
    coarse_state = (short_cols.astype(jnp.float32) + attended).astype(jnp.bfloat16)
    prior_row = from_behind(coarse_state[coarse_rows - 1 :], "seq", 1)
    delayed = jnp.concatenate([prior_row, coarse_state[: coarse_rows - 1]], 0)
    lifted = lax.psum_scatter(
        jnp.dot(delayed, up_weight, preferred_element_type=jnp.float32).astype(jnp.bfloat16),
        "tp",
        scatter_dimension=0,
        tiled=True,
    ).astype(jnp.float32)
    result = fine_state.astype(jnp.float32) + jnp.repeat(lifted, SHORT, axis=0)
    return result.astype(jnp.bfloat16)


def flip(index, bit):
    return index + bit - 2 * bit * lax.rem(lax.div(index, jnp.int32(bit)), jnp.int32(2))


def bits_of(size):
    out, bit = [], size // 2
    while bit:
        out.append(bit)
        bit //= 2
    return out


def dot32(left, right):
    return jnp.dot(left, right, preferred_element_type=jnp.float32)


def dot_t(left, right):
    return lax.dot_general(
        left, right, (((1,), (1,)), ((), ())), preferred_element_type=jnp.float32
    )


BULK_QK = (4, 2, 4, 0, 1, 2, 3)
BULK_V = (1, 1, 2)
BULK_DOWN = (0, 3, 4, 5)


def section_kernel(
    seq, tp,
    tokens, fine_gain, fine_query, fine_keyval, fine_out, down_weight, coarse_gain, coarse_query,
    coarse_kv, coarse_out, up_weight,
    result,
    both, wq, wkv, wo, down_own, down_g, wqk, wv, wout, wup,
    normed, queries, key_rows, local, fine_state, pooled_all, mv, pv_out, pv_in, mixed_qk,
    mixed_v, qkv, factors, terms, denoms, shifted, heads_out, heads_in, coarse_heads, short_cols,
    ss_tp, ss_seq, send1, recv1, state, send2, recv2,
    load_sem, halo_s, halo_r, qk_s, qk_r, v_s, v_r, d_s, d_r, pa_s, pa_r, pb_s, pb_r, pc_s, pc_r,
    ssa_s, ssa_r, ssb_s, ssb_r, pv_s, pv_r, h_s, h_r, r1_s, r1_r, r2_s, r2_r,
):
    me_s = lax.axis_index("seq")
    me_t = lax.axis_index("tp")
    rows, width = tokens.shape
    scale = 1.0 / math.sqrt(HEAD)
    total = seq * tp
    lin = me_s * tp + me_t
    after = lax.rem(lin + 1, total)
    before = lax.rem(lin + total - 1, total)
    bf, f32 = jnp.bfloat16, jnp.float32

    def around(index, step, size):
        return lax.rem(index + step, size)

    def toggle(index, mask):
        bit = 1
        while bit <= mask:
            if mask & bit:
                index = flip(index, bit)
            bit *= 2
        return index

    def remote(src, dst, send, recv, device):
        copy = pltpu.make_async_remote_copy(
            src_ref=src, dst_ref=dst, send_sem=send, recv_sem=recv,
            device_id=device, device_id_type=pl.DeviceIdType.MESH,
        )
        copy.start()
        return copy

    def load(src, dst, sem):
        copy = pltpu.make_async_copy(src, dst, sem)
        copy.start()
        return copy

    def arrived(dst, sem):
        pltpu.make_async_copy(dst, dst, sem).wait()

    def linear(index):
        return {"seq": lax.div(index, tp), "tp": lax.rem(index, tp)}

    depth = coarse_query.shape[0]
    own = coarse_query.shape[1] // seq
    fcols = down_own.shape[1]
    half = seq // 2
    zh = lax.div(me_s, half)
    in_half = lax.rem(me_s, half)
    partner = flip(me_s, half)
    pool_rows = rows // SHORT
    crows = pool_rows * tp
    count = crows * seq
    tile = 2 * HEAD

    def head_cols(dest):
        return pl.ds(pl.multiple_of(dest * own, own), own)

    def block_of(source):
        return pl.ds(pl.multiple_of(source * depth, depth), depth)

    barrier = pltpu.get_barrier_semaphore()
    peers = [{"seq": around(me_s, d, seq)} for d in range(1, seq)]
    peers += [{"tp": around(me_t, d, tp)} for d in range(1, tp)]
    peers += [linear(after), linear(before)]
    in_tokens = load(tokens, both.at[pl.ds(rows, rows)], load_sem.at[0])
    in_down = load(down_weight, down_own, load_sem.at[4])
    in_wq = load(fine_query, wq, load_sem.at[2])
    in_wkv = load(fine_keyval, wkv, load_sem.at[1])
    in_wo = load(fine_out, wo, load_sem.at[3])
    for pl_part, source in ((0, coarse_query), (1, coarse_kv.at[0])):
        load(source.at[:, head_cols(me_s)], wqk.at[block_of(me_s), pl.ds(pl_part * own, own)],
             qk_r.at[me_s])
    for k, head in enumerate((partner, me_s)):
        load(coarse_kv.at[1, :, head_cols(head)], wv.at[block_of(in_half), pl.ds(k * own, own)],
             v_r.at[in_half])
    in_wout = load(coarse_out, wout, load_sem.at[5])
    in_wup = load(up_weight, wup, load_sem.at[6])
    for peer in peers:
        pl.semaphore_signal(barrier, inc=1, device_id=peer, device_id_type=pl.DeviceIdType.MESH)
    pl.semaphore_wait(barrier, len(peers))

    sent = []
    halo = remote(tokens, both.at[pl.ds(0, rows)], halo_s, halo_r, linear(after))

    def send_qk(offsets):
        for d in offsets:
            dest = toggle(me_s, d)
            for k, source in enumerate((coarse_query, coarse_kv.at[0])):
                sent.append(
                    remote(
                        source.at[:, head_cols(dest)], wqk.at[block_of(me_s), pl.ds(k * own, own)],
                        qk_s.at[2 * (d - 1) + k], qk_r.at[me_s], {"seq": dest},
                    )
                )

    def send_v(offsets):
        for d in offsets:
            dest = toggle(me_s, d)
            for k, head in enumerate((flip(dest, half), dest)):
                sent.append(
                    remote(
                        coarse_kv.at[1, :, head_cols(head)],
                        wv.at[block_of(in_half), pl.ds(k * own, own)],
                        v_s.at[2 * (d - 1) + k], v_r.at[in_half], {"seq": dest},
                    )
                )

    tp_bits = bits_of(tp)
    pieces = 4
    span = width // pieces
    in_down.wait()
    cgain = coarse_gain[:, pl.ds(pl.multiple_of(me_t * fcols, fcols), fcols)]

    def slot_cols(slot):
        return pl.ds(pl.multiple_of(slot * fcols, fcols), fcols)

    def down_piece(slot, bit, number, r):
        part = down_g.at[pl.ds(r * span, span), slot_cols(slot)]
        at = number * pieces + r
        return remote(part, part, d_s.at[at], d_r.at[at], {"tp": flip(me_t, bit)})

    direct = {}

    def launch_down(r):
        at = pl.ds(r * span, span)
        down_g[at, slot_cols(me_t)] = (down_own[at, :].astype(f32) * cgain).astype(bf)
        for bit in tp_bits:
            direct[r, bit] = down_piece(me_t, bit, bit - 1, r)

    def forward_down(r):
        direct[r, tp_bits[0]].wait_recv()
        for bit in tp_bits[1:]:
            if bit != tp_bits[1]:
                for copy in later[r]:
                    copy.wait_recv()
            later.setdefault(r, []).extend(
                down_piece(toggle(me_t, sub), bit, bit + sub - 1, r)
                for sub in range(2 * bit, tp, 2 * bit)
            )
            later[r].append(direct[r, bit])

    later = {}

    def finish_down(r):
        for copy in later[r]:
            copy.wait_recv()
        sent.extend(later[r] + [direct[r, tp_bits[0]]])

    bulk = {}
    for d in range(1, seq):
        bulk.setdefault(BULK_QK[d - 1] if seq == 8 else 0, []).append(("qk", d))
    for d in range(1, half):
        bulk.setdefault(BULK_V[d - 1] if seq == 8 else 0, []).append(("v", d))
    for r in range(pieces):
        bulk.setdefault(BULK_DOWN[r], []).append(("down", r))

    def issue(stage):
        for kind, d in bulk.get(stage, []):
            if kind == "qk":
                send_qk([d])
            elif kind == "v":
                send_v([d])
            else:
                launch_down(d)

    issue(0)

    gain = fine_gain[...]

    def norm_rows(first):
        values = both[pl.ds(first, rows), :].astype(f32)
        normed[pl.ds(first, rows), :] = normalize(values, gain).astype(bf)

    in_tokens.wait()
    norm_rows(rows)
    in_wq.wait()

    @pl.loop(0, width // tile)
    def _(i):
        cols = pl.ds(pl.multiple_of(i * tile, tile), tile)
        queries[:, cols] = dot32(normed[rows:, :], wq[:, cols]).astype(bf)

    in_wkv.wait()

    def project_rows(first):
        @pl.loop(0, 2 * width // tile)
        def _(i):
            cols = pl.ds(pl.multiple_of(i * tile, tile), tile)
            key_rows[pl.ds(first, rows), cols] = dot32(
                normed[pl.ds(first, rows), :], wkv[:, cols]
            ).astype(bf)

    project_rows(rows)
    issue(1)
    halo.wait()
    norm_rows(0)
    project_rows(0)
    issue(2)

    row_index = lax.broadcasted_iota(jnp.int32, (rows, 2 * rows), 0)
    col_index = lax.broadcasted_iota(jnp.int32, (rows, 2 * rows), 1)
    offset = row_index + rows - col_index
    allowed = (offset >= 0) & (offset < WINDOW) & (lin * rows - rows + col_index >= 0)

    def weigh(query, key, mask):
        scores = jnp.where(mask, dot_t(query, key) * scale, big_negative)
        peak = jnp.max(scores, axis=-1, keepdims=True)
        weights = jnp.where(mask, jnp.exp(scores - peak), 0.0)
        return weights.astype(bf), jnp.sum(weights, axis=-1, keepdims=True)

    @pl.loop(0, width // HEAD)
    def _(h):
        cols = pl.ds(pl.multiple_of(h * HEAD, HEAD), HEAD)
        vcols = pl.ds(pl.multiple_of(width + h * HEAD, HEAD), HEAD)
        weights, denom = weigh(queries[:, cols], key_rows[:, cols], allowed)
        local[:, cols] = (dot32(weights, key_rows[:, vcols]) / denom).astype(bf)

    in_wo.wait()

    @pl.loop(0, width // tile)
    def _(i):
        cols = pl.ds(pl.multiple_of(i * tile, tile), tile)
        value = both[rows:, cols].astype(f32) + dot32(local[...], wo[:, cols])
        value = value.astype(bf)
        fine_state[:, cols] = value
        mean = jnp.mean(value.astype(f32).reshape(pool_rows, SHORT, tile), axis=1)
        pooled_all[lin, :, cols] = mean.astype(bf)

    group = []
    for d in range(1, tp):
        slot = pooled_all.at[lin]
        group.append(remote(slot, slot, pa_s.at[d - 1], pa_r.at[d - 1], {"tp": toggle(me_t, d)}))
    issue(3)
    for copy in group:
        copy.wait_recv()
    sent.extend(group)

    core_bit = tp_bits[-1]
    share = tp // 2
    mine_first = lax.rem(me_t, 2) * share

    def blocks(first_s, offset_t):
        return pooled_all.at[pl.ds(first_s * tp + offset_t, share)]

    seq_bits = bits_of(seq)
    gather = {}

    def spread_block(mask):
        for bit in seq_bits:
            if mask == 0 or bit < (mask & -mask):
                part = blocks(toggle(me_s, mask), mine_first)
                at = (mask | bit) - 1
                gather[at + 1] = remote(
                    part, part, pb_s.at[at], pb_r.at[at], {"seq": flip(me_s, bit)}
                )

    spread_block(0)
    issue(4)

    mine = pooled_all[pl.ds(me_s * tp, tp)].reshape(crows, width)
    square_sum = jnp.zeros((8, crows), f32)
    for u in range(2):
        cols = slice(u * fcols // 2, (u + 1) * fcols // 2)
        wide = dot32(mine, down_own[:, cols]).astype(bf).astype(f32)
        short_cols[pl.ds(0, crows), cols] = wide
        square_sum += lax.dot_general(
            jnp.ones((8, fcols // 2), f32), wide * wide, (((1,), (1,)), ((), ())),
            preferred_element_type=f32, precision=lax.Precision.HIGHEST,
        )
    ss_tp[me_t] = square_sum
    group = []
    for d in range(1, tp):
        slot = ss_tp.at[me_t]
        group.append(remote(slot, slot, ssa_s.at[d - 1], ssa_r.at[d - 1], {"tp": toggle(me_t, d)}))
    evens = sorted(range(2, seq, 2), key=lambda m: (bin(m).count("1"), m))
    for at, mask in enumerate(evens):
        gather[mask].wait_recv()
        spread_block(mask)
        issue(5 + at)

    for piece in range(pieces):
        forward_down(piece)
    for copy in group:
        copy.wait_recv()
    sent.extend(group)
    whole_sum = ss_tp[0]
    for t in range(1, tp):
        whole_sum += ss_tp[t]
    ss_seq[me_s] = whole_sum
    ss_copies = []
    for d in range(1, seq):
        slot = ss_seq.at[me_s]
        ss_copies.append(
            remote(slot, slot, ssb_s.at[d - 1], ssb_r.at[d - 1], {"seq": toggle(me_s, d)})
        )
    sent.extend(ss_copies)
    for hs in range(half):
        arrived(wv.at[pl.ds(hs * depth, depth)], v_r.at[hs])
    half_cols = pl.ds(pl.multiple_of(zh * half * depth, half * depth), half * depth)
    pv_copies = []
    for piece in range(pieces):
        finish_down(piece)
        at = slice(piece * span, (piece + 1) * span)
        product = dot32(down_g[at, half_cols], wv[...])
        pv_out[at, :] = product[:, :own].astype(bf)
        mv[at, :] = product[:, own:]
        at = pl.ds(piece * span, span)
        pv_copies.append(
            remote(pv_out.at[at], pv_in.at[at], pv_s.at[piece], pv_r.at[piece], {"seq": partner})
        )
    sent.extend(pv_copies)
    for mask in range(1, seq, 2):
        gather[mask].wait_recv()
    sent.extend(gather.values())
    pending = []
    for k in range(seq - 1):
        part = blocks(toggle(me_s, k + 1), mine_first)
        pending.append(
            remote(part, part, pc_s.at[k], pc_r.at[k], {"tp": flip(me_t, core_bit)})
        )
    for copy in pending:
        copy.wait_recv()
    sent.extend(pending)

    for source in range(seq):
        arrived(wqk.at[pl.ds(source * depth, depth)], qk_r.at[source])

    @pl.loop(0, pieces)
    def _(i):
        at = pl.ds(pl.multiple_of(i * span, span), span)
        mixed_qk[at, :] = dot32(down_g[at, :], wqk[...]).astype(bf)

    for copy in ss_copies:
        copy.wait_recv()
    sums = jnp.concatenate([ss_seq[s, 0:1, :] for s in range(seq)], 0)
    inverse = lax.rsqrt(sums / (tp * fcols) + epsilon)
    turned = jnp.transpose(jnp.concatenate([inverse] * (crows // seq), 0))
    for s in range(seq):
        factors[s * crows : (s + 1) * crows, :] = jnp.broadcast_to(
            turned[:, s : s + 1], (crows, HEAD)
        )
    block = 2 * crows

    def project(columns, mixed):
        @pl.loop(0, seq // 2)
        def _(i):
            at = pl.ds(pl.multiple_of(i * block, block), block)
            pooled = pooled_all[pl.ds(i * 2 * tp, 2 * tp)].reshape(block, width)
            product = dot32(pooled, mixed[...])
            for c in range(product.shape[1] // HEAD):
                part = product[:, c * HEAD : (c + 1) * HEAD] * factors[at, :]
                first = columns + c * HEAD
                qkv[at, first : first + HEAD] = part.astype(bf)

    project(0, mixed_qk)
    for i in range(seq // 2):
        extent = (i + 1) * block
        r = lax.broadcasted_iota(jnp.int32, (block, extent), 0) + i * block
        c = lax.broadcasted_iota(jnp.int32, (block, extent), 1)
        for h in range(own // HEAD):
            part = slice(h * HEAD, (h + 1) * HEAD)
            kpart = slice(own + h * HEAD, own + (h + 1) * HEAD)
            weights, denom = weigh(qkv[i * block : extent, part], qkv[:extent, kpart], c <= r)
            terms[h, i * block : extent, :extent] = weights
            denoms[h, i * block : extent, :] = jnp.broadcast_to(denom, (block, HEAD))

    earlier = pooled_all[before_slot(me_s, tp, total), pool_rows - 16 :, :]
    for u in range(2):
        cols = slice(u * fcols // 2, (u + 1) * fcols // 2)
        last = dot32(earlier, down_own[:, cols]).astype(bf).astype(f32)[15:16, :]
        last = jnp.where(me_s > 0, last, 0.0)
        rolled = pltpu.roll(short_cols[pl.ds(0, crows), cols], 1, 0)
        top = lax.broadcasted_iota(jnp.int32, rolled.shape, 0) == 0
        short_cols[pl.ds(0, crows), cols] = jnp.where(top, last, rolled)

    for copy in pv_copies:
        copy.wait_recv()
    mixed_v[...] = (mv[...] + pv_in[...].astype(f32)).astype(bf)
    project(2 * own, mixed_v)
    shifted[0:1, :] = jnp.zeros((1, own), f32)
    for i in range(seq // 2):
        extent = (i + 1) * block
        for h in range(own // HEAD):
            part = slice(h * HEAD, (h + 1) * HEAD)
            vpart = slice(2 * own + h * HEAD, 2 * own + (h + 1) * HEAD)
            out = dot32(terms[h, i * block : extent, :extent], qkv[:extent, vpart])
            shifted[i * block + 1 : extent + 1, part] = out / denoms[h, i * block : extent, :]
    heads_out[...] = shifted[:count, :].astype(bf).reshape(seq, crows, own)

    heads_in[me_s] = heads_out[me_s]
    h_copies = []
    order = sorted(range(1, seq), key=lambda d: -d)
    for d in order:
        dest = toggle(me_s, d)
        h_copies.append(
            remote(
                heads_out.at[dest], heads_in.at[me_s], h_s.at[d - 1], h_r.at[d - 1],
                {"seq": dest},
            )
        )
    sent.extend(h_copies)
    in_wout.wait()
    in_wup.wait()
    for copy in h_copies:
        copy.wait_recv()
    for j in range(seq):
        coarse_heads[:, j * own : (j + 1) * own] = heads_in[j]

    def partial(t, store):
        @pl.loop(0, fcols // tile)
        def _(i):
            cols = pl.ds(pl.multiple_of(i * tile, tile), tile)
            wcols = pl.ds(pl.multiple_of(t * fcols + i * tile, tile), tile)
            store(cols, dot32(coarse_heads[...], wout[:, wcols]))

    tp_order = sorted(range(1, tp), key=lambda d: abs(2 * d - tp))
    r1 = {}
    low_bits = tp_bits[::-1]
    for k, bit in enumerate(low_bits):
        for sub in range(tp - bit, 0, -2 * bit):
            dest = toggle(me_t, sub)
            for low in low_bits[:k]:
                r1[sub + low].wait_recv()

            def put(cols, value, sub=sub, k=k):
                for low in low_bits[:k]:
                    value += recv1[sub + low - 1, :, cols].astype(f32)
                send1[sub - 1, :, cols] = value.astype(bf)

            partial(dest, put)
            r1[sub] = remote(
                send1.at[sub - 1], recv1.at[sub - 1], r1_s.at[sub - 1], r1_r.at[sub - 1],
                {"tp": flip(me_t, bit)},
            )
    sent.extend(r1.values())

    def keep(cols, value):
        short_cols[:, cols] += value

    partial(me_t, keep)
    for bit in low_bits:
        r1[bit].wait_recv()
    whole = short_cols[...]
    for bit in low_bits:
        whole += recv1[bit - 1].astype(f32)
    top = lax.broadcasted_iota(jnp.int32, whole.shape, 0) == 0
    state[...] = jnp.where(top & (me_s == 0), 0.0, whole).astype(bf)

    @pl.loop(0, width // tile)
    def _(i):
        cols = pl.ds(pl.multiple_of(i * tile, tile), tile)
        short_cols[:, cols] = dot32(state[...], wup[:, cols])

    r2 = []
    for d in tp_order:
        dest = around(me_t, d, tp)
        part = short_cols[pl.ds(pl.multiple_of(dest * pool_rows, pool_rows), pool_rows), :]
        send2[d - 1] = part.astype(bf)
        r2.append(
            remote(
                send2.at[d - 1], recv2.at[d - 1], r2_s.at[d - 1], r2_r.at[d - 1], {"tp": dest}
            )
        )
    sent.extend(r2)
    lifted = short_cols[pl.ds(pl.multiple_of(me_t * pool_rows, pool_rows), pool_rows), :]
    for copy in r2:
        copy.wait_recv()
    for d in range(1, tp):
        lifted += recv2[d - 1].astype(f32)
    spread = jnp.broadcast_to(lifted[:, None, :], (pool_rows, SHORT, width)).reshape(rows, width)
    result[...] = (fine_state[...].astype(f32) + spread).astype(bf)
    for copy in sent:
        copy.wait_send()


def before_slot(me_s, tp, total):
    return lax.rem(me_s * tp + total - 1, total)


def head_body(
    tokens,
    fine_gain,
    fine_query,
    fine_keyval,
    fine_out,
    down_weight,
    coarse_gain,
    coarse_query,
    coarse_keyval,
    coarse_out,
    up_weight,
):
    seq, tp = lax.axis_size("seq"), lax.axis_size("tp")
    rows, width = tokens.shape
    depth, local_cols = coarse_query.shape
    own = local_cols // seq
    half = seq // 2
    pool_rows = rows // SHORT
    crows = pool_rows * tp
    count = crows * seq
    bf, f32 = jnp.bfloat16, jnp.float32
    V = pltpu.VMEM
    dma = lambda n: pltpu.SemaphoreType.DMA((n,))
    one = pltpu.SemaphoreType.DMA
    anywhere = pl.BlockSpec(memory_space=pl.ANY)
    vmem = pl.BlockSpec(memory_space=pltpu.VMEM)
    return pl.pallas_call(
        functools.partial(section_kernel, seq, tp),
        out_shape=jax.ShapeDtypeStruct((rows, width), bf),
        in_specs=[anywhere, vmem, anywhere, anywhere, anywhere, anywhere, vmem, anywhere,
                  anywhere, anywhere, anywhere],
        out_specs=vmem,
        scratch_shapes=[
            V((2 * rows, width), bf), V(fine_query.shape, bf), V(fine_keyval.shape, bf),
            V(fine_out.shape, bf), V(down_weight.shape, bf), V((width, seq * depth), bf),
            V((seq * depth, 2 * own), bf), V((half * depth, 2 * own), bf),
            V(coarse_out.shape, bf), V(up_weight.shape, bf),
            V((2 * rows, width), bf), V((rows, width), bf), V((2 * rows, 2 * width), bf),
            V((rows, width), bf), V((rows, width), bf), V((seq * tp, pool_rows, width), bf),
            V((width, own), f32), V((width, own), bf),
            V((width, own), bf), V((width, 2 * own), bf), V((width, own), bf),
            V((count, 3 * own), bf), V((count, HEAD), f32),
            V((own // HEAD, count, count), bf), V((own // HEAD, count, HEAD), f32),
            V((count + 8, own), f32), V((seq, crows, own), bf), V((seq, crows, own), bf),
            V((crows, local_cols), bf), V((crows, local_cols), f32),
            V((tp, 8, crows), f32), V((seq, 8, crows), f32),
            V((tp - 1, crows, local_cols), bf), V((tp - 1, crows, local_cols), bf),
            V((crows, local_cols), bf),
            V((tp - 1, pool_rows, width), bf), V((tp - 1, pool_rows, width), bf),
            dma(7), one(()), one(()), dma(2 * (seq - 1)), dma(seq), dma(2 * (half - 1)), dma(half),
            dma(4 * (tp - 1)), dma(4 * (tp - 1)), dma(tp - 1), dma(tp - 1),
            dma(seq - 1), dma(seq - 1), dma(seq - 1), dma(seq - 1),
            dma(tp - 1), dma(tp - 1), dma(seq - 1), dma(seq - 1), dma(4), dma(4),
            dma(seq - 1), dma(seq - 1), dma(tp - 1), dma(tp - 1), dma(tp - 1), dma(tp - 1),
        ],
        compiler_params=pltpu.CompilerParams(
            collective_id=0, has_side_effects=True, vmem_limit_bytes=62 * 1024 * 1024
        ),
    )(tokens, fine_gain[None], fine_query, fine_keyval, fine_out, down_weight, coarse_gain[None],
      coarse_query, jnp.transpose(coarse_keyval, (1, 0, 2)), coarse_out, up_weight)


def chosen(*args):
    seq, tp = lax.axis_size("seq"), lax.axis_size("tp")
    local_heads = args[7].shape[1] // HEAD
    powers = seq & (seq - 1) == 0 and tp & (tp - 1) == 0 and seq > 1 and tp > 1
    square = args[10].shape[0] == args[10].shape[1] == args[7].shape[1]
    paired = seq % tp == 0 and seq > 2 and args[7].shape[0] * (seq // tp) == args[7].shape[1]
    paired = paired and args[0].shape[0] // SHORT * tp == HEAD
    if local_heads % seq == 0 and args[0].shape[0] == WINDOW and powers and square and paired:
        return head_body(*args)
    return body(*args)


def solution(mesh):
    return jax.shard_map(
        chosen,
        mesh=mesh,
        in_specs=(
            P(("seq", "tp"), None),
            P(),
            P(),
            P(),
            P(),
            P(None, "tp"),
            P(),
            P("seq", "tp"),
            P("seq", None, "tp"),
            P("tp", None),
            P("tp", None),
        ),
        out_specs=P(("seq", "tp"), None),
        check_vma=False,
    )
```

```python
import functools
import math

import jax
import jax.numpy as jnp
from jax import lax
from jax.experimental import pallas as pl
from jax.experimental.pallas import tpu as pltpu
from jax.sharding import PartitionSpec as P

HEAD = 128
WINDOW = 256
SHORT = 8


epsilon = 1e-06
big_negative = -1e30


def from_behind(array, axis, by):
    size = lax.axis_size(axis)
    pairs = [(i, i + by) for i in range(size) if 0 <= i + by < size]
    return lax.ppermute(array, axis, pairs)


def normalize(values, scale_gain):
    mean_square = jnp.mean(values * values, axis=-1, keepdims=True)
    return values * lax.rsqrt(mean_square + epsilon) * scale_gain


def online_update(state, query_heads, key_piece, value_piece, query_index):
    running_max, running_sum, accumulate = state
    scale = 1.0 / math.sqrt(HEAD)
    scores = (
        jnp.einsum("qhd,khd->hqk", query_heads, key_piece, preferred_element_type=jnp.float32)
        * scale
    )
    key_index = jnp.arange(key_piece.shape[0], dtype=jnp.int32)
    allowed = key_index[None, :] <= query_index[:, None]
    scores = jnp.where(allowed[None], scores, big_negative)
    new_max = jnp.maximum(running_max, jnp.max(scores, axis=-1))
    terms = jnp.where(allowed[None], jnp.exp(scores - new_max[..., None]), 0.0)
    new_sum = jnp.sum(terms, axis=-1)
    product = jnp.einsum(
        "hqk,khd->hqd", terms.astype(jnp.bfloat16), value_piece, preferred_element_type=jnp.float32
    )
    return (new_max, new_sum, product)


def body(
    tokens,
    fine_gain,
    fine_query,
    fine_keyval,
    fine_out,
    down_weight,
    coarse_gain,
    coarse_query,
    coarse_keyval,
    coarse_out,
    up_weight,
):
    tok_rows = tokens.shape[0]
    width = tokens.shape[1]
    fine_heads = width // HEAD
    scale = 1.0 / math.sqrt(HEAD)
    start_row = lax.axis_index(("seq", "tp")) * tok_rows
    inputs = tokens.astype(jnp.float32)
    normed = normalize(inputs, fine_gain).astype(jnp.bfloat16)
    queries = jnp.dot(normed, fine_query, preferred_element_type=jnp.float32).astype(jnp.bfloat16)
    keyvals = jnp.dot(normed, fine_keyval, preferred_element_type=jnp.float32).astype(jnp.bfloat16)
    earlier = from_behind(keyvals, ("seq", "tp"), 1)
    key_rows = jnp.concatenate([earlier, keyvals], 0)
    span = key_rows.shape[0]
    key_heads = key_rows[:, :width].reshape(span, fine_heads, HEAD)
    value_heads = key_rows[:, width:].reshape(span, fine_heads, HEAD)
    query_heads = queries.reshape(tok_rows, fine_heads, HEAD)
    scores = (
        jnp.einsum("qhd,khd->hqk", query_heads, key_heads, preferred_element_type=jnp.float32)
        * scale
    )
    row_index = jnp.arange(tok_rows, dtype=jnp.int32)[:, None]
    col_index = jnp.arange(span, dtype=jnp.int32)[None, :]
    offset = row_index + WINDOW - col_index
    allowed = (offset >= 0) & (offset < WINDOW) & (start_row - WINDOW + col_index >= 0)
    scores = jnp.where(allowed[None], scores, big_negative)
    peak = jnp.max(scores, axis=-1, keepdims=True)
    terms = jnp.where(allowed[None], jnp.exp(scores - peak), 0.0)
    denom = jnp.sum(terms, axis=-1)
    mixed = jnp.einsum(
        "hqk,khd->qhd", terms.astype(jnp.bfloat16), value_heads, preferred_element_type=jnp.float32
    )
    local = (mixed / jnp.transpose(denom)[..., None]).reshape(tok_rows, width).astype(jnp.bfloat16)
    fine_state = (inputs + jnp.dot(local, fine_out, preferred_element_type=jnp.float32)).astype(
        jnp.bfloat16
    )
    pooled = jnp.mean(
        fine_state.astype(jnp.float32).reshape(tok_rows // SHORT, SHORT, width), axis=1
    ).astype(jnp.bfloat16)
    pooled_all = lax.all_gather(pooled, "tp", axis=0, tiled=True)
    short_cols = jnp.dot(pooled_all, down_weight, preferred_element_type=jnp.float32).astype(
        jnp.bfloat16
    )
    shortened = lax.all_gather(short_cols, "tp", axis=1, tiled=True)
    coarse_normed = normalize(shortened.astype(jnp.float32), coarse_gain).astype(jnp.bfloat16)
    coarse_rows = coarse_normed.shape[0]
    local_cols = coarse_query.shape[1]
    local_heads = local_cols // HEAD
    query_rows = lax.all_gather(coarse_query, "seq", axis=0, tiled=True)
    keyval_rows = lax.all_gather(coarse_keyval, "seq", axis=0, tiled=True)
    count = query_rows.shape[0]
    query_sum = jnp.dot(coarse_normed, query_rows, preferred_element_type=jnp.float32)
    keyval_sum = jnp.dot(
        coarse_normed,
        keyval_rows.reshape(count, 2 * local_cols),
        preferred_element_type=jnp.float32,
    )
    coarse_queries = query_sum.astype(jnp.bfloat16).reshape(coarse_rows, local_heads, HEAD)
    coarse_kv = keyval_sum.astype(jnp.bfloat16).reshape(coarse_rows, 2, local_cols)
    my_first = lax.axis_index("seq") * coarse_rows
    query_index = my_first + jnp.arange(coarse_rows, dtype=jnp.int32)
    initial = (
        jnp.full((local_heads, coarse_rows), big_negative, jnp.float32),
        jnp.zeros((local_heads, coarse_rows), jnp.float32),
        jnp.zeros((local_heads, coarse_rows, HEAD), jnp.float32),
    )
    piece = lax.all_gather(coarse_kv, "seq", axis=0, tiled=True)
    count = piece.shape[0]
    key_piece = piece[:, 0].reshape(count, local_heads, HEAD)
    value_piece = piece[:, 1].reshape(count, local_heads, HEAD)
    final = lax.cond(
        jnp.int32(0) < my_first + coarse_rows,
        lambda: online_update(initial, coarse_queries, key_piece, value_piece, query_index),
        lambda: initial,
    )
    head_out = final[2] / final[1][..., None]
    coarse_heads = (
        jnp.transpose(head_out, (1, 0, 2)).reshape(coarse_rows, local_cols).astype(jnp.bfloat16)
    )
    partials = jnp.dot(coarse_heads, coarse_out, preferred_element_type=jnp.float32)
    attended = lax.psum_scatter(
        partials.astype(jnp.bfloat16), "tp", scatter_dimension=1, tiled=True
    ).astype(jnp.float32)
    coarse_state = (short_cols.astype(jnp.float32) + attended).astype(jnp.bfloat16)
    prior_row = from_behind(coarse_state[coarse_rows - 1 :], "seq", 1)
    delayed = jnp.concatenate([prior_row, coarse_state[: coarse_rows - 1]], 0)
    lifted = lax.psum_scatter(
        jnp.dot(delayed, up_weight, preferred_element_type=jnp.float32).astype(jnp.bfloat16),
        "tp",
        scatter_dimension=0,
        tiled=True,
    ).astype(jnp.float32)
    result = fine_state.astype(jnp.float32) + jnp.repeat(lifted, SHORT, axis=0)
    return result.astype(jnp.bfloat16)


def flip(index, bit):
    return index + bit - 2 * bit * lax.rem(lax.div(index, jnp.int32(bit)), jnp.int32(2))


def bits_of(size):
    out, bit = [], size // 2
    while bit:
        out.append(bit)
        bit //= 2
    return out


def dot32(left, right):
    return jnp.dot(left, right, preferred_element_type=jnp.float32)


def dot_t(left, right):
    return lax.dot_general(
        left, right, (((1,), (1,)), ((), ())), preferred_element_type=jnp.float32
    )


PLAN = (
    (("down", 0), ("qk", 4)),
    (("v", 3), ("v", 1), ("v", 2), ("qk", 6), ("qk", 1)),
    (),
    (("down", 1),),
    (("qk", 5), ("qk", 2), ("down", 2)),
    (("down", 3),),
    (("qk", 7), ("qk", 3)),
    (),
)


def section_kernel(
    seq, tp,
    tokens, fine_gain, fine_query, fine_keyval, fine_out, down_weight, coarse_gain, coarse_query,
    coarse_kv, coarse_out, up_weight,
    result,
    both, wq, wkv, wo, down_own, down_g, wqk, wv, wout, wup,
    normed, queries, key_rows, local, fine_state, pooled_all, mv, pv_out, pv_in, mixed_qk,
    mixed_v, qkv, factors, shifted, heads_out, heads_in, coarse_heads, short_cols, lift,
    ss_tp, ss_seq, send1, recv1, state, send2, recv2,
    load_sem, halo_s, halo_r, qk_s, qk_r, v_s, v_r, d_s, d_r, pa_s, pa_r, pb_s, pb_r, pc_s, pc_r,
    ssa_s, ssa_r, ssb_s, ssb_r, pv_s, pv_r, h_s, h_r, r1_s, r1_r, r2_s, r2_r,
):
    me_s = lax.axis_index("seq")
    me_t = lax.axis_index("tp")
    rows, width = tokens.shape
    scale = 1.0 / math.sqrt(HEAD)
    total = seq * tp
    lin = me_s * tp + me_t
    after = lax.rem(lin + 1, total)
    before = lax.rem(lin + total - 1, total)
    bf, f32 = jnp.bfloat16, jnp.float32

    def around(index, step, size):
        return lax.rem(index + step, size)

    def toggle(index, mask):
        bit = 1
        while bit <= mask:
            if mask & bit:
                index = flip(index, bit)
            bit *= 2
        return index

    def remote(src, dst, send, recv, device):
        copy = pltpu.make_async_remote_copy(
            src_ref=src, dst_ref=dst, send_sem=send, recv_sem=recv,
            device_id=device, device_id_type=pl.DeviceIdType.MESH,
        )
        copy.start()
        return copy

    def load(src, dst, sem):
        copy = pltpu.make_async_copy(src, dst, sem)
        copy.start()
        return copy

    def arrived(dst, sem):
        pltpu.make_async_copy(dst, dst, sem).wait()

    def linear(index):
        return {"seq": lax.div(index, tp), "tp": lax.rem(index, tp)}

    depth = coarse_query.shape[0]
    own = coarse_query.shape[1] // seq
    fcols = down_own.shape[1]
    half = seq // 2
    zh = lax.div(me_s, half)
    in_half = lax.rem(me_s, half)
    partner = flip(me_s, half)
    pool_rows = rows // SHORT
    crows = pool_rows * tp
    count = crows * seq
    tile = 2 * HEAD

    def head_cols(dest):
        return pl.ds(pl.multiple_of(dest * own, own), own)

    def block_of(source):
        return pl.ds(pl.multiple_of(source * depth, depth), depth)

    barrier = pltpu.get_barrier_semaphore()
    peers = [{"seq": around(me_s, d, seq)} for d in range(1, seq)]
    peers += [{"tp": around(me_t, d, tp)} for d in range(1, tp)]
    peers += [linear(after), linear(before)]
    in_tokens = load(tokens, both.at[pl.ds(rows, rows)], load_sem.at[0])
    in_down = load(down_weight, down_own, load_sem.at[4])
    in_wq = load(fine_query, wq, load_sem.at[2])
    in_wkv = load(fine_keyval, wkv, load_sem.at[1])
    in_wo = load(fine_out, wo, load_sem.at[3])
    for pl_part, source in ((0, coarse_query), (1, coarse_kv.at[0])):
        load(source.at[:, head_cols(me_s)], wqk.at[block_of(me_s), pl.ds(pl_part * own, own)],
             qk_r.at[me_s])
    for k, head in enumerate((partner, me_s)):
        load(coarse_kv.at[1, :, head_cols(head)], wv.at[block_of(in_half), pl.ds(k * own, own)],
             v_r.at[in_half])
    in_wout = load(coarse_out, wout, load_sem.at[5])
    in_wup = load(up_weight, wup, load_sem.at[6])
    for peer in peers:
        pl.semaphore_signal(barrier, inc=1, device_id=peer, device_id_type=pl.DeviceIdType.MESH)
    pl.semaphore_wait(barrier, len(peers))

    sent = []
    halo = remote(tokens, both.at[pl.ds(0, rows)], halo_s, halo_r, linear(after))

    def send_qk(offsets):
        for d in offsets:
            dest = toggle(me_s, d)
            for k, source in enumerate((coarse_query, coarse_kv.at[0])):
                sent.append(
                    remote(
                        source.at[:, head_cols(dest)], wqk.at[block_of(me_s), pl.ds(k * own, own)],
                        qk_s.at[2 * (d - 1) + k], qk_r.at[me_s], {"seq": dest},
                    )
                )

    def send_v(offsets):
        for d in offsets:
            dest = toggle(me_s, d)
            for k, head in enumerate((flip(dest, half), dest)):
                sent.append(
                    remote(
                        coarse_kv.at[1, :, head_cols(head)],
                        wv.at[block_of(in_half), pl.ds(k * own, own)],
                        v_s.at[2 * (d - 1) + k], v_r.at[in_half], {"seq": dest},
                    )
                )

    tp_bits = bits_of(tp)
    pieces = 4
    span = width // pieces
    in_down.wait()
    cgain = coarse_gain[:, pl.ds(pl.multiple_of(me_t * fcols, fcols), fcols)]

    def slot_cols(slot):
        return pl.ds(pl.multiple_of(slot * fcols, fcols), fcols)

    def down_piece(slot, bit, number, r):
        part = down_g.at[pl.ds(r * span, span), slot_cols(slot)]
        at = number * pieces + r
        return remote(part, part, d_s.at[at], d_r.at[at], {"tp": flip(me_t, bit)})

    direct = {}

    def launch_down(r):
        at = pl.ds(r * span, span)
        down_g[at, slot_cols(me_t)] = (down_own[at, :].astype(f32) * cgain).astype(bf)
        for bit in tp_bits:
            direct[r, bit] = down_piece(me_t, bit, bit - 1, r)

    def forward_down(r):
        direct[r, tp_bits[0]].wait_recv()
        for bit in tp_bits[1:]:
            if bit != tp_bits[1]:
                for copy in later[r]:
                    copy.wait_recv()
            later.setdefault(r, []).extend(
                down_piece(toggle(me_t, sub), bit, bit + sub - 1, r)
                for sub in range(2 * bit, tp, 2 * bit)
            )
            later[r].append(direct[r, bit])

    later = {}

    def finish_down(r):
        for copy in later[r]:
            copy.wait_recv()
        sent.extend(later[r] + [direct[r, tp_bits[0]]])

    plan = PLAN
    if sum(len(stage) for stage in PLAN) != seq - 1 + half - 1 + pieces:
        plan = [[("qk", d) for d in range(1, seq)] + [("v", d) for d in range(1, half)]]
        plan[0] += [("down", r) for r in range(pieces)]

    def issue(stage):
        for kind, d in plan[stage] if stage < len(plan) else ():
            if kind == "qk":
                send_qk([d])
            elif kind == "v":
                send_v([d])
            else:
                launch_down(d)

    issue(0)

    gain = fine_gain[...]

    def norm_rows(first):
        values = both[pl.ds(first, rows), :].astype(f32)
        normed[pl.ds(first, rows), :] = normalize(values, gain).astype(bf)

    in_tokens.wait()
    norm_rows(rows)
    in_wq.wait()

    @pl.loop(0, width // tile)
    def _(i):
        cols = pl.ds(pl.multiple_of(i * tile, tile), tile)
        queries[:, cols] = dot32(normed[rows:, :], wq[:, cols]).astype(bf)

    in_wkv.wait()

    def project_rows(first):
        @pl.loop(0, 2 * width // tile)
        def _(i):
            cols = pl.ds(pl.multiple_of(i * tile, tile), tile)
            key_rows[pl.ds(first, rows), cols] = dot32(
                normed[pl.ds(first, rows), :], wkv[:, cols]
            ).astype(bf)

    project_rows(rows)
    issue(1)
    halo.wait_recv()
    sent.append(halo)
    norm_rows(0)
    project_rows(0)
    issue(2)

    row_index = lax.broadcasted_iota(jnp.int32, (rows, 2 * rows), 0)
    col_index = lax.broadcasted_iota(jnp.int32, (rows, 2 * rows), 1)
    offset = row_index + rows - col_index
    allowed = (offset >= 0) & (offset < WINDOW) & (lin * rows - rows + col_index >= 0)

    def weigh(query, key, mask):
        scores = jnp.where(mask, dot_t(query, key) * scale, big_negative)
        peak = jnp.max(scores, axis=-1, keepdims=True)
        weights = jnp.where(mask, jnp.exp(scores - peak), 0.0)
        return weights.astype(bf), jnp.sum(weights, axis=-1, keepdims=True)

    @pl.loop(0, width // HEAD)
    def _(h):
        cols = pl.ds(pl.multiple_of(h * HEAD, HEAD), HEAD)
        vcols = pl.ds(pl.multiple_of(width + h * HEAD, HEAD), HEAD)
        weights, denom = weigh(queries[:, cols], key_rows[:, cols], allowed)
        local[:, cols] = (dot32(weights, key_rows[:, vcols]) / denom).astype(bf)

    in_wo.wait()

    @pl.loop(0, width // tile)
    def _(i):
        cols = pl.ds(pl.multiple_of(i * tile, tile), tile)
        value = both[rows:, cols].astype(f32) + dot32(local[...], wo[:, cols])
        value = value.astype(bf)
        fine_state[:, cols] = value
        mean = jnp.mean(value.astype(f32).reshape(pool_rows, SHORT, tile), axis=1)
        pooled_all[lin, :, cols] = mean.astype(bf)

    group = []
    for d in range(1, tp):
        slot = pooled_all.at[lin]
        group.append(remote(slot, slot, pa_s.at[d - 1], pa_r.at[d - 1], {"tp": toggle(me_t, d)}))
    issue(3)
    for copy in group:
        copy.wait_recv()
    sent.extend(group)

    core_bit = tp_bits[-1]
    share = tp // 2
    mine_first = lax.rem(me_t, 2) * share

    def blocks(first_s, offset_t):
        return pooled_all.at[pl.ds(first_s * tp + offset_t, share)]

    seq_bits = bits_of(seq)
    gather = {}

    def spread_block(mask):
        for bit in seq_bits:
            if mask == 0 or bit < (mask & -mask):
                part = blocks(toggle(me_s, mask), mine_first)
                at = (mask | bit) - 1
                gather[at + 1] = remote(
                    part, part, pb_s.at[at], pb_r.at[at], {"seq": flip(me_s, bit)}
                )

    spread_block(0)
    issue(4)

    mine = pooled_all[pl.ds(me_s * tp, tp)].reshape(crows, width)
    square_sum = jnp.zeros((8, crows), f32)
    for u in range(2):
        cols = slice(u * fcols // 2, (u + 1) * fcols // 2)
        wide = dot32(mine, down_own[:, cols]).astype(bf).astype(f32)
        short_cols[pl.ds(0, crows), cols] = wide
        square_sum += lax.dot_general(
            jnp.ones((8, fcols // 2), f32), wide * wide, (((1,), (1,)), ((), ())),
            preferred_element_type=f32, precision=lax.Precision.HIGHEST,
        )
    ss_tp[me_t] = square_sum
    group = []
    for d in range(1, tp):
        slot = ss_tp.at[me_t]
        group.append(remote(slot, slot, ssa_s.at[d - 1], ssa_r.at[d - 1], {"tp": toggle(me_t, d)}))
    evens = sorted(range(2, seq, 2), key=lambda m: (bin(m).count("1"), m))
    for at, mask in enumerate(evens):
        gather[mask].wait_recv()
        spread_block(mask)
        issue(5 + at)

    for piece in range(pieces):
        forward_down(piece)
    for copy in group:
        copy.wait_recv()
    sent.extend(group)
    whole_sum = ss_tp[0]
    for t in range(1, tp):
        whole_sum += ss_tp[t]
    ss_seq[me_s] = whole_sum
    ss_copies = []
    for d in range(1, seq):
        slot = ss_seq.at[me_s]
        ss_copies.append(
            remote(slot, slot, ssb_s.at[d - 1], ssb_r.at[d - 1], {"seq": toggle(me_s, d)})
        )
    sent.extend(ss_copies)
    for hs in range(half):
        arrived(wv.at[pl.ds(hs * depth, depth)], v_r.at[hs])
    half_cols = pl.ds(pl.multiple_of(zh * half * depth, half * depth), half * depth)
    pv_copies = []
    for piece in range(pieces):
        finish_down(piece)
        at = slice(piece * span, (piece + 1) * span)
        product = dot32(down_g[at, half_cols], wv[...])
        pv_out[at, :] = product[:, :own].astype(bf)
        mv[at, :] = product[:, own:]
        at = pl.ds(piece * span, span)
        pv_copies.append(
            remote(pv_out.at[at], pv_in.at[at], pv_s.at[piece], pv_r.at[piece], {"seq": partner})
        )
    sent.extend(pv_copies)
    for mask in range(1, seq, 2):
        gather[mask].wait_recv()
    sent.extend(gather.values())
    pending = []
    for k in range(seq - 1):
        part = blocks(toggle(me_s, k + 1), mine_first)
        pending.append(
            remote(part, part, pc_s.at[k], pc_r.at[k], {"tp": flip(me_t, core_bit)})
        )
    for copy in pending:
        copy.wait_recv()
    sent.extend(pending)

    for source in range(seq):
        arrived(wqk.at[pl.ds(source * depth, depth)], qk_r.at[source])

    @pl.loop(0, pieces)
    def _(i):
        at = pl.ds(pl.multiple_of(i * span, span), span)
        mixed_qk[at, :] = dot32(down_g[at, :], wqk[...]).astype(bf)

    for copy in ss_copies:
        copy.wait_recv()
    sums = jnp.concatenate([ss_seq[s, 0:1, :] for s in range(seq)], 0)
    inverse = lax.rsqrt(sums / (tp * fcols) + epsilon)
    turned = jnp.transpose(jnp.concatenate([inverse] * (crows // seq), 0))
    for s in range(seq):
        factors[s * crows : (s + 1) * crows, :] = jnp.broadcast_to(
            turned[:, s : s + 1], (crows, HEAD)
        )
    block = 2 * crows

    def project(columns, mixed):
        @pl.loop(0, seq // 2)
        def _(i):
            at = pl.ds(pl.multiple_of(i * block, block), block)
            pooled = pooled_all[pl.ds(i * 2 * tp, 2 * tp)].reshape(block, width)
            product = dot32(pooled, mixed[...])
            for c in range(product.shape[1] // HEAD):
                part = product[:, c * HEAD : (c + 1) * HEAD] * factors[at, :]
                first = columns + c * HEAD
                qkv[at, first : first + HEAD] = part.astype(bf)

    project(0, mixed_qk)

    earlier = pooled_all[before_slot(me_s, tp, total), pool_rows - 16 :, :]
    for u in range(2):
        cols = slice(u * fcols // 2, (u + 1) * fcols // 2)
        last = dot32(earlier, down_own[:, cols]).astype(bf).astype(f32)[15:16, :]
        last = jnp.where(me_s > 0, last, 0.0)
        rolled = pltpu.roll(short_cols[pl.ds(0, crows), cols], 1, 0)
        top = lax.broadcasted_iota(jnp.int32, rolled.shape, 0) == 0
        short_cols[pl.ds(0, crows), cols] = jnp.where(top, last, rolled)

    for copy in pv_copies:
        copy.wait_recv()
    mixed_v[...] = (mv[...] + pv_in[...].astype(f32)).astype(bf)
    project(2 * own, mixed_v)
    shifted[0:1, :] = jnp.zeros((1, own), f32)

    def heads_copy(index):
        return pltpu.make_async_remote_copy(
            src_ref=heads_out.at[index], dst_ref=heads_in.at[me_s], send_sem=h_s.at[index],
            recv_sem=h_r.at[me_s], device_id={"seq": index}, device_id_type=pl.DeviceIdType.MESH,
        )

    for i in range(seq // 2):
        extent = (i + 1) * block
        r = lax.broadcasted_iota(jnp.int32, (block, extent), 0) + i * block
        c = lax.broadcasted_iota(jnp.int32, (block, extent), 1)
        for h in range(own // HEAD):
            part = slice(h * HEAD, (h + 1) * HEAD)
            kpart = slice(own + h * HEAD, own + (h + 1) * HEAD)
            vpart = slice(2 * own + h * HEAD, 2 * own + (h + 1) * HEAD)
            weights, denom = weigh(qkv[i * block : extent, part], qkv[:extent, kpart], c <= r)
            out = dot32(weights, qkv[:extent, vpart]) / denom
            shifted[i * block + 1 : extent + 1, part] = out
        for index in (2 * i, 2 * i + 1):
            heads_out[index] = shifted[index * crows : (index + 1) * crows, :].astype(bf)

            @pl.when(me_s != index)
            def _(index=index):
                heads_copy(index).start()

    heads_in[me_s] = heads_out[me_s]
    in_wout.wait()
    in_wup.wait()
    for j in range(seq):

        @pl.when(me_s != j)
        def _(j=j):
            arrived(heads_in.at[j], h_r.at[j])

        coarse_heads[:, j * own : (j + 1) * own] = heads_in[j]

    sides = 2
    side = fcols // sides

    def partial(t, u, store):
        @pl.loop(0, side // tile)
        def _(i):
            cols = pl.ds(pl.multiple_of(u * side + i * tile, tile), tile)
            wcols = pl.ds(pl.multiple_of(t * fcols + u * side + i * tile, tile), tile)
            store(cols, dot32(coarse_heads[...], wout[:, wcols]))

    r1 = {}
    for sub in range(tp - 1, 0, -1):
        bit = sub & -sub
        lows = [low for low in tp_bits if low < bit]
        for u in range(sides):
            ucols = pl.ds(u * side, side)
            for low in lows:
                r1[sub + low, u].wait_recv()

            def put(cols, value, sub=sub, lows=lows):
                for low in lows:
                    value += recv1[sub + low - 1, :, cols].astype(f32)
                send1[sub - 1, :, cols] = value.astype(bf)

            partial(toggle(me_t, sub), u, put)
            at = (sub - 1) * sides + u
            r1[sub, u] = remote(
                send1.at[sub - 1, :, ucols], recv1.at[sub - 1, :, ucols], r1_s.at[at], r1_r.at[at],
                {"tp": flip(me_t, bit)},
            )
    sent.extend(r1.values())

    def keep(cols, value):
        short_cols[:, cols] += value

    for u in range(sides):
        partial(me_t, u, keep)
    tp_order = sorted(range(1, tp), key=lambda d: abs(2 * d - tp))
    r2 = []
    for u in range(sides):
        ucols = slice(u * side, (u + 1) * side)
        for bit in tp_bits:
            r1[bit, u].wait_recv()
        whole = short_cols[:, ucols]
        for bit in tp_bits:
            whole += recv1[bit - 1, :, ucols].astype(f32)
        top = lax.broadcasted_iota(jnp.int32, whole.shape, 0) == 0
        state[:, ucols] = jnp.where(top & (me_s == 0), 0.0, whole).astype(bf)
        for w in range(sides):
            wcols = slice(w * width // sides, (w + 1) * width // sides)
            product = dot32(state[:, ucols], wup[ucols, wcols])
            if u:
                product += lift[:, wcols]
            lift[:, wcols] = product
            if u == sides - 1:
                for d in tp_order:
                    dest = around(me_t, d, tp)
                    some = pl.ds(pl.multiple_of(dest * pool_rows, pool_rows), pool_rows)
                    at = (d - 1) * sides + w
                    send2[at] = lift[some, wcols].astype(bf)
                    r2.append(
                        remote(
                            send2.at[at], recv2.at[at], r2_s.at[at], r2_r.at[at], {"tp": dest}
                        )
                    )
    sent.extend(r2)
    for w in range(sides):
        wcols = slice(w * width // sides, (w + 1) * width // sides)
        for copy in r2[w * (tp - 1) : (w + 1) * (tp - 1)]:
            copy.wait_recv()
        lifted = lift[pl.ds(pl.multiple_of(me_t * pool_rows, pool_rows), pool_rows), wcols]
        for d in range(1, tp):
            lifted += recv2[(d - 1) * sides + w].astype(f32)
        spread = jnp.broadcast_to(lifted[:, None, :], (pool_rows, SHORT, width // sides))
        spread = spread.reshape(rows, width // sides)
        result[:, wcols] = (fine_state[:, wcols].astype(f32) + spread).astype(bf)
    for index in range(seq):

        @pl.when(me_s != index)
        def _(index=index):
            heads_copy(index).wait_send()

    for copy in sent:
        copy.wait_send()


def before_slot(me_s, tp, total):
    return lax.rem(me_s * tp + total - 1, total)


def head_body(
    tokens,
    fine_gain,
    fine_query,
    fine_keyval,
    fine_out,
    down_weight,
    coarse_gain,
    coarse_query,
    coarse_keyval,
    coarse_out,
    up_weight,
):
    seq, tp = lax.axis_size("seq"), lax.axis_size("tp")
    rows, width = tokens.shape
    depth, local_cols = coarse_query.shape
    own = local_cols // seq
    half = seq // 2
    pool_rows = rows // SHORT
    crows = pool_rows * tp
    count = crows * seq
    bf, f32 = jnp.bfloat16, jnp.float32
    V = pltpu.VMEM
    dma = lambda n: pltpu.SemaphoreType.DMA((n,))
    one = pltpu.SemaphoreType.DMA
    anywhere = pl.BlockSpec(memory_space=pl.ANY)
    vmem = pl.BlockSpec(memory_space=pltpu.VMEM)
    return pl.pallas_call(
        functools.partial(section_kernel, seq, tp),
        out_shape=jax.ShapeDtypeStruct((rows, width), bf),
        in_specs=[anywhere, vmem, anywhere, anywhere, anywhere, anywhere, vmem, anywhere,
                  anywhere, anywhere, anywhere],
        out_specs=vmem,
        scratch_shapes=[
            V((2 * rows, width), bf), V(fine_query.shape, bf), V(fine_keyval.shape, bf),
            V(fine_out.shape, bf), V(down_weight.shape, bf), V((width, seq * depth), bf),
            V((seq * depth, 2 * own), bf), V((half * depth, 2 * own), bf),
            V(coarse_out.shape, bf), V(up_weight.shape, bf),
            V((2 * rows, width), bf), V((rows, width), bf), V((2 * rows, 2 * width), bf),
            V((rows, width), bf), V((rows, width), bf), V((seq * tp, pool_rows, width), bf),
            V((width, own), f32), V((width, own), bf),
            V((width, own), bf), V((width, 2 * own), bf), V((width, own), bf),
            V((count, 3 * own), bf), V((count, HEAD), f32),
            V((count + 8, own), f32), V((seq, crows, own), bf), V((seq, crows, own), bf),
            V((crows, local_cols), bf), V((crows, local_cols), f32), V((crows, width), f32),
            V((tp, 8, crows), f32), V((seq, 8, crows), f32),
            V((tp - 1, crows, local_cols), bf), V((tp - 1, crows, local_cols), bf),
            V((crows, local_cols), bf),
            V((2 * (tp - 1), pool_rows, width // 2), bf), V((2 * (tp - 1), pool_rows, width // 2), bf),
            dma(7), one(()), one(()), dma(2 * (seq - 1)), dma(seq), dma(2 * (half - 1)), dma(half),
            dma(4 * (tp - 1)), dma(4 * (tp - 1)), dma(tp - 1), dma(tp - 1),
            dma(seq - 1), dma(seq - 1), dma(seq - 1), dma(seq - 1),
            dma(tp - 1), dma(tp - 1), dma(seq - 1), dma(seq - 1), dma(4), dma(4),
            dma(seq), dma(seq), dma(2 * (tp - 1)), dma(2 * (tp - 1)), dma(2 * (tp - 1)),
            dma(2 * (tp - 1)),
        ],
        compiler_params=pltpu.CompilerParams(
            collective_id=0, has_side_effects=True, vmem_limit_bytes=62 * 1024 * 1024
        ),
    )(tokens, fine_gain[None], fine_query, fine_keyval, fine_out, down_weight, coarse_gain[None],
      coarse_query, jnp.transpose(coarse_keyval, (1, 0, 2)), coarse_out, up_weight)


def chosen(*args):
    seq, tp = lax.axis_size("seq"), lax.axis_size("tp")
    local_heads = args[7].shape[1] // HEAD
    powers = seq & (seq - 1) == 0 and tp & (tp - 1) == 0 and seq > 1 and tp > 1
    square = args[10].shape[0] == args[10].shape[1] == args[7].shape[1]
    paired = seq % tp == 0 and seq > 2 and args[7].shape[0] * (seq // tp) == args[7].shape[1]
    paired = paired and args[0].shape[0] // SHORT * tp == HEAD
    if local_heads % seq == 0 and args[0].shape[0] == WINDOW and powers and square and paired:
        return head_body(*args)
    return body(*args)


def solution(mesh):
    return jax.shard_map(
        chosen,
        mesh=mesh,
        in_specs=(
            P(("seq", "tp"), None),
            P(),
            P(),
            P(),
            P(),
            P(None, "tp"),
            P(),
            P("seq", "tp"),
            P("seq", None, "tp"),
            P("tp", None),
            P("tp", None),
        ),
        out_specs=P(("seq", "tp"), None),
        check_vma=False,
    )
```

```python
import functools
import math

import jax
import jax.numpy as jnp
from jax import lax
from jax.experimental import pallas as pl
from jax.experimental.pallas import tpu as pltpu
from jax.sharding import PartitionSpec as P

HEAD = 128
WINDOW = 256
SHORT = 8


epsilon = 1e-06
big_negative = -1e30


def from_behind(array, axis, by):
    size = lax.axis_size(axis)
    pairs = [(i, i + by) for i in range(size) if 0 <= i + by < size]
    return lax.ppermute(array, axis, pairs)


def normalize(values, scale_gain):
    mean_square = jnp.mean(values * values, axis=-1, keepdims=True)
    return values * lax.rsqrt(mean_square + epsilon) * scale_gain


def online_update(state, query_heads, key_piece, value_piece, query_index):
    running_max, running_sum, accumulate = state
    scale = 1.0 / math.sqrt(HEAD)
    scores = (
        jnp.einsum("qhd,khd->hqk", query_heads, key_piece, preferred_element_type=jnp.float32)
        * scale
    )
    key_index = jnp.arange(key_piece.shape[0], dtype=jnp.int32)
    allowed = key_index[None, :] <= query_index[:, None]
    scores = jnp.where(allowed[None], scores, big_negative)
    new_max = jnp.maximum(running_max, jnp.max(scores, axis=-1))
    terms = jnp.where(allowed[None], jnp.exp(scores - new_max[..., None]), 0.0)
    new_sum = jnp.sum(terms, axis=-1)
    product = jnp.einsum(
        "hqk,khd->hqd", terms.astype(jnp.bfloat16), value_piece, preferred_element_type=jnp.float32
    )
    return (new_max, new_sum, product)


def body(
    tokens,
    fine_gain,
    fine_query,
    fine_keyval,
    fine_out,
    down_weight,
    coarse_gain,
    coarse_query,
    coarse_keyval,
    coarse_out,
    up_weight,
):
    tok_rows = tokens.shape[0]
    width = tokens.shape[1]
    fine_heads = width // HEAD
    scale = 1.0 / math.sqrt(HEAD)
    start_row = lax.axis_index(("seq", "tp")) * tok_rows
    inputs = tokens.astype(jnp.float32)
    normed = normalize(inputs, fine_gain).astype(jnp.bfloat16)
    queries = jnp.dot(normed, fine_query, preferred_element_type=jnp.float32).astype(jnp.bfloat16)
    keyvals = jnp.dot(normed, fine_keyval, preferred_element_type=jnp.float32).astype(jnp.bfloat16)
    earlier = from_behind(keyvals, ("seq", "tp"), 1)
    key_rows = jnp.concatenate([earlier, keyvals], 0)
    span = key_rows.shape[0]
    key_heads = key_rows[:, :width].reshape(span, fine_heads, HEAD)
    value_heads = key_rows[:, width:].reshape(span, fine_heads, HEAD)
    query_heads = queries.reshape(tok_rows, fine_heads, HEAD)
    scores = (
        jnp.einsum("qhd,khd->hqk", query_heads, key_heads, preferred_element_type=jnp.float32)
        * scale
    )
    row_index = jnp.arange(tok_rows, dtype=jnp.int32)[:, None]
    col_index = jnp.arange(span, dtype=jnp.int32)[None, :]
    offset = row_index + WINDOW - col_index
    allowed = (offset >= 0) & (offset < WINDOW) & (start_row - WINDOW + col_index >= 0)
    scores = jnp.where(allowed[None], scores, big_negative)
    peak = jnp.max(scores, axis=-1, keepdims=True)
    terms = jnp.where(allowed[None], jnp.exp(scores - peak), 0.0)
    denom = jnp.sum(terms, axis=-1)
    mixed = jnp.einsum(
        "hqk,khd->qhd", terms.astype(jnp.bfloat16), value_heads, preferred_element_type=jnp.float32
    )
    local = (mixed / jnp.transpose(denom)[..., None]).reshape(tok_rows, width).astype(jnp.bfloat16)
    fine_state = (inputs + jnp.dot(local, fine_out, preferred_element_type=jnp.float32)).astype(
        jnp.bfloat16
    )
    pooled = jnp.mean(
        fine_state.astype(jnp.float32).reshape(tok_rows // SHORT, SHORT, width), axis=1
    ).astype(jnp.bfloat16)
    pooled_all = lax.all_gather(pooled, "tp", axis=0, tiled=True)
    short_cols = jnp.dot(pooled_all, down_weight, preferred_element_type=jnp.float32).astype(
        jnp.bfloat16
    )
    shortened = lax.all_gather(short_cols, "tp", axis=1, tiled=True)
    coarse_normed = normalize(shortened.astype(jnp.float32), coarse_gain).astype(jnp.bfloat16)
    coarse_rows = coarse_normed.shape[0]
    local_cols = coarse_query.shape[1]
    local_heads = local_cols // HEAD
    query_rows = lax.all_gather(coarse_query, "seq", axis=0, tiled=True)
    keyval_rows = lax.all_gather(coarse_keyval, "seq", axis=0, tiled=True)
    count = query_rows.shape[0]
    query_sum = jnp.dot(coarse_normed, query_rows, preferred_element_type=jnp.float32)
    keyval_sum = jnp.dot(
        coarse_normed,
        keyval_rows.reshape(count, 2 * local_cols),
        preferred_element_type=jnp.float32,
    )
    coarse_queries = query_sum.astype(jnp.bfloat16).reshape(coarse_rows, local_heads, HEAD)
    coarse_kv = keyval_sum.astype(jnp.bfloat16).reshape(coarse_rows, 2, local_cols)
    my_first = lax.axis_index("seq") * coarse_rows
    query_index = my_first + jnp.arange(coarse_rows, dtype=jnp.int32)
    initial = (
        jnp.full((local_heads, coarse_rows), big_negative, jnp.float32),
        jnp.zeros((local_heads, coarse_rows), jnp.float32),
        jnp.zeros((local_heads, coarse_rows, HEAD), jnp.float32),
    )
    piece = lax.all_gather(coarse_kv, "seq", axis=0, tiled=True)
    count = piece.shape[0]
    key_piece = piece[:, 0].reshape(count, local_heads, HEAD)
    value_piece = piece[:, 1].reshape(count, local_heads, HEAD)
    final = lax.cond(
        jnp.int32(0) < my_first + coarse_rows,
        lambda: online_update(initial, coarse_queries, key_piece, value_piece, query_index),
        lambda: initial,
    )
    head_out = final[2] / final[1][..., None]
    coarse_heads = (
        jnp.transpose(head_out, (1, 0, 2)).reshape(coarse_rows, local_cols).astype(jnp.bfloat16)
    )
    partials = jnp.dot(coarse_heads, coarse_out, preferred_element_type=jnp.float32)
    attended = lax.psum_scatter(
        partials.astype(jnp.bfloat16), "tp", scatter_dimension=1, tiled=True
    ).astype(jnp.float32)
    coarse_state = (short_cols.astype(jnp.float32) + attended).astype(jnp.bfloat16)
    prior_row = from_behind(coarse_state[coarse_rows - 1 :], "seq", 1)
    delayed = jnp.concatenate([prior_row, coarse_state[: coarse_rows - 1]], 0)
    lifted = lax.psum_scatter(
        jnp.dot(delayed, up_weight, preferred_element_type=jnp.float32).astype(jnp.bfloat16),
        "tp",
        scatter_dimension=0,
        tiled=True,
    ).astype(jnp.float32)
    result = fine_state.astype(jnp.float32) + jnp.repeat(lifted, SHORT, axis=0)
    return result.astype(jnp.bfloat16)


def flip(index, bit):
    return index + bit - 2 * bit * lax.rem(lax.div(index, jnp.int32(bit)), jnp.int32(2))


def bits_of(size):
    out, bit = [], size // 2
    while bit:
        out.append(bit)
        bit //= 2
    return out


def dot32(left, right):
    return jnp.dot(left, right, preferred_element_type=jnp.float32)


def dot_t(left, right):
    return lax.dot_general(
        left, right, (((1,), (1,)), ((), ())), preferred_element_type=jnp.float32
    )


PLAN = (
    (("down", 0), ("qk", 4)),
    (("v", 3), ("v", 1), ("v", 2), ("qk", 6), ("qk", 1)),
    (),
    (("down", 1),),
    (("qk", 5), ("qk", 2)),
    (("down", 2),),
    (("down", 3),),
    (("qk", 7), ("qk", 3)),
    (),
)


def section_kernel(
    seq, tp,
    tokens, fine_gain, fine_query, fine_keyval, fine_out, down_weight, coarse_gain, coarse_query,
    coarse_kv, coarse_out, up_weight,
    result,
    kv_raw, kv, both, wq, wkv, wo, down_own, down_g, wqk, wv, wout, wup,
    normed, queries, key_rows, local, fine_state, pooled_all, mv, pv_out, pv_in, mixed_qk,
    mixed_v, qkv, factors, shifted, heads_out, heads_in, coarse_heads, short_cols, lift,
    ss_tp, ss_seq, send1, recv1, state, send2, recv2,
    load_sem, halo_s, halo_r, qk_s, qk_r, v_s, v_r, d_s, d_r, pa_s, pa_r, pb_s, pb_r, pc_s, pc_r,
    ssa_s, ssa_r, ssb_s, ssb_r, pv_s, pv_r, h_s, h_r, r1_s, r1_r, r2_s, r2_r,
):
    me_s = lax.axis_index("seq")
    me_t = lax.axis_index("tp")
    rows, width = tokens.shape
    scale = 1.0 / math.sqrt(HEAD)
    total = seq * tp
    lin = me_s * tp + me_t
    after = lax.rem(lin + 1, total)
    before = lax.rem(lin + total - 1, total)
    bf, f32 = jnp.bfloat16, jnp.float32

    def around(index, step, size):
        return lax.rem(index + step, size)

    def toggle(index, mask):
        bit = 1
        while bit <= mask:
            if mask & bit:
                index = flip(index, bit)
            bit *= 2
        return index

    def remote(src, dst, send, recv, device):
        copy = pltpu.make_async_remote_copy(
            src_ref=src, dst_ref=dst, send_sem=send, recv_sem=recv,
            device_id=device, device_id_type=pl.DeviceIdType.MESH,
        )
        copy.start()
        return copy

    def load(src, dst, sem):
        copy = pltpu.make_async_copy(src, dst, sem)
        copy.start()
        return copy

    def arrived(dst, sem):
        pltpu.make_async_copy(dst, dst, sem).wait()

    def linear(index):
        return {"seq": lax.div(index, tp), "tp": lax.rem(index, tp)}

    depth = coarse_query.shape[0]
    own = coarse_query.shape[1] // seq
    fcols = down_own.shape[1]
    half = seq // 2
    zh = lax.div(me_s, half)
    in_half = lax.rem(me_s, half)
    partner = flip(me_s, half)
    pool_rows = rows // SHORT
    crows = pool_rows * tp
    count = crows * seq
    tile = 2 * HEAD

    def head_cols(dest):
        return pl.ds(pl.multiple_of(dest * own, own), own)

    def block_of(source):
        return pl.ds(pl.multiple_of(source * depth, depth), depth)

    barrier = pltpu.get_barrier_semaphore()
    peers = [{"seq": around(me_s, d, seq)} for d in range(1, seq)]
    peers += [{"tp": around(me_t, d, tp)} for d in range(1, tp)]
    peers += [linear(after), linear(before)]
    in_kv = load(coarse_kv, kv_raw, load_sem.at[5])
    in_down = load(down_weight, down_own, load_sem.at[4])
    in_tokens = load(tokens, both.at[pl.ds(rows, rows)], load_sem.at[0])
    load(coarse_query.at[:, head_cols(me_s)], wqk.at[block_of(me_s), pl.ds(0, own)], qk_r.at[me_s])
    for peer in peers:
        pl.semaphore_signal(barrier, inc=1, device_id=peer, device_id_type=pl.DeviceIdType.MESH)
    in_kv.wait()
    in_wq = load(fine_query, wq, load_sem.at[2])
    in_wkv = load(fine_keyval, wkv, load_sem.at[1])
    in_wo = load(fine_out, wo, load_sem.at[3])
    step = HEAD
    picks = []
    for k in range(2):
        r = lax.broadcasted_iota(jnp.int32, (step, 2 * step), 0)
        c = lax.broadcasted_iota(jnp.int32, (step, 2 * step), 1)
        picks.append((c == 2 * r + k).astype(bf))

    @pl.loop(0, depth // step, unroll=2)
    def _(i):
        at = pl.ds(pl.multiple_of(i * step, step), step)
        turns = kv_raw[at].reshape(2 * step, kv_raw.shape[2])
        for k in range(2):
            kv[k, at, :] = dot32(picks[k], turns).astype(bf)

    load(kv.at[0, :, head_cols(me_s)], wqk.at[block_of(me_s), pl.ds(own, own)], qk_r.at[me_s])
    for k, head in enumerate((partner, me_s)):
        load(kv.at[1, :, head_cols(head)], wv.at[block_of(in_half), pl.ds(k * own, own)],
             v_r.at[in_half])
    pl.semaphore_wait(barrier, len(peers))
    in_wout = load(coarse_out, wout, load_sem.at[6])
    in_wup = load(up_weight, wup, load_sem.at[7])

    sent = []
    halo = remote(tokens, both.at[pl.ds(0, rows)], halo_s, halo_r, linear(after))

    def send_qk(offsets):
        for d in offsets:
            dest = toggle(me_s, d)
            for k, source in enumerate((coarse_query, kv.at[0])):
                sent.append(
                    remote(
                        source.at[:, head_cols(dest)], wqk.at[block_of(me_s), pl.ds(k * own, own)],
                        qk_s.at[2 * (d - 1) + k], qk_r.at[me_s], {"seq": dest},
                    )
                )

    def send_v(offsets):
        for d in offsets:
            dest = toggle(me_s, d)
            for k, head in enumerate((flip(dest, half), dest)):
                sent.append(
                    remote(
                        kv.at[1, :, head_cols(head)],
                        wv.at[block_of(in_half), pl.ds(k * own, own)],
                        v_s.at[2 * (d - 1) + k], v_r.at[in_half], {"seq": dest},
                    )
                )

    tp_bits = bits_of(tp)
    pieces = 4
    span = width // pieces
    in_down.wait()
    cgain = coarse_gain[:, pl.ds(pl.multiple_of(me_t * fcols, fcols), fcols)]

    def slot_cols(slot):
        return pl.ds(pl.multiple_of(slot * fcols, fcols), fcols)

    def down_piece(slot, bit, number, r):
        part = down_g.at[pl.ds(r * span, span), slot_cols(slot)]
        at = number * pieces + r
        return remote(part, part, d_s.at[at], d_r.at[at], {"tp": flip(me_t, bit)})

    direct = {}

    def launch_down(r):
        at = pl.ds(r * span, span)
        down_g[at, slot_cols(me_t)] = (down_own[at, :].astype(f32) * cgain).astype(bf)
        for bit in tp_bits:
            direct[r, bit] = down_piece(me_t, bit, bit - 1, r)

    def forward_down(r):
        direct[r, tp_bits[0]].wait_recv()
        for bit in tp_bits[1:]:
            if bit != tp_bits[1]:
                for copy in later[r]:
                    copy.wait_recv()
            later.setdefault(r, []).extend(
                down_piece(toggle(me_t, sub), bit, bit + sub - 1, r)
                for sub in range(2 * bit, tp, 2 * bit)
            )
            later[r].append(direct[r, bit])

    later = {}

    def finish_down(r):
        for copy in later[r]:
            copy.wait_recv()
        sent.extend(later[r] + [direct[r, tp_bits[0]]])

    plan = PLAN
    if sum(len(stage) for stage in PLAN) != seq - 1 + half - 1 + pieces:
        plan = [[("qk", d) for d in range(1, seq)] + [("v", d) for d in range(1, half)]]
        plan[0] += [("down", r) for r in range(pieces)]

    def issue(stage):
        for kind, d in plan[stage] if stage < len(plan) else ():
            if kind == "qk":
                send_qk([d])
            elif kind == "v":
                send_v([d])
            else:
                launch_down(d)

    issue(0)

    gain = fine_gain[...]

    def norm_rows(first):
        values = both[pl.ds(first, rows), :].astype(f32)
        normed[pl.ds(first, rows), :] = normalize(values, gain).astype(bf)

    in_tokens.wait()
    norm_rows(rows)
    in_wq.wait()

    @pl.loop(0, width // tile)
    def _(i):
        cols = pl.ds(pl.multiple_of(i * tile, tile), tile)
        queries[:, cols] = dot32(normed[rows:, :], wq[:, cols]).astype(bf)

    in_wkv.wait()

    def project_rows(first):
        @pl.loop(0, 2 * width // tile)
        def _(i):
            cols = pl.ds(pl.multiple_of(i * tile, tile), tile)
            key_rows[pl.ds(first, rows), cols] = dot32(
                normed[pl.ds(first, rows), :], wkv[:, cols]
            ).astype(bf)

    project_rows(rows)
    issue(1)
    halo.wait_recv()
    sent.append(halo)
    norm_rows(0)
    project_rows(0)
    issue(2)

    own_side = lax.broadcasted_iota(jnp.int32, (rows, rows), 1) <= lax.broadcasted_iota(
        jnp.int32, (rows, rows), 0
    )
    bias = jnp.where(lin > 0, 0.0, big_negative)

    @pl.loop(0, width // HEAD, unroll=4)
    def _(h):
        cols = pl.ds(pl.multiple_of(h * HEAD, HEAD), HEAD)
        vcols = pl.ds(pl.multiple_of(width + h * HEAD, HEAD), HEAD)
        query = queries[:, cols]
        late = dot_t(query, key_rows[rows:, cols])
        early = dot_t(query, key_rows[:rows, cols]) + bias
        scores = jnp.where(own_side, late, early) * scale
        peak = jnp.max(scores, axis=-1, keepdims=True)
        weights = jnp.exp(scores - peak)
        denom = jnp.sum(weights, axis=-1, keepdims=True)
        late = jnp.where(own_side, weights, 0.0).astype(bf)
        early = jnp.where(own_side, 0.0, weights).astype(bf)
        out = dot32(late, key_rows[rows:, vcols]) + dot32(early, key_rows[:rows, vcols])
        local[:, cols] = (out / denom).astype(bf)

    in_wo.wait()

    @pl.loop(0, width // tile)
    def _(i):
        cols = pl.ds(pl.multiple_of(i * tile, tile), tile)
        value = both[rows:, cols].astype(f32) + dot32(local[...], wo[:, cols])
        value = value.astype(bf)
        fine_state[:, cols] = value
        mean = jnp.mean(value.astype(f32).reshape(pool_rows, SHORT, tile), axis=1)
        pooled_all[lin, :, cols] = mean.astype(bf)

    group = []
    for d in range(1, tp):
        slot = pooled_all.at[lin]
        group.append(remote(slot, slot, pa_s.at[d - 1], pa_r.at[d - 1], {"tp": toggle(me_t, d)}))
    issue(3)
    for copy in group:
        copy.wait_recv()
    sent.extend(group)

    core_bit = tp_bits[-1]
    share = tp // 2
    mine_first = lax.rem(me_t, 2) * share

    def blocks(first_s, offset_t):
        return pooled_all.at[pl.ds(first_s * tp + offset_t, share)]

    seq_bits = bits_of(seq)
    gather = {}

    def spread_block(mask):
        for bit in seq_bits:
            if mask == 0 or bit < (mask & -mask):
                part = blocks(toggle(me_s, mask), mine_first)
                at = (mask | bit) - 1
                gather[at + 1] = remote(
                    part, part, pb_s.at[at], pb_r.at[at], {"seq": flip(me_s, bit)}
                )

    spread_block(0)
    issue(4)

    mine = pooled_all[pl.ds(me_s * tp, tp)].reshape(crows, width)
    square_sum = jnp.zeros((8, crows), f32)
    for u in range(2):
        cols = slice(u * fcols // 2, (u + 1) * fcols // 2)
        wide = dot32(mine, down_own[:, cols]).astype(bf).astype(f32)
        short_cols[pl.ds(0, crows), cols] = wide
        square_sum += lax.dot_general(
            jnp.ones((8, fcols // 2), f32), wide * wide, (((1,), (1,)), ((), ())),
            preferred_element_type=f32, precision=lax.Precision.HIGHEST,
        )
    ss_tp[me_t] = square_sum
    group = []
    for d in range(1, tp):
        slot = ss_tp.at[me_t]
        group.append(remote(slot, slot, ssa_s.at[d - 1], ssa_r.at[d - 1], {"tp": toggle(me_t, d)}))
    issue(5)
    ss_copies = []

    def gather_sums():
        for copy in group:
            copy.wait_recv()
        sent.extend(group)
        whole_sum = ss_tp[0]
        for t in range(1, tp):
            whole_sum += ss_tp[t]
        ss_seq[me_s] = whole_sum
        for d in range(1, seq):
            slot = ss_seq.at[me_s]
            ss_copies.append(
                remote(slot, slot, ssb_s.at[d - 1], ssb_r.at[d - 1], {"seq": toggle(me_s, d)})
            )
        sent.extend(ss_copies)

    half_cols = pl.ds(pl.multiple_of(zh * half * depth, half * depth), half * depth)
    pv_copies = []

    def v_piece(piece):
        finish_down(piece)
        at = slice(piece * span, (piece + 1) * span)
        product = dot32(down_g[at, half_cols], wv[...])
        pv_out[at, :] = product[:, :own].astype(bf)
        mv[at, :] = product[:, own:]
        at = pl.ds(piece * span, span)
        pv_copies.append(
            remote(pv_out.at[at], pv_in.at[at], pv_s.at[piece], pv_r.at[piece], {"seq": partner})
        )

    evens = sorted(range(2, seq, 2), key=lambda m: (bin(m).count("1"), m))
    for at, mask in enumerate(evens):
        gather[mask].wait_recv()
        spread_block(mask)
        if at == max(0, len(evens) - 2):
            gather_sums()
        issue(6 + at)
        if at == max(0, len(evens) - 2):
            for hs in range(half):
                arrived(wv.at[pl.ds(hs * depth, depth)], v_r.at[hs])
            for piece in range(pieces // 2):
                forward_down(piece)
            for piece in range(pieces // 2):
                v_piece(piece)
    for piece in range(pieces // 2, pieces):
        forward_down(piece)
        v_piece(piece)
    sent.extend(pv_copies)
    for mask in range(1, seq, 2):
        gather[mask].wait_recv()
    sent.extend(gather.values())
    pending = []
    for k in range(seq - 1):
        part = blocks(toggle(me_s, k + 1), mine_first)
        pending.append(
            remote(part, part, pc_s.at[k], pc_r.at[k], {"tp": flip(me_t, core_bit)})
        )
    for copy in pending:
        copy.wait_recv()
    sent.extend(pending)

    for copy in ss_copies:
        copy.wait_recv()
    sums = jnp.concatenate([ss_seq[s, 0:1, :] for s in range(seq)], 0)
    inverse = lax.rsqrt(sums / (tp * fcols) + epsilon)
    turned = jnp.transpose(jnp.concatenate([inverse] * (crows // seq), 0))
    for s in range(seq):
        factors[s * crows : (s + 1) * crows, :] = jnp.broadcast_to(
            turned[:, s : s + 1], (crows, HEAD)
        )

    earlier = pooled_all[before_slot(me_s, tp, total), pool_rows - 16 :, :]
    for u in range(2):
        cols = slice(u * fcols // 2, (u + 1) * fcols // 2)
        last = dot32(earlier, down_own[:, cols]).astype(bf).astype(f32)[15:16, :]
        last = jnp.where(me_s > 0, last, 0.0)
        rolled = pltpu.roll(short_cols[pl.ds(0, crows), cols], 1, 0)
        top = lax.broadcasted_iota(jnp.int32, rolled.shape, 0) == 0
        short_cols[pl.ds(0, crows), cols] = jnp.where(top, last, rolled)

    for source in range(seq):
        arrived(wqk.at[pl.ds(source * depth, depth)], qk_r.at[source])

    @pl.loop(0, pieces)
    def _(i):
        at = pl.ds(pl.multiple_of(i * span, span), span)
        mixed_qk[at, :] = dot32(down_g[at, :], wqk[...]).astype(bf)

    block = 2 * crows

    def project(columns, mixed):
        @pl.loop(0, seq // 2)
        def _(i):
            at = pl.ds(pl.multiple_of(i * block, block), block)
            pooled = pooled_all[pl.ds(i * 2 * tp, 2 * tp)].reshape(block, width)
            product = dot32(pooled, mixed[...])
            for c in range(product.shape[1] // HEAD):
                first = columns + c * HEAD
                part = product[:, c * HEAD : (c + 1) * HEAD] * factors[at, :]
                if first < own:
                    part = part * scale
                qkv[at, first : first + HEAD] = part.astype(bf)

    project(0, mixed_qk)

    for copy in pv_copies:
        copy.wait_recv()
    mixed_v[...] = (mv[...] + pv_in[...].astype(f32)).astype(bf)
    project(2 * own, mixed_v)
    shifted[0:1, :] = jnp.zeros((1, own), f32)

    def heads_copy(index):
        return pltpu.make_async_remote_copy(
            src_ref=heads_out.at[index], dst_ref=heads_in.at[me_s], send_sem=h_s.at[index],
            recv_sem=h_r.at[me_s], device_id={"seq": index}, device_id_type=pl.DeviceIdType.MESH,
        )

    r = lax.broadcasted_iota(jnp.int32, (block, block), 0)
    causal = lax.broadcasted_iota(jnp.int32, (block, block), 1) <= r
    for i in range(seq // 2):
        extent = (i + 1) * block
        start = i * block
        for h in range(own // HEAD):
            part = slice(h * HEAD, (h + 1) * HEAD)
            kpart = slice(own + h * HEAD, own + (h + 1) * HEAD)
            vpart = slice(2 * own + h * HEAD, 2 * own + (h + 1) * HEAD)
            query = qkv[start:extent, part]
            near = jnp.where(causal, dot_t(query, qkv[start:extent, kpart]), big_negative)
            peak = jnp.max(near, axis=-1, keepdims=True)
            if i:
                far = dot_t(query, qkv[:start, kpart])
                peak = jnp.maximum(peak, jnp.max(far, axis=-1, keepdims=True))
            weights = jnp.exp(near - peak)
            denom = jnp.sum(weights, axis=-1, keepdims=True)
            out = dot32(weights.astype(bf), qkv[start:extent, vpart])
            if i:
                weights = jnp.exp(far - peak)
                denom += jnp.sum(weights, axis=-1, keepdims=True)
                out += dot32(weights.astype(bf), qkv[:start, vpart])
            out = out / denom
            shifted[i * block + 1 : extent + 1, part] = out
        for index in (2 * i, 2 * i + 1):
            heads_out[index] = shifted[index * crows : (index + 1) * crows, :].astype(bf)

            @pl.when(me_s != index)
            def _(index=index):
                heads_copy(index).start()

    heads_in[me_s] = heads_out[me_s]
    in_wout.wait()
    in_wup.wait()
    for j in range(seq):

        @pl.when(me_s != j)
        def _(j=j):
            arrived(heads_in.at[j], h_r.at[j])

        coarse_heads[:, j * own : (j + 1) * own] = heads_in[j]

    sides = 2
    side = fcols // sides

    def partial(t, u, store):
        @pl.loop(0, side // tile)
        def _(i):
            cols = pl.ds(pl.multiple_of(u * side + i * tile, tile), tile)
            wcols = pl.ds(pl.multiple_of(t * fcols + u * side + i * tile, tile), tile)
            store(cols, dot32(coarse_heads[...], wout[:, wcols]))

    r1 = {}
    for sub in range(tp - 1, 0, -1):
        bit = sub & -sub
        lows = [low for low in tp_bits if low < bit]
        for u in range(sides):
            ucols = pl.ds(u * side, side)
            for low in lows:
                r1[sub + low, u].wait_recv()

            def put(cols, value, sub=sub, lows=lows):
                for low in lows:
                    value += recv1[sub + low - 1, :, cols].astype(f32)
                send1[sub - 1, :, cols] = value.astype(bf)

            partial(toggle(me_t, sub), u, put)
            at = (sub - 1) * sides + u
            r1[sub, u] = remote(
                send1.at[sub - 1, :, ucols], recv1.at[sub - 1, :, ucols], r1_s.at[at], r1_r.at[at],
                {"tp": flip(me_t, bit)},
            )
    sent.extend(r1.values())

    def keep(cols, value):
        short_cols[:, cols] += value

    for u in range(sides):
        partial(me_t, u, keep)
    tp_order = sorted(range(1, tp), key=lambda d: abs(2 * d - tp))
    r2 = []
    for u in range(sides):
        ucols = slice(u * side, (u + 1) * side)
        for bit in tp_bits:
            r1[bit, u].wait_recv()
        whole = short_cols[:, ucols]
        for bit in tp_bits:
            whole += recv1[bit - 1, :, ucols].astype(f32)
        top = lax.broadcasted_iota(jnp.int32, whole.shape, 0) == 0
        state[:, ucols] = jnp.where(top & (me_s == 0), 0.0, whole).astype(bf)
        for w in range(sides):
            wcols = slice(w * width // sides, (w + 1) * width // sides)
            product = dot32(state[:, ucols], wup[ucols, wcols])
            if u:
                product += lift[:, wcols]
            lift[:, wcols] = product
            if u == sides - 1:
                for d in tp_order:
                    dest = around(me_t, d, tp)
                    some = pl.ds(pl.multiple_of(dest * pool_rows, pool_rows), pool_rows)
                    at = (d - 1) * sides + w
                    send2[at] = lift[some, wcols].astype(bf)
                    r2.append(
                        remote(
                            send2.at[at], recv2.at[at], r2_s.at[at], r2_r.at[at], {"tp": dest}
                        )
                    )
    sent.extend(r2)
    for w in range(sides):
        wcols = slice(w * width // sides, (w + 1) * width // sides)
        for copy in r2[w * (tp - 1) : (w + 1) * (tp - 1)]:
            copy.wait_recv()
        lifted = lift[pl.ds(pl.multiple_of(me_t * pool_rows, pool_rows), pool_rows), wcols]
        for d in range(1, tp):
            lifted += recv2[(d - 1) * sides + w].astype(f32)
        spread = jnp.broadcast_to(lifted[:, None, :], (pool_rows, SHORT, width // sides))
        spread = spread.reshape(rows, width // sides)
        result[:, wcols] = (fine_state[:, wcols].astype(f32) + spread).astype(bf)
    for index in range(seq):

        @pl.when(me_s != index)
        def _(index=index):
            heads_copy(index).wait_send()

    for copy in sent:
        copy.wait_send()


def before_slot(me_s, tp, total):
    return lax.rem(me_s * tp + total - 1, total)


def head_body(
    tokens,
    fine_gain,
    fine_query,
    fine_keyval,
    fine_out,
    down_weight,
    coarse_gain,
    coarse_query,
    coarse_keyval,
    coarse_out,
    up_weight,
):
    seq, tp = lax.axis_size("seq"), lax.axis_size("tp")
    rows, width = tokens.shape
    depth, local_cols = coarse_query.shape
    own = local_cols // seq
    half = seq // 2
    pool_rows = rows // SHORT
    crows = pool_rows * tp
    count = crows * seq
    bf, f32 = jnp.bfloat16, jnp.float32
    V = pltpu.VMEM
    dma = lambda n: pltpu.SemaphoreType.DMA((n,))
    one = pltpu.SemaphoreType.DMA
    anywhere = pl.BlockSpec(memory_space=pl.ANY)
    vmem = pl.BlockSpec(memory_space=pltpu.VMEM)
    return pl.pallas_call(
        functools.partial(section_kernel, seq, tp),
        out_shape=jax.ShapeDtypeStruct((rows, width), bf),
        in_specs=[anywhere, vmem, anywhere, anywhere, anywhere, anywhere, vmem, anywhere,
                  anywhere, anywhere, anywhere],
        out_specs=vmem,
        scratch_shapes=[
            V(coarse_keyval.shape, bf), V((2, depth, local_cols), bf),
            V((2 * rows, width), bf), V(fine_query.shape, bf), V(fine_keyval.shape, bf),
            V(fine_out.shape, bf), V(down_weight.shape, bf), V((width, seq * depth), bf),
            V((seq * depth, 2 * own), bf), V((half * depth, 2 * own), bf),
            V(coarse_out.shape, bf), V(up_weight.shape, bf),
            V((2 * rows, width), bf), V((rows, width), bf), V((2 * rows, 2 * width), bf),
            V((rows, width), bf), V((rows, width), bf), V((seq * tp, pool_rows, width), bf),
            V((width, own), f32), V((width, own), bf),
            V((width, own), bf), V((width, 2 * own), bf), V((width, own), bf),
            V((count, 3 * own), bf), V((count, HEAD), f32),
            V((count + 8, own), f32), V((seq, crows, own), bf), V((seq, crows, own), bf),
            V((crows, local_cols), bf), V((crows, local_cols), f32), V((crows, width), f32),
            V((tp, 8, crows), f32), V((seq, 8, crows), f32),
            V((tp - 1, crows, local_cols), bf), V((tp - 1, crows, local_cols), bf),
            V((crows, local_cols), bf),
            V((2 * (tp - 1), pool_rows, width // 2), bf), V((2 * (tp - 1), pool_rows, width // 2), bf),
            dma(8), one(()), one(()), dma(2 * (seq - 1)), dma(seq), dma(2 * (half - 1)), dma(half),
            dma(4 * (tp - 1)), dma(4 * (tp - 1)), dma(tp - 1), dma(tp - 1),
            dma(seq - 1), dma(seq - 1), dma(seq - 1), dma(seq - 1),
            dma(tp - 1), dma(tp - 1), dma(seq - 1), dma(seq - 1), dma(4), dma(4),
            dma(seq), dma(seq), dma(2 * (tp - 1)), dma(2 * (tp - 1)), dma(2 * (tp - 1)),
            dma(2 * (tp - 1)),
        ],
        compiler_params=pltpu.CompilerParams(
            collective_id=0, has_side_effects=True, vmem_limit_bytes=62 * 1024 * 1024
        ),
    )(tokens, fine_gain[None], fine_query, fine_keyval, fine_out, down_weight, coarse_gain[None],
      coarse_query, coarse_keyval, coarse_out, up_weight)


def chosen(*args):
    seq, tp = lax.axis_size("seq"), lax.axis_size("tp")
    local_heads = args[7].shape[1] // HEAD
    powers = seq & (seq - 1) == 0 and tp & (tp - 1) == 0 and seq > 1 and tp > 1
    square = args[10].shape[0] == args[10].shape[1] == args[7].shape[1]
    paired = seq % tp == 0 and seq > 2 and args[7].shape[0] * (seq // tp) == args[7].shape[1]
    paired = paired and args[0].shape[0] // SHORT * tp == HEAD
    if local_heads % seq == 0 and args[0].shape[0] == WINDOW and powers and square and paired:
        return head_body(*args)
    return body(*args)


def solution(mesh):
    return jax.shard_map(
        chosen,
        mesh=mesh,
        in_specs=(
            P(("seq", "tp"), None),
            P(),
            P(),
            P(),
            P(),
            P(None, "tp"),
            P(),
            P("seq", "tp"),
            P("seq", None, "tp"),
            P("tp", None),
            P("tp", None),
        ),
        out_specs=P(("seq", "tp"), None),
        check_vma=False,
    )
```

```python
import functools
import math

import jax
import jax.numpy as jnp
from jax import lax
from jax.experimental import pallas as pl
from jax.experimental.pallas import tpu as pltpu
from jax.sharding import PartitionSpec as P

HEAD = 128
WINDOW = 256
SHORT = 8


epsilon = 1e-06
big_negative = -1e30


def from_behind(array, axis, by):
    size = lax.axis_size(axis)
    pairs = [(i, i + by) for i in range(size) if 0 <= i + by < size]
    return lax.ppermute(array, axis, pairs)


def normalize(values, scale_gain):
    mean_square = jnp.mean(values * values, axis=-1, keepdims=True)
    return values * lax.rsqrt(mean_square + epsilon) * scale_gain


def online_update(state, query_heads, key_piece, value_piece, query_index):
    running_max, running_sum, accumulate = state
    scale = 1.0 / math.sqrt(HEAD)
    scores = (
        jnp.einsum("qhd,khd->hqk", query_heads, key_piece, preferred_element_type=jnp.float32)
        * scale
    )
    key_index = jnp.arange(key_piece.shape[0], dtype=jnp.int32)
    allowed = key_index[None, :] <= query_index[:, None]
    scores = jnp.where(allowed[None], scores, big_negative)
    new_max = jnp.maximum(running_max, jnp.max(scores, axis=-1))
    terms = jnp.where(allowed[None], jnp.exp(scores - new_max[..., None]), 0.0)
    new_sum = jnp.sum(terms, axis=-1)
    product = jnp.einsum(
        "hqk,khd->hqd", terms.astype(jnp.bfloat16), value_piece, preferred_element_type=jnp.float32
    )
    return (new_max, new_sum, product)


def body(
    tokens,
    fine_gain,
    fine_query,
    fine_keyval,
    fine_out,
    down_weight,
    coarse_gain,
    coarse_query,
    coarse_keyval,
    coarse_out,
    up_weight,
):
    tok_rows = tokens.shape[0]
    width = tokens.shape[1]
    fine_heads = width // HEAD
    scale = 1.0 / math.sqrt(HEAD)
    start_row = lax.axis_index(("seq", "tp")) * tok_rows
    inputs = tokens.astype(jnp.float32)
    normed = normalize(inputs, fine_gain).astype(jnp.bfloat16)
    queries = jnp.dot(normed, fine_query, preferred_element_type=jnp.float32).astype(jnp.bfloat16)
    keyvals = jnp.dot(normed, fine_keyval, preferred_element_type=jnp.float32).astype(jnp.bfloat16)
    earlier = from_behind(keyvals, ("seq", "tp"), 1)
    key_rows = jnp.concatenate([earlier, keyvals], 0)
    span = key_rows.shape[0]
    key_heads = key_rows[:, :width].reshape(span, fine_heads, HEAD)
    value_heads = key_rows[:, width:].reshape(span, fine_heads, HEAD)
    query_heads = queries.reshape(tok_rows, fine_heads, HEAD)
    scores = (
        jnp.einsum("qhd,khd->hqk", query_heads, key_heads, preferred_element_type=jnp.float32)
        * scale
    )
    row_index = jnp.arange(tok_rows, dtype=jnp.int32)[:, None]
    col_index = jnp.arange(span, dtype=jnp.int32)[None, :]
    offset = row_index + WINDOW - col_index
    allowed = (offset >= 0) & (offset < WINDOW) & (start_row - WINDOW + col_index >= 0)
    scores = jnp.where(allowed[None], scores, big_negative)
    peak = jnp.max(scores, axis=-1, keepdims=True)
    terms = jnp.where(allowed[None], jnp.exp(scores - peak), 0.0)
    denom = jnp.sum(terms, axis=-1)
    mixed = jnp.einsum(
        "hqk,khd->qhd", terms.astype(jnp.bfloat16), value_heads, preferred_element_type=jnp.float32
    )
    local = (mixed / jnp.transpose(denom)[..., None]).reshape(tok_rows, width).astype(jnp.bfloat16)
    fine_state = (inputs + jnp.dot(local, fine_out, preferred_element_type=jnp.float32)).astype(
        jnp.bfloat16
    )
    pooled = jnp.mean(
        fine_state.astype(jnp.float32).reshape(tok_rows // SHORT, SHORT, width), axis=1
    ).astype(jnp.bfloat16)
    pooled_all = lax.all_gather(pooled, "tp", axis=0, tiled=True)
    short_cols = jnp.dot(pooled_all, down_weight, preferred_element_type=jnp.float32).astype(
        jnp.bfloat16
    )
    shortened = lax.all_gather(short_cols, "tp", axis=1, tiled=True)
    coarse_normed = normalize(shortened.astype(jnp.float32), coarse_gain).astype(jnp.bfloat16)
    coarse_rows = coarse_normed.shape[0]
    local_cols = coarse_query.shape[1]
    local_heads = local_cols // HEAD
    query_rows = lax.all_gather(coarse_query, "seq", axis=0, tiled=True)
    keyval_rows = lax.all_gather(coarse_keyval, "seq", axis=0, tiled=True)
    count = query_rows.shape[0]
    query_sum = jnp.dot(coarse_normed, query_rows, preferred_element_type=jnp.float32)
    keyval_sum = jnp.dot(
        coarse_normed,
        keyval_rows.reshape(count, 2 * local_cols),
        preferred_element_type=jnp.float32,
    )
    coarse_queries = query_sum.astype(jnp.bfloat16).reshape(coarse_rows, local_heads, HEAD)
    coarse_kv = keyval_sum.astype(jnp.bfloat16).reshape(coarse_rows, 2, local_cols)
    my_first = lax.axis_index("seq") * coarse_rows
    query_index = my_first + jnp.arange(coarse_rows, dtype=jnp.int32)
    initial = (
        jnp.full((local_heads, coarse_rows), big_negative, jnp.float32),
        jnp.zeros((local_heads, coarse_rows), jnp.float32),
        jnp.zeros((local_heads, coarse_rows, HEAD), jnp.float32),
    )
    piece = lax.all_gather(coarse_kv, "seq", axis=0, tiled=True)
    count = piece.shape[0]
    key_piece = piece[:, 0].reshape(count, local_heads, HEAD)
    value_piece = piece[:, 1].reshape(count, local_heads, HEAD)
    final = lax.cond(
        jnp.int32(0) < my_first + coarse_rows,
        lambda: online_update(initial, coarse_queries, key_piece, value_piece, query_index),
        lambda: initial,
    )
    head_out = final[2] / final[1][..., None]
    coarse_heads = (
        jnp.transpose(head_out, (1, 0, 2)).reshape(coarse_rows, local_cols).astype(jnp.bfloat16)
    )
    partials = jnp.dot(coarse_heads, coarse_out, preferred_element_type=jnp.float32)
    attended = lax.psum_scatter(
        partials.astype(jnp.bfloat16), "tp", scatter_dimension=1, tiled=True
    ).astype(jnp.float32)
    coarse_state = (short_cols.astype(jnp.float32) + attended).astype(jnp.bfloat16)
    prior_row = from_behind(coarse_state[coarse_rows - 1 :], "seq", 1)
    delayed = jnp.concatenate([prior_row, coarse_state[: coarse_rows - 1]], 0)
    lifted = lax.psum_scatter(
        jnp.dot(delayed, up_weight, preferred_element_type=jnp.float32).astype(jnp.bfloat16),
        "tp",
        scatter_dimension=0,
        tiled=True,
    ).astype(jnp.float32)
    result = fine_state.astype(jnp.float32) + jnp.repeat(lifted, SHORT, axis=0)
    return result.astype(jnp.bfloat16)


def flip(index, bit):
    return index + bit - 2 * bit * lax.rem(lax.div(index, jnp.int32(bit)), jnp.int32(2))


def bits_of(size):
    out, bit = [], size // 2
    while bit:
        out.append(bit)
        bit //= 2
    return out


def dot32(left, right):
    return jnp.dot(left, right, preferred_element_type=jnp.float32)


def dot_t(left, right):
    return lax.dot_general(
        left, right, (((1,), (1,)), ((), ())), preferred_element_type=jnp.float32
    )


END_ORDER = (4, 6, 1, 5, 2, 7, 3)
INNER_ORDER = (4, 6, 1, 5, 2, 7, 3)
PLAN = (
    (("down", 0), ("qk", 1)),
    (("v", 3), ("v", 1), ("v", 2), ("qk", 2), ("qk", 3)),
    (),
    (("down", 1),),
    (("qk", 4), ("qk", 5)),
    (("down", 2),),
    (("down", 3),),
    (("qk", 6), ("qk", 7)),
    (),
)


def section_kernel(
    seq, tp,
    tokens, fine_gain, fine_query, fine_keyval, fine_out, down_weight, coarse_gain, coarse_query,
    coarse_kv, coarse_out, up_weight,
    result,
    fgain, cgains, kv_raw, kv, both, wq, wkv, wo, down_own, down_g, wqk, wv, wout, wup,
    normed, queries, key_rows, local, fine_state, pooled_all, mv, pv_out, pv_in, mixed_qk,
    mixed_v, qkv, factors, shifted, heads_out, heads_in, coarse_heads, short_cols, lift,
    ss_tp, ss_seq, send1, recv1, state, send2, recv2,
    load_sem, halo_s, halo_r, qk_s, qk_r, v_s, v_r, d_s, d_r, pa_s, pa_r, pb_s, pb_r, pc_s, pc_r,
    ssa_s, ssa_r, ssb_s, ssb_r, pv_s, pv_r, h_s, h_r, r1_s, r1_r, r2_s, r2_r,
):
    me_s = lax.axis_index("seq")
    me_t = lax.axis_index("tp")
    rows, width = tokens.shape
    scale = 1.0 / math.sqrt(HEAD)
    total = seq * tp
    lin = me_s * tp + me_t
    after = lax.rem(lin + 1, total)
    before = lax.rem(lin + total - 1, total)
    bf, f32 = jnp.bfloat16, jnp.float32

    def around(index, step, size):
        return lax.rem(index + step, size)

    def toggle(index, mask):
        bit = 1
        while bit <= mask:
            if mask & bit:
                index = flip(index, bit)
            bit *= 2
        return index

    def remote(src, dst, send, recv, device):
        copy = pltpu.make_async_remote_copy(
            src_ref=src, dst_ref=dst, send_sem=send, recv_sem=recv,
            device_id=device, device_id_type=pl.DeviceIdType.MESH,
        )
        copy.start()
        return copy

    def load(src, dst, sem):
        copy = pltpu.make_async_copy(src, dst, sem)
        copy.start()
        return copy

    def arrived(dst, sem):
        pltpu.make_async_copy(dst, dst, sem).wait()

    def linear(index):
        return {"seq": lax.div(index, tp), "tp": lax.rem(index, tp)}

    depth = coarse_query.shape[0]
    own = coarse_query.shape[1] // seq
    fcols = down_own.shape[1]
    half = seq // 2
    zh = lax.div(me_s, half)
    in_half = lax.rem(me_s, half)
    partner = flip(me_s, half)
    pool_rows = rows // SHORT
    crows = pool_rows * tp
    count = crows * seq
    tile = 2 * HEAD

    def head_cols(dest):
        return pl.ds(pl.multiple_of(dest * own, own), own)

    def block_of(source):
        return pl.ds(pl.multiple_of(source * depth, depth), depth)

    barrier = pltpu.get_barrier_semaphore()
    peers = [{"seq": around(me_s, d, seq)} for d in range(1, seq)]
    peers += [{"tp": around(me_t, d, tp)} for d in range(1, tp)]
    peers += [linear(after), linear(before)]
    in_kv = load(coarse_kv, kv_raw, load_sem.at[5])
    in_down = load(down_weight, down_own, load_sem.at[4])
    in_cgain = load(coarse_gain, cgains, load_sem.at[8])
    in_fgain = load(fine_gain, fgain, load_sem.at[9])
    in_tokens = load(tokens, both.at[pl.ds(rows, rows)], load_sem.at[0])
    load(coarse_query.at[:, head_cols(me_s)], wqk.at[block_of(me_s), pl.ds(0, own)], qk_r.at[me_s])
    for peer in peers:
        pl.semaphore_signal(barrier, inc=1, device_id=peer, device_id_type=pl.DeviceIdType.MESH)
    in_kv.wait()
    in_wq = load(fine_query, wq, load_sem.at[2])
    in_wkv = load(fine_keyval, wkv, load_sem.at[1])
    in_wo = load(fine_out, wo, load_sem.at[3])
    step = HEAD
    picks = []
    for k in range(2):
        r = lax.broadcasted_iota(jnp.int32, (step, 2 * step), 0)
        c = lax.broadcasted_iota(jnp.int32, (step, 2 * step), 1)
        picks.append((c == 2 * r + k).astype(bf))

    @pl.loop(0, depth // step, unroll=2)
    def _(i):
        at = pl.ds(pl.multiple_of(i * step, step), step)
        turns = kv_raw[at].reshape(2 * step, kv_raw.shape[2])
        for k in range(2):
            kv[k, at, :] = dot32(picks[k], turns).astype(bf)

    load(kv.at[0, :, head_cols(me_s)], wqk.at[block_of(me_s), pl.ds(own, own)], qk_r.at[me_s])
    for k, head in enumerate((partner, me_s)):
        load(kv.at[1, :, head_cols(head)], wv.at[block_of(in_half), pl.ds(k * own, own)],
             v_r.at[in_half])
    pl.semaphore_wait(barrier, len(peers))
    in_wout = load(coarse_out, wout, load_sem.at[6])
    in_wup = load(up_weight, wup, load_sem.at[7])

    sent = []
    halo = remote(tokens, both.at[pl.ds(0, rows)], halo_s, halo_r, linear(after))

    inner = lax.rem(lax.div(me_s, half) + lax.div(me_s, max(half // 2, 1)), 2)

    def send_qk(slots):
        for n in slots:
            dest = toggle(me_s, n)
            if seq == len(END_ORDER) + 1:
                dest = toggle(me_s, END_ORDER[n - 1])
                dest += inner * (toggle(me_s, INNER_ORDER[n - 1]) - dest)
            for k, source in enumerate((coarse_query, kv.at[0])):
                sent.append(
                    remote(
                        source.at[:, head_cols(dest)], wqk.at[block_of(me_s), pl.ds(k * own, own)],
                        qk_s.at[2 * (n - 1) + k], qk_r.at[me_s], {"seq": dest},
                    )
                )

    def send_v(offsets):
        for d in offsets:
            dest = toggle(me_s, d)
            for k, head in enumerate((flip(dest, half), dest)):
                sent.append(
                    remote(
                        kv.at[1, :, head_cols(head)],
                        wv.at[block_of(in_half), pl.ds(k * own, own)],
                        v_s.at[2 * (d - 1) + k], v_r.at[in_half], {"seq": dest},
                    )
                )

    tp_bits = bits_of(tp)
    pieces = 4
    span = width // pieces
    in_down.wait()
    in_cgain.wait()
    cgain = cgains[:, pl.ds(pl.multiple_of(me_t * fcols, fcols), fcols)]

    def slot_cols(slot):
        return pl.ds(pl.multiple_of(slot * fcols, fcols), fcols)

    def down_piece(slot, bit, number, r):
        part = down_g.at[pl.ds(r * span, span), slot_cols(slot)]
        at = number * pieces + r
        return remote(part, part, d_s.at[at], d_r.at[at], {"tp": flip(me_t, bit)})

    direct = {}

    def launch_down(r):
        at = pl.ds(r * span, span)
        down_g[at, slot_cols(me_t)] = (down_own[at, :].astype(f32) * cgain).astype(bf)
        for bit in tp_bits:
            direct[r, bit] = down_piece(me_t, bit, bit - 1, r)

    def forward_down(r):
        direct[r, tp_bits[0]].wait_recv()
        for bit in tp_bits[1:]:
            if bit != tp_bits[1]:
                for copy in later[r]:
                    copy.wait_recv()
            later.setdefault(r, []).extend(
                down_piece(toggle(me_t, sub), bit, bit + sub - 1, r)
                for sub in range(2 * bit, tp, 2 * bit)
            )
            later[r].append(direct[r, bit])

    later = {}

    def finish_down(r):
        for copy in later[r]:
            copy.wait_recv()
        sent.extend(later[r] + [direct[r, tp_bits[0]]])

    plan = PLAN
    if sum(len(stage) for stage in PLAN) != seq - 1 + half - 1 + pieces:
        plan = [[("qk", d) for d in range(1, seq)] + [("v", d) for d in range(1, half)]]
        plan[0] += [("down", r) for r in range(pieces)]

    def issue(stage):
        for kind, d in plan[stage] if stage < len(plan) else ():
            if kind == "qk":
                send_qk([d])
            elif kind == "v":
                send_v([d])
            else:
                launch_down(d)

    issue(0)

    in_fgain.wait()
    gain = fgain[...]

    def norm_rows(first):
        values = both[pl.ds(first, rows), :].astype(f32)
        normed[pl.ds(first, rows), :] = normalize(values, gain).astype(bf)

    in_tokens.wait()
    norm_rows(rows)
    in_wq.wait()

    @pl.loop(0, width // tile)
    def _(i):
        cols = pl.ds(pl.multiple_of(i * tile, tile), tile)
        queries[:, cols] = dot32(normed[rows:, :], wq[:, cols]).astype(bf)

    in_wkv.wait()

    def project_rows(first):
        @pl.loop(0, 2 * width // tile)
        def _(i):
            cols = pl.ds(pl.multiple_of(i * tile, tile), tile)
            key_rows[pl.ds(first, rows), cols] = dot32(
                normed[pl.ds(first, rows), :], wkv[:, cols]
            ).astype(bf)

    project_rows(rows)
    issue(1)
    halo.wait_recv()
    sent.append(halo)
    norm_rows(0)
    project_rows(0)
    issue(2)

    own_side = lax.broadcasted_iota(jnp.int32, (rows, rows), 1) <= lax.broadcasted_iota(
        jnp.int32, (rows, rows), 0
    )
    bias = jnp.where(lin > 0, 0.0, big_negative)

    @pl.loop(0, width // HEAD, unroll=4)
    def _(h):
        cols = pl.ds(pl.multiple_of(h * HEAD, HEAD), HEAD)
        vcols = pl.ds(pl.multiple_of(width + h * HEAD, HEAD), HEAD)
        query = queries[:, cols]
        late = dot_t(query, key_rows[rows:, cols])
        early = dot_t(query, key_rows[:rows, cols]) + bias
        scores = jnp.where(own_side, late, early) * scale
        peak = jnp.max(scores, axis=-1, keepdims=True)
        weights = jnp.exp(scores - peak)
        denom = jnp.sum(weights, axis=-1, keepdims=True)
        late = jnp.where(own_side, weights, 0.0).astype(bf)
        early = jnp.where(own_side, 0.0, weights).astype(bf)
        out = dot32(late, key_rows[rows:, vcols]) + dot32(early, key_rows[:rows, vcols])
        local[:, cols] = (out / denom).astype(bf)

    in_wo.wait()

    @pl.loop(0, width // tile)
    def _(i):
        cols = pl.ds(pl.multiple_of(i * tile, tile), tile)
        value = both[rows:, cols].astype(f32) + dot32(local[...], wo[:, cols])
        value = value.astype(bf)
        fine_state[:, cols] = value
        mean = jnp.mean(value.astype(f32).reshape(pool_rows, SHORT, tile), axis=1)
        pooled_all[lin, :, cols] = mean.astype(bf)

    group = []
    for d in range(1, tp):
        slot = pooled_all.at[lin]
        group.append(remote(slot, slot, pa_s.at[d - 1], pa_r.at[d - 1], {"tp": toggle(me_t, d)}))
    issue(3)
    for copy in group:
        copy.wait_recv()
    sent.extend(group)

    core_bit = tp_bits[-1]
    share = tp // 2
    mine_first = lax.rem(me_t, 2) * share

    def blocks(first_s, offset_t):
        return pooled_all.at[pl.ds(first_s * tp + offset_t, share)]

    seq_bits = bits_of(seq)
    gather = {}

    def spread_block(mask):
        for bit in seq_bits:
            if mask == 0 or bit < (mask & -mask):
                part = blocks(toggle(me_s, mask), mine_first)
                at = (mask | bit) - 1
                gather[at + 1] = remote(
                    part, part, pb_s.at[at], pb_r.at[at], {"seq": flip(me_s, bit)}
                )

    spread_block(0)
    issue(4)

    mine = pooled_all[pl.ds(me_s * tp, tp)].reshape(crows, width)
    square_sum = jnp.zeros((8, crows), f32)
    for u in range(2):
        cols = slice(u * fcols // 2, (u + 1) * fcols // 2)
        wide = dot32(mine, down_own[:, cols]).astype(bf).astype(f32)
        short_cols[pl.ds(0, crows), cols] = wide
        square_sum += lax.dot_general(
            jnp.ones((8, fcols // 2), f32), wide * wide, (((1,), (1,)), ((), ())),
            preferred_element_type=f32, precision=lax.Precision.HIGHEST,
        )
    ss_tp[me_t] = square_sum
    group = []
    for d in range(1, tp):
        slot = ss_tp.at[me_t]
        group.append(remote(slot, slot, ssa_s.at[d - 1], ssa_r.at[d - 1], {"tp": toggle(me_t, d)}))
    issue(5)
    ss_copies = []

    def gather_sums():
        for copy in group:
            copy.wait_recv()
        sent.extend(group)
        whole_sum = ss_tp[0]
        for t in range(1, tp):
            whole_sum += ss_tp[t]
        ss_seq[me_s] = whole_sum
        for d in range(1, seq):
            slot = ss_seq.at[me_s]
            ss_copies.append(
                remote(slot, slot, ssb_s.at[d - 1], ssb_r.at[d - 1], {"seq": toggle(me_s, d)})
            )
        sent.extend(ss_copies)

    half_cols = pl.ds(pl.multiple_of(zh * half * depth, half * depth), half * depth)
    pv_copies = []

    def v_piece(piece):
        finish_down(piece)
        at = slice(piece * span, (piece + 1) * span)
        product = dot32(down_g[at, half_cols], wv[...])
        pv_out[at, :] = product[:, :own].astype(bf)
        mv[at, :] = product[:, own:]
        at = pl.ds(piece * span, span)
        pv_copies.append(
            remote(pv_out.at[at], pv_in.at[at], pv_s.at[piece], pv_r.at[piece], {"seq": partner})
        )

    evens = sorted(range(2, seq, 2), key=lambda m: (bin(m).count("1"), m))
    for at, mask in enumerate(evens):
        gather[mask].wait_recv()
        spread_block(mask)
        if at == max(0, len(evens) - 2):
            gather_sums()
        issue(6 + at)
        if at == max(0, len(evens) - 2):
            for hs in range(half):
                arrived(wv.at[pl.ds(hs * depth, depth)], v_r.at[hs])
            for piece in range(pieces // 2):
                forward_down(piece)
            for piece in range(pieces // 2):
                v_piece(piece)
    for piece in range(pieces // 2, pieces):
        forward_down(piece)
        v_piece(piece)
    sent.extend(pv_copies)
    for mask in range(1, seq, 2):
        gather[mask].wait_recv()
    sent.extend(gather.values())
    pending = []
    for k in range(seq - 1):
        part = blocks(toggle(me_s, k + 1), mine_first)
        pending.append(
            remote(part, part, pc_s.at[k], pc_r.at[k], {"tp": flip(me_t, core_bit)})
        )
    for copy in pending:
        copy.wait_recv()
    sent.extend(pending)

    for copy in ss_copies:
        copy.wait_recv()
    sums = jnp.concatenate([ss_seq[s, 0:1, :] for s in range(seq)], 0)
    inverse = lax.rsqrt(sums / (tp * fcols) + epsilon)
    turned = jnp.transpose(jnp.concatenate([inverse] * (crows // seq), 0))
    for s in range(seq):
        factors[s * crows : (s + 1) * crows, :] = jnp.broadcast_to(
            turned[:, s : s + 1], (crows, HEAD)
        )

    earlier = pooled_all[before_slot(me_s, tp, total), pool_rows - 16 :, :]
    for u in range(2):
        cols = slice(u * fcols // 2, (u + 1) * fcols // 2)
        last = dot32(earlier, down_own[:, cols]).astype(bf).astype(f32)[15:16, :]
        last = jnp.where(me_s > 0, last, 0.0)
        rolled = pltpu.roll(short_cols[pl.ds(0, crows), cols], 1, 0)
        top = lax.broadcasted_iota(jnp.int32, rolled.shape, 0) == 0
        short_cols[pl.ds(0, crows), cols] = jnp.where(top, last, rolled)

    for source in range(seq):
        arrived(wqk.at[pl.ds(source * depth, depth)], qk_r.at[source])

    @pl.loop(0, pieces)
    def _(i):
        at = pl.ds(pl.multiple_of(i * span, span), span)
        mixed_qk[at, :] = dot32(down_g[at, :], wqk[...]).astype(bf)

    block = 2 * crows

    def project(columns, mixed):
        @pl.loop(0, seq // 2)
        def _(i):
            at = pl.ds(pl.multiple_of(i * block, block), block)
            pooled = pooled_all[pl.ds(i * 2 * tp, 2 * tp)].reshape(block, width)
            product = dot32(pooled, mixed[...])
            for c in range(product.shape[1] // HEAD):
                first = columns + c * HEAD
                part = product[:, c * HEAD : (c + 1) * HEAD] * factors[at, :]
                if first < own:
                    part = part * scale
                qkv[at, first : first + HEAD] = part.astype(bf)

    project(0, mixed_qk)

    for copy in pv_copies:
        copy.wait_recv()
    mixed_v[...] = (mv[...] + pv_in[...].astype(f32)).astype(bf)
    project(2 * own, mixed_v)
    shifted[0:1, :] = jnp.zeros((1, own), f32)

    def heads_copy(index):
        return pltpu.make_async_remote_copy(
            src_ref=heads_out.at[index], dst_ref=heads_in.at[me_s], send_sem=h_s.at[index],
            recv_sem=h_r.at[me_s], device_id={"seq": index}, device_id_type=pl.DeviceIdType.MESH,
        )

    r = lax.broadcasted_iota(jnp.int32, (block, block), 0)
    causal = lax.broadcasted_iota(jnp.int32, (block, block), 1) <= r
    for i in range(seq // 2):
        extent = (i + 1) * block
        start = i * block
        for h in range(own // HEAD):
            part = slice(h * HEAD, (h + 1) * HEAD)
            kpart = slice(own + h * HEAD, own + (h + 1) * HEAD)
            vpart = slice(2 * own + h * HEAD, 2 * own + (h + 1) * HEAD)
            query = qkv[start:extent, part]
            near = jnp.where(causal, dot_t(query, qkv[start:extent, kpart]), big_negative)
            peak = jnp.max(near, axis=-1, keepdims=True)
            if i:
                far = dot_t(query, qkv[:start, kpart])
                peak = jnp.maximum(peak, jnp.max(far, axis=-1, keepdims=True))
            weights = jnp.exp(near - peak)
            denom = jnp.sum(weights, axis=-1, keepdims=True)
            out = dot32(weights.astype(bf), qkv[start:extent, vpart])
            if i:
                weights = jnp.exp(far - peak)
                denom += jnp.sum(weights, axis=-1, keepdims=True)
                out += dot32(weights.astype(bf), qkv[:start, vpart])
            out = out / denom
            shifted[i * block + 1 : extent + 1, part] = out
        for index in (2 * i, 2 * i + 1):
            heads_out[index] = shifted[index * crows : (index + 1) * crows, :].astype(bf)

            @pl.when(me_s != index)
            def _(index=index):
                heads_copy(index).start()

    heads_in[me_s] = heads_out[me_s]
    in_wout.wait()
    in_wup.wait()
    for j in range(seq):

        @pl.when(me_s != j)
        def _(j=j):
            arrived(heads_in.at[j], h_r.at[j])

        coarse_heads[:, j * own : (j + 1) * own] = heads_in[j]

    sides = 2
    side = fcols // sides

    def partial(t, u, store):
        @pl.loop(0, side // tile)
        def _(i):
            cols = pl.ds(pl.multiple_of(u * side + i * tile, tile), tile)
            wcols = pl.ds(pl.multiple_of(t * fcols + u * side + i * tile, tile), tile)
            store(cols, dot32(coarse_heads[...], wout[:, wcols]))

    r1 = {}
    for sub in range(tp - 1, 0, -1):
        bit = sub & -sub
        lows = [low for low in tp_bits if low < bit]
        for u in range(sides):
            ucols = pl.ds(u * side, side)
            for low in lows:
                r1[sub + low, u].wait_recv()

            def put(cols, value, sub=sub, lows=lows):
                for low in lows:
                    value += recv1[sub + low - 1, :, cols].astype(f32)
                send1[sub - 1, :, cols] = value.astype(bf)

            partial(toggle(me_t, sub), u, put)
            at = (sub - 1) * sides + u
            r1[sub, u] = remote(
                send1.at[sub - 1, :, ucols], recv1.at[sub - 1, :, ucols], r1_s.at[at], r1_r.at[at],
                {"tp": flip(me_t, bit)},
            )
    sent.extend(r1.values())

    def keep(cols, value):
        short_cols[:, cols] += value

    for u in range(sides):
        partial(me_t, u, keep)
    tp_order = sorted(range(1, tp), key=lambda d: abs(2 * d - tp))
    r2 = []
    for u in range(sides):
        ucols = slice(u * side, (u + 1) * side)
        for bit in tp_bits:
            r1[bit, u].wait_recv()
        whole = short_cols[:, ucols]
        for bit in tp_bits:
            whole += recv1[bit - 1, :, ucols].astype(f32)
        top = lax.broadcasted_iota(jnp.int32, whole.shape, 0) == 0
        state[:, ucols] = jnp.where(top & (me_s == 0), 0.0, whole).astype(bf)
        for w in range(sides):
            wcols = slice(w * width // sides, (w + 1) * width // sides)
            product = dot32(state[:, ucols], wup[ucols, wcols])
            if u:
                product += lift[:, wcols]
            lift[:, wcols] = product
            if u == sides - 1:
                for d in tp_order:
                    dest = around(me_t, d, tp)
                    some = pl.ds(pl.multiple_of(dest * pool_rows, pool_rows), pool_rows)
                    at = (d - 1) * sides + w
                    send2[at] = lift[some, wcols].astype(bf)
                    r2.append(
                        remote(
                            send2.at[at], recv2.at[at], r2_s.at[at], r2_r.at[at], {"tp": dest}
                        )
                    )
    sent.extend(r2)
    for w in range(sides):
        wcols = slice(w * width // sides, (w + 1) * width // sides)
        for copy in r2[w * (tp - 1) : (w + 1) * (tp - 1)]:
            copy.wait_recv()
        lifted = lift[pl.ds(pl.multiple_of(me_t * pool_rows, pool_rows), pool_rows), wcols]
        for d in range(1, tp):
            lifted += recv2[(d - 1) * sides + w].astype(f32)
        spread = jnp.broadcast_to(lifted[:, None, :], (pool_rows, SHORT, width // sides))
        spread = spread.reshape(rows, width // sides)
        result[:, wcols] = (fine_state[:, wcols].astype(f32) + spread).astype(bf)
    for index in range(seq):

        @pl.when(me_s != index)
        def _(index=index):
            heads_copy(index).wait_send()

    for copy in sent:
        copy.wait_send()


def before_slot(me_s, tp, total):
    return lax.rem(me_s * tp + total - 1, total)


def head_body(
    tokens,
    fine_gain,
    fine_query,
    fine_keyval,
    fine_out,
    down_weight,
    coarse_gain,
    coarse_query,
    coarse_keyval,
    coarse_out,
    up_weight,
):
    seq, tp = lax.axis_size("seq"), lax.axis_size("tp")
    rows, width = tokens.shape
    depth, local_cols = coarse_query.shape
    own = local_cols // seq
    half = seq // 2
    pool_rows = rows // SHORT
    crows = pool_rows * tp
    count = crows * seq
    bf, f32 = jnp.bfloat16, jnp.float32
    V = pltpu.VMEM
    dma = lambda n: pltpu.SemaphoreType.DMA((n,))
    one = pltpu.SemaphoreType.DMA
    anywhere = pl.BlockSpec(memory_space=pl.ANY)
    vmem = pl.BlockSpec(memory_space=pltpu.VMEM)
    return pl.pallas_call(
        functools.partial(section_kernel, seq, tp),
        out_shape=jax.ShapeDtypeStruct((rows, width), bf),
        in_specs=[anywhere] * 11,
        out_specs=vmem,
        scratch_shapes=[
            V((1, width), f32), V((1, tp * local_cols), f32),
            V(coarse_keyval.shape, bf), V((2, depth, local_cols), bf),
            V((2 * rows, width), bf), V(fine_query.shape, bf), V(fine_keyval.shape, bf),
            V(fine_out.shape, bf), V(down_weight.shape, bf), V((width, seq * depth), bf),
            V((seq * depth, 2 * own), bf), V((half * depth, 2 * own), bf),
            V(coarse_out.shape, bf), V(up_weight.shape, bf),
            V((2 * rows, width), bf), V((rows, width), bf), V((2 * rows, 2 * width), bf),
            V((rows, width), bf), V((rows, width), bf), V((seq * tp, pool_rows, width), bf),
            V((width, own), f32), V((width, own), bf),
            V((width, own), bf), V((width, 2 * own), bf), V((width, own), bf),
            V((count, 3 * own), bf), V((count, HEAD), f32),
            V((count + 8, own), f32), V((seq, crows, own), bf), V((seq, crows, own), bf),
            V((crows, local_cols), bf), V((crows, local_cols), f32), V((crows, width), f32),
            V((tp, 8, crows), f32), V((seq, 8, crows), f32),
            V((tp - 1, crows, local_cols), bf), V((tp - 1, crows, local_cols), bf),
            V((crows, local_cols), bf),
            V((2 * (tp - 1), pool_rows, width // 2), bf), V((2 * (tp - 1), pool_rows, width // 2), bf),
            dma(10), one(()), one(()), dma(2 * (seq - 1)), dma(seq), dma(2 * (half - 1)), dma(half),
            dma(4 * (tp - 1)), dma(4 * (tp - 1)), dma(tp - 1), dma(tp - 1),
            dma(seq - 1), dma(seq - 1), dma(seq - 1), dma(seq - 1),
            dma(tp - 1), dma(tp - 1), dma(seq - 1), dma(seq - 1), dma(4), dma(4),
            dma(seq), dma(seq), dma(2 * (tp - 1)), dma(2 * (tp - 1)), dma(2 * (tp - 1)),
            dma(2 * (tp - 1)),
        ],
        compiler_params=pltpu.CompilerParams(
            collective_id=0, has_side_effects=True, vmem_limit_bytes=54000 * 1024
        ),
    )(*(pltpu.with_memory_space_constraint(x, pltpu.HBM) for x in (
        tokens, fine_gain[None], fine_query, fine_keyval, fine_out, down_weight, coarse_gain[None],
        coarse_query, coarse_keyval, coarse_out, up_weight)))


def chosen(*args):
    seq, tp = lax.axis_size("seq"), lax.axis_size("tp")
    local_heads = args[7].shape[1] // HEAD
    powers = seq & (seq - 1) == 0 and tp & (tp - 1) == 0 and seq > 1 and tp > 1
    square = args[10].shape[0] == args[10].shape[1] == args[7].shape[1]
    paired = seq % tp == 0 and seq > 2 and args[7].shape[0] * (seq // tp) == args[7].shape[1]
    paired = paired and args[0].shape[0] // SHORT * tp == HEAD
    if local_heads % seq == 0 and args[0].shape[0] == WINDOW and powers and square and paired:
        return head_body(*args)
    return body(*args)


def solution(mesh):
    return jax.shard_map(
        chosen,
        mesh=mesh,
        in_specs=(
            P(("seq", "tp"), None),
            P(),
            P(),
            P(),
            P(),
            P(None, "tp"),
            P(),
            P("seq", "tp"),
            P("seq", None, "tp"),
            P("tp", None),
            P("tp", None),
        ),
        out_specs=P(("seq", "tp"), None),
        check_vma=False,
    )
```

```python
import functools
import math

import jax
import jax.numpy as jnp
from jax import lax
from jax.experimental import pallas as pl
from jax.experimental.pallas import tpu as pltpu
from jax.sharding import PartitionSpec as P

HEAD = 128
WINDOW = 256
SHORT = 8


epsilon = 1e-06
big_negative = -1e30


def from_behind(array, axis, by):
    size = lax.axis_size(axis)
    pairs = [(i, i + by) for i in range(size) if 0 <= i + by < size]
    return lax.ppermute(array, axis, pairs)


def normalize(values, scale_gain):
    mean_square = jnp.mean(values * values, axis=-1, keepdims=True)
    return values * lax.rsqrt(mean_square + epsilon) * scale_gain


def online_update(state, query_heads, key_piece, value_piece, query_index):
    running_max, running_sum, accumulate = state
    scale = 1.0 / math.sqrt(HEAD)
    scores = (
        jnp.einsum("qhd,khd->hqk", query_heads, key_piece, preferred_element_type=jnp.float32)
        * scale
    )
    key_index = jnp.arange(key_piece.shape[0], dtype=jnp.int32)
    allowed = key_index[None, :] <= query_index[:, None]
    scores = jnp.where(allowed[None], scores, big_negative)
    new_max = jnp.maximum(running_max, jnp.max(scores, axis=-1))
    terms = jnp.where(allowed[None], jnp.exp(scores - new_max[..., None]), 0.0)
    new_sum = jnp.sum(terms, axis=-1)
    product = jnp.einsum(
        "hqk,khd->hqd", terms.astype(jnp.bfloat16), value_piece, preferred_element_type=jnp.float32
    )
    return (new_max, new_sum, product)


def body(
    tokens,
    fine_gain,
    fine_query,
    fine_keyval,
    fine_out,
    down_weight,
    coarse_gain,
    coarse_query,
    coarse_keyval,
    coarse_out,
    up_weight,
):
    tok_rows = tokens.shape[0]
    width = tokens.shape[1]
    fine_heads = width // HEAD
    scale = 1.0 / math.sqrt(HEAD)
    start_row = lax.axis_index(("seq", "tp")) * tok_rows
    inputs = tokens.astype(jnp.float32)
    normed = normalize(inputs, fine_gain).astype(jnp.bfloat16)
    queries = jnp.dot(normed, fine_query, preferred_element_type=jnp.float32).astype(jnp.bfloat16)
    keyvals = jnp.dot(normed, fine_keyval, preferred_element_type=jnp.float32).astype(jnp.bfloat16)
    earlier = from_behind(keyvals, ("seq", "tp"), 1)
    key_rows = jnp.concatenate([earlier, keyvals], 0)
    span = key_rows.shape[0]
    key_heads = key_rows[:, :width].reshape(span, fine_heads, HEAD)
    value_heads = key_rows[:, width:].reshape(span, fine_heads, HEAD)
    query_heads = queries.reshape(tok_rows, fine_heads, HEAD)
    scores = (
        jnp.einsum("qhd,khd->hqk", query_heads, key_heads, preferred_element_type=jnp.float32)
        * scale
    )
    row_index = jnp.arange(tok_rows, dtype=jnp.int32)[:, None]
    col_index = jnp.arange(span, dtype=jnp.int32)[None, :]
    offset = row_index + WINDOW - col_index
    allowed = (offset >= 0) & (offset < WINDOW) & (start_row - WINDOW + col_index >= 0)
    scores = jnp.where(allowed[None], scores, big_negative)
    peak = jnp.max(scores, axis=-1, keepdims=True)
    terms = jnp.where(allowed[None], jnp.exp(scores - peak), 0.0)
    denom = jnp.sum(terms, axis=-1)
    mixed = jnp.einsum(
        "hqk,khd->qhd", terms.astype(jnp.bfloat16), value_heads, preferred_element_type=jnp.float32
    )
    local = (mixed / jnp.transpose(denom)[..., None]).reshape(tok_rows, width).astype(jnp.bfloat16)
    fine_state = (inputs + jnp.dot(local, fine_out, preferred_element_type=jnp.float32)).astype(
        jnp.bfloat16
    )
    pooled = jnp.mean(
        fine_state.astype(jnp.float32).reshape(tok_rows // SHORT, SHORT, width), axis=1
    ).astype(jnp.bfloat16)
    pooled_all = lax.all_gather(pooled, "tp", axis=0, tiled=True)
    short_cols = jnp.dot(pooled_all, down_weight, preferred_element_type=jnp.float32).astype(
        jnp.bfloat16
    )
    shortened = lax.all_gather(short_cols, "tp", axis=1, tiled=True)
    coarse_normed = normalize(shortened.astype(jnp.float32), coarse_gain).astype(jnp.bfloat16)
    coarse_rows = coarse_normed.shape[0]
    local_cols = coarse_query.shape[1]
    local_heads = local_cols // HEAD
    query_rows = lax.all_gather(coarse_query, "seq", axis=0, tiled=True)
    keyval_rows = lax.all_gather(coarse_keyval, "seq", axis=0, tiled=True)
    count = query_rows.shape[0]
    query_sum = jnp.dot(coarse_normed, query_rows, preferred_element_type=jnp.float32)
    keyval_sum = jnp.dot(
        coarse_normed,
        keyval_rows.reshape(count, 2 * local_cols),
        preferred_element_type=jnp.float32,
    )
    coarse_queries = query_sum.astype(jnp.bfloat16).reshape(coarse_rows, local_heads, HEAD)
    coarse_kv = keyval_sum.astype(jnp.bfloat16).reshape(coarse_rows, 2, local_cols)
    my_first = lax.axis_index("seq") * coarse_rows
    query_index = my_first + jnp.arange(coarse_rows, dtype=jnp.int32)
    initial = (
        jnp.full((local_heads, coarse_rows), big_negative, jnp.float32),
        jnp.zeros((local_heads, coarse_rows), jnp.float32),
        jnp.zeros((local_heads, coarse_rows, HEAD), jnp.float32),
    )
    piece = lax.all_gather(coarse_kv, "seq", axis=0, tiled=True)
    count = piece.shape[0]
    key_piece = piece[:, 0].reshape(count, local_heads, HEAD)
    value_piece = piece[:, 1].reshape(count, local_heads, HEAD)
    final = lax.cond(
        jnp.int32(0) < my_first + coarse_rows,
        lambda: online_update(initial, coarse_queries, key_piece, value_piece, query_index),
        lambda: initial,
    )
    head_out = final[2] / final[1][..., None]
    coarse_heads = (
        jnp.transpose(head_out, (1, 0, 2)).reshape(coarse_rows, local_cols).astype(jnp.bfloat16)
    )
    partials = jnp.dot(coarse_heads, coarse_out, preferred_element_type=jnp.float32)
    attended = lax.psum_scatter(
        partials.astype(jnp.bfloat16), "tp", scatter_dimension=1, tiled=True
    ).astype(jnp.float32)
    coarse_state = (short_cols.astype(jnp.float32) + attended).astype(jnp.bfloat16)
    prior_row = from_behind(coarse_state[coarse_rows - 1 :], "seq", 1)
    delayed = jnp.concatenate([prior_row, coarse_state[: coarse_rows - 1]], 0)
    lifted = lax.psum_scatter(
        jnp.dot(delayed, up_weight, preferred_element_type=jnp.float32).astype(jnp.bfloat16),
        "tp",
        scatter_dimension=0,
        tiled=True,
    ).astype(jnp.float32)
    result = fine_state.astype(jnp.float32) + jnp.repeat(lifted, SHORT, axis=0)
    return result.astype(jnp.bfloat16)


def flip(index, bit):
    return index + bit - 2 * bit * lax.rem(lax.div(index, jnp.int32(bit)), jnp.int32(2))


def bits_of(size):
    out, bit = [], size // 2
    while bit:
        out.append(bit)
        bit //= 2
    return out


def dot32(left, right):
    return jnp.dot(left, right, preferred_element_type=jnp.float32)


def dot_t(left, right):
    return lax.dot_general(
        left, right, (((1,), (1,)), ((), ())), preferred_element_type=jnp.float32
    )


END_ORDER = (1, 2, 3, 4, 5, 6, 7)
INNER_ORDER = (1, 2, 3, 4, 5, 6, 7)
PLAN = (
    (("down", 0), ("qk", 4)),
    (("v", 3), ("v", 1), ("v", 2), ("qk", 6), ("qk", 1)),
    (),
    (("down", 1),),
    (("qk", 5),),
    (("down", 2),),
    (("qk", 7), ("down", 3)),
    (("qk", 2), ("qk", 3)),
    (),
)


def section_kernel(
    seq, tp,
    tokens, fine_gain, fine_query, fine_keyval, fine_out, down_weight, coarse_gain, coarse_query,
    coarse_kv, coarse_out, up_weight,
    result,
    fgain, cgains, kv_raw, kv, both, wq, wkv, wo, down_own, down_g, wqk, wv, wout, wup,
    normed, queries, key_rows, local, fine_state, pooled_all, mqk, mv, pv_out, pv_in, mixed_qk,
    mixed_v, qkv, factors, shifted, heads_out, coarse_heads, short_cols, lift,
    ss_tp, ss_seq, send1, recv1, state, send2, recv2,
    load_sem, halo_s, halo_r, qk_s, qk_r, v_s, v_r, d_s, d_r, pa_s, pa_r, pb_s, pb_r, pc_s, pc_r,
    ssa_s, ssa_r, ssb_s, ssb_r, pv_s, pv_r, h_s, h_r, r1_s, r1_r, r2_s, r2_r,
):
    me_s = lax.axis_index("seq")
    me_t = lax.axis_index("tp")
    rows, width = tokens.shape
    scale = 1.0 / math.sqrt(HEAD)
    total = seq * tp
    lin = me_s * tp + me_t
    after = lax.rem(lin + 1, total)
    before = lax.rem(lin + total - 1, total)
    bf, f32 = jnp.bfloat16, jnp.float32

    def around(index, step, size):
        return lax.rem(index + step, size)

    def toggle(index, mask):
        bit = 1
        while bit <= mask:
            if mask & bit:
                index = flip(index, bit)
            bit *= 2
        return index

    def remote(src, dst, send, recv, device):
        copy = pltpu.make_async_remote_copy(
            src_ref=src, dst_ref=dst, send_sem=send, recv_sem=recv,
            device_id=device, device_id_type=pl.DeviceIdType.MESH,
        )
        copy.start()
        return copy

    def load(src, dst, sem):
        copy = pltpu.make_async_copy(src, dst, sem)
        copy.start()
        return copy

    def arrived(dst, sem):
        pltpu.make_async_copy(dst, dst, sem).wait()

    def linear(index):
        return {"seq": lax.div(index, tp), "tp": lax.rem(index, tp)}

    depth = coarse_query.shape[0]
    own = coarse_query.shape[1] // seq
    fcols = down_own.shape[1]
    half = seq // 2
    zh = lax.div(me_s, half)
    in_half = lax.rem(me_s, half)
    partner = flip(me_s, half)
    pool_rows = rows // SHORT
    crows = pool_rows * tp
    count = crows * seq
    tile = 2 * HEAD

    def head_cols(dest):
        return pl.ds(pl.multiple_of(dest * own, own), own)

    def block_of(source):
        return pl.ds(pl.multiple_of(source * depth, depth), depth)

    barrier = pltpu.get_barrier_semaphore()
    peers = [{"seq": around(me_s, d, seq)} for d in range(1, seq)]
    peers += [{"tp": around(me_t, d, tp)} for d in range(1, tp)]
    peers += [linear(after), linear(before)]
    in_kv = load(coarse_kv, kv_raw, load_sem.at[5])
    in_down = load(down_weight, down_own, load_sem.at[4])
    in_cgain = load(coarse_gain, cgains, load_sem.at[8])
    in_fgain = load(fine_gain, fgain, load_sem.at[9])
    in_tokens = load(tokens, both.at[pl.ds(rows, rows)], load_sem.at[0])
    load(coarse_query.at[:, head_cols(me_s)], wqk.at[block_of(me_s), pl.ds(0, own)], qk_r.at[me_s])
    for peer in peers:
        pl.semaphore_signal(barrier, inc=1, device_id=peer, device_id_type=pl.DeviceIdType.MESH)
    in_kv.wait()
    in_wq = load(fine_query, wq, load_sem.at[2])
    in_wkv = load(fine_keyval, wkv, load_sem.at[1])
    in_wo = load(fine_out, wo, load_sem.at[3])
    step = HEAD
    picks = []
    for k in range(2):
        r = lax.broadcasted_iota(jnp.int32, (step, 2 * step), 0)
        c = lax.broadcasted_iota(jnp.int32, (step, 2 * step), 1)
        picks.append((c == 2 * r + k).astype(bf))

    @pl.loop(0, depth // step, unroll=2)
    def _(i):
        at = pl.ds(pl.multiple_of(i * step, step), step)
        turns = kv_raw[at].reshape(2 * step, kv_raw.shape[2])
        for k in range(2):
            kv[k, at, :] = dot32(picks[k], turns).astype(bf)

    load(kv.at[0, :, head_cols(me_s)], wqk.at[block_of(me_s), pl.ds(own, own)], qk_r.at[me_s])
    for k, head in enumerate((partner, me_s)):
        load(kv.at[1, :, head_cols(head)], wv.at[block_of(in_half), pl.ds(k * own, own)],
             v_r.at[in_half])
    pl.semaphore_wait(barrier, len(peers))
    in_wout = load(coarse_out, wout, load_sem.at[6])
    in_wup = load(up_weight, wup, load_sem.at[7])

    sent = []
    halo = remote(tokens, both.at[pl.ds(0, rows)], halo_s, halo_r, linear(after))

    inner = lax.rem(lax.div(me_s, half) + lax.div(me_s, max(half // 2, 1)), 2)

    def send_qk(slots):
        for n in slots:
            dest = toggle(me_s, n)
            if seq == len(END_ORDER) + 1:
                dest = toggle(me_s, END_ORDER[n - 1])
                dest += inner * (toggle(me_s, INNER_ORDER[n - 1]) - dest)
            for k, source in enumerate((coarse_query, kv.at[0])):
                sent.append(
                    remote(
                        source.at[:, head_cols(dest)], wqk.at[block_of(me_s), pl.ds(k * own, own)],
                        qk_s.at[2 * (n - 1) + k], qk_r.at[me_s], {"seq": dest},
                    )
                )

    def send_v(offsets):
        for d in offsets:
            dest = toggle(me_s, d)
            for k, head in enumerate((flip(dest, half), dest)):
                sent.append(
                    remote(
                        kv.at[1, :, head_cols(head)],
                        wv.at[block_of(in_half), pl.ds(k * own, own)],
                        v_s.at[2 * (d - 1) + k], v_r.at[in_half], {"seq": dest},
                    )
                )

    tp_bits = bits_of(tp)
    pieces = 4
    span = width // pieces
    in_down.wait()
    in_cgain.wait()
    cgain = cgains[:, pl.ds(pl.multiple_of(me_t * fcols, fcols), fcols)]

    def slot_cols(slot):
        return pl.ds(pl.multiple_of(slot * fcols, fcols), fcols)

    def down_piece(slot, bit, number, r):
        part = down_g.at[pl.ds(r * span, span), slot_cols(slot)]
        at = number * pieces + r
        return remote(part, part, d_s.at[at], d_r.at[at], {"tp": flip(me_t, bit)})

    direct = {}

    def launch_down(r):
        at = pl.ds(r * span, span)
        down_g[at, slot_cols(me_t)] = (down_own[at, :].astype(f32) * cgain).astype(bf)
        for bit in tp_bits:
            direct[r, bit] = down_piece(me_t, bit, bit - 1, r)

    def forward_down(r):
        direct[r, tp_bits[0]].wait_recv()
        for bit in tp_bits[1:]:
            if bit != tp_bits[1]:
                for copy in later[r]:
                    copy.wait_recv()
            later.setdefault(r, []).extend(
                down_piece(toggle(me_t, sub), bit, bit + sub - 1, r)
                for sub in range(2 * bit, tp, 2 * bit)
            )
            later[r].append(direct[r, bit])

    later = {}

    def finish_down(r):
        for copy in later[r]:
            copy.wait_recv()
        sent.extend(later[r] + [direct[r, tp_bits[0]]])

    plan = PLAN
    if sum(len(stage) for stage in PLAN) != seq - 1 + half - 1 + pieces:
        plan = [[("qk", d) for d in range(1, seq)] + [("v", d) for d in range(1, half)]]
        plan[0] += [("down", r) for r in range(pieces)]

    def issue(stage):
        for kind, d in plan[stage] if stage < len(plan) else ():
            if kind == "qk":
                send_qk([d])
            elif kind == "v":
                send_v([d])
            else:
                launch_down(d)

    issue(0)

    in_fgain.wait()
    gain = fgain[...]

    def norm_rows(first):
        values = both[pl.ds(first, rows), :].astype(f32)
        normed[pl.ds(first, rows), :] = normalize(values, gain).astype(bf)

    in_tokens.wait()
    norm_rows(rows)
    in_wq.wait()

    @pl.loop(0, width // tile)
    def _(i):
        cols = pl.ds(pl.multiple_of(i * tile, tile), tile)
        queries[:, cols] = dot32(normed[rows:, :], wq[:, cols]).astype(bf)

    in_wkv.wait()

    def project_rows(first):
        @pl.loop(0, 2 * width // tile)
        def _(i):
            cols = pl.ds(pl.multiple_of(i * tile, tile), tile)
            key_rows[pl.ds(first, rows), cols] = dot32(
                normed[pl.ds(first, rows), :], wkv[:, cols]
            ).astype(bf)

    project_rows(rows)
    issue(1)
    halo.wait_recv()
    sent.append(halo)
    norm_rows(0)
    project_rows(0)
    issue(2)

    own_side = lax.broadcasted_iota(jnp.int32, (rows, rows), 1) <= lax.broadcasted_iota(
        jnp.int32, (rows, rows), 0
    )
    bias = jnp.where(lin > 0, 0.0, big_negative)

    @pl.loop(0, width // HEAD, unroll=4)
    def _(h):
        cols = pl.ds(pl.multiple_of(h * HEAD, HEAD), HEAD)
        vcols = pl.ds(pl.multiple_of(width + h * HEAD, HEAD), HEAD)
        query = queries[:, cols]
        late = dot_t(query, key_rows[rows:, cols])
        early = dot_t(query, key_rows[:rows, cols]) + bias
        scores = jnp.where(own_side, late, early) * scale
        peak = jnp.max(scores, axis=-1, keepdims=True)
        weights = jnp.exp(scores - peak)
        denom = jnp.sum(weights, axis=-1, keepdims=True)
        late = jnp.where(own_side, weights, 0.0).astype(bf)
        early = jnp.where(own_side, 0.0, weights).astype(bf)
        out = dot32(late, key_rows[rows:, vcols]) + dot32(early, key_rows[:rows, vcols])
        local[:, cols] = (out / denom).astype(bf)

    in_wo.wait()

    @pl.loop(0, width // tile)
    def _(i):
        cols = pl.ds(pl.multiple_of(i * tile, tile), tile)
        value = both[rows:, cols].astype(f32) + dot32(local[...], wo[:, cols])
        value = value.astype(bf)
        fine_state[:, cols] = value
        mean = jnp.mean(value.astype(f32).reshape(pool_rows, SHORT, tile), axis=1)
        pooled_all[lin, :, cols] = mean.astype(bf)

    group = []
    for d in range(1, tp):
        slot = pooled_all.at[lin]
        group.append(remote(slot, slot, pa_s.at[d - 1], pa_r.at[d - 1], {"tp": toggle(me_t, d)}))
    issue(3)
    for copy in group:
        copy.wait_recv()
    sent.extend(group)

    core_bit = tp_bits[-1]
    share = tp // 2
    mine_first = lax.rem(me_t, 2) * share

    def blocks(first_s, offset_t):
        return pooled_all.at[pl.ds(first_s * tp + offset_t, share)]

    seq_bits = bits_of(seq)
    gather = {}

    def spread_block(mask):
        for bit in seq_bits:
            if mask == 0 or bit < (mask & -mask):
                part = blocks(toggle(me_s, mask), mine_first)
                at = (mask | bit) - 1
                gather[at + 1] = remote(
                    part, part, pb_s.at[at], pb_r.at[at], {"seq": flip(me_s, bit)}
                )

    spread_block(0)
    issue(4)

    mine = pooled_all[pl.ds(me_s * tp, tp)].reshape(crows, width)
    square_sum = jnp.zeros((8, crows), f32)
    for u in range(2):
        cols = slice(u * fcols // 2, (u + 1) * fcols // 2)
        wide = dot32(mine, down_own[:, cols]).astype(bf).astype(f32)
        short_cols[pl.ds(0, crows), cols] = wide
        square_sum += lax.dot_general(
            jnp.ones((8, fcols // 2), f32), wide * wide, (((1,), (1,)), ((), ())),
            preferred_element_type=f32, precision=lax.Precision.HIGHEST,
        )
    ss_tp[me_t] = square_sum
    group = []
    for d in range(1, tp):
        slot = ss_tp.at[me_t]
        group.append(remote(slot, slot, ssa_s.at[d - 1], ssa_r.at[d - 1], {"tp": toggle(me_t, d)}))
    issue(5)
    ss_copies = []

    def gather_sums():
        for copy in group:
            copy.wait_recv()
        sent.extend(group)
        whole_sum = ss_tp[0]
        for t in range(1, tp):
            whole_sum += ss_tp[t]
        ss_seq[me_s] = whole_sum
        for d in range(1, seq):
            slot = ss_seq.at[me_s]
            ss_copies.append(
                remote(slot, slot, ssb_s.at[d - 1], ssb_r.at[d - 1], {"seq": toggle(me_s, d)})
            )
        sent.extend(ss_copies)

    half_cols = pl.ds(pl.multiple_of(zh * half * depth, half * depth), half * depth)
    pv_copies = []

    def v_piece(piece):
        finish_down(piece)
        at = slice(piece * span, (piece + 1) * span)
        product = dot32(down_g[at, half_cols], wv[...])
        pv_out[at, :] = product[:, :own].astype(bf)
        mv[at, :] = product[:, own:]
        at = pl.ds(piece * span, span)
        pv_copies.append(
            remote(pv_out.at[at], pv_in.at[at], pv_s.at[piece], pv_r.at[piece], {"seq": partner})
        )

    evens = sorted(range(2, seq, 2), key=lambda m: (bin(m).count("1"), m))
    for at, mask in enumerate(evens):
        gather[mask].wait_recv()
        spread_block(mask)
        if at == max(0, len(evens) - 2):
            gather_sums()
        issue(6 + at)
        if at == max(0, len(evens) - 2):
            for hs in range(half):
                arrived(wv.at[pl.ds(hs * depth, depth)], v_r.at[hs])
            for piece in range(pieces // 2):
                forward_down(piece)
            for piece in range(pieces // 2):
                v_piece(piece)
    for piece in range(pieces // 2, pieces):
        forward_down(piece)
        v_piece(piece)
    sent.extend(pv_copies)
    def add_pair(pair, first, last):
        for j in range(2):
            arrived(wqk.at[block_of(2 * pair + j)], qk_r.at[2 * pair + j])
        both_rows = pl.ds(pl.multiple_of(2 * depth * pair, 2 * depth), 2 * depth)

        @pl.loop(0, pieces)
        def _(i):
            at = pl.ds(pl.multiple_of(i * span, span), span)
            product = dot32(down_g[at, both_rows], wqk[both_rows, :])
            if not first:
                product += mqk[at, :]
            if last:
                mixed_qk[at, :] = product.astype(bf)
            else:
                mqk[at, :] = product

    pair_masks = [0] + [m for m in range(half - 1, 1, -1)][::-1] + [1]
    pairs = [toggle(lax.div(me_s, 2), mask) for mask in pair_masks]
    for n, pair in enumerate(pairs[: half // 2]):
        add_pair(pair, n == 0, False)

    for mask in range(1, seq, 2):
        gather[mask].wait_recv()
    sent.extend(gather.values())
    pending = []
    for k in range(seq - 1):
        part = blocks(toggle(me_s, k + 1), mine_first)
        pending.append(
            remote(part, part, pc_s.at[k], pc_r.at[k], {"tp": flip(me_t, core_bit)})
        )
    for pair in pairs[half // 2 : -1]:
        add_pair(pair, False, False)
    for copy in pending:
        copy.wait_recv()
    sent.extend(pending)

    for copy in ss_copies:
        copy.wait_recv()
    sums = jnp.concatenate([ss_seq[s, 0:1, :] for s in range(seq)], 0)
    inverse = lax.rsqrt(sums / (tp * fcols) + epsilon)
    turned = jnp.transpose(jnp.concatenate([inverse] * (crows // seq), 0))
    for s in range(seq):
        factors[s * crows : (s + 1) * crows, :] = jnp.broadcast_to(
            turned[:, s : s + 1], (crows, HEAD)
        )

    earlier = pooled_all[before_slot(me_s, tp, total), pool_rows - 16 :, :]
    for u in range(2):
        cols = slice(u * fcols // 2, (u + 1) * fcols // 2)
        last = dot32(earlier, down_own[:, cols]).astype(bf).astype(f32)[15:16, :]
        last = jnp.where(me_s > 0, last, 0.0)
        rolled = pltpu.roll(short_cols[pl.ds(0, crows), cols], 1, 0)
        top = lax.broadcasted_iota(jnp.int32, rolled.shape, 0) == 0
        short_cols[pl.ds(0, crows), cols] = jnp.where(top, last, rolled)

    add_pair(pairs[-1], False, True)
    block = 2 * crows

    def project(columns, mixed):
        @pl.loop(0, seq // 2)
        def _(i):
            at = pl.ds(pl.multiple_of(i * block, block), block)
            pooled = pooled_all[pl.ds(i * 2 * tp, 2 * tp)].reshape(block, width)
            product = dot32(pooled, mixed[...])
            for c in range(product.shape[1] // HEAD):
                first = columns + c * HEAD
                part = product[:, c * HEAD : (c + 1) * HEAD] * factors[at, :]
                if first < own:
                    part = part * scale
                qkv[at, first : first + HEAD] = part.astype(bf)

    project(0, mixed_qk)

    for copy in pv_copies:
        copy.wait_recv()
    mixed_v[...] = (mv[...] + pv_in[...].astype(f32)).astype(bf)
    project(2 * own, mixed_v)
    shifted[0:1, :] = jnp.zeros((1, own), f32)

    def heads_copy(index):
        return pltpu.make_async_remote_copy(
            src_ref=heads_out.at[index], dst_ref=coarse_heads.at[:, head_cols(me_s)], send_sem=h_s.at[index],
            recv_sem=h_r.at[me_s], device_id={"seq": index}, device_id_type=pl.DeviceIdType.MESH,
        )

    r = lax.broadcasted_iota(jnp.int32, (block, block), 0)
    causal = lax.broadcasted_iota(jnp.int32, (block, block), 1) <= r
    for i in range(seq // 2):
        extent = (i + 1) * block
        start = i * block
        for h in range(own // HEAD):
            part = slice(h * HEAD, (h + 1) * HEAD)
            kpart = slice(own + h * HEAD, own + (h + 1) * HEAD)
            vpart = slice(2 * own + h * HEAD, 2 * own + (h + 1) * HEAD)
            query = qkv[start:extent, part]
            near = jnp.where(causal, dot_t(query, qkv[start:extent, kpart]), big_negative)
            peak = jnp.max(near, axis=-1, keepdims=True)
            if i:
                far = dot_t(query, qkv[:start, kpart])
                peak = jnp.maximum(peak, jnp.max(far, axis=-1, keepdims=True))
            weights = jnp.exp(near - peak)
            denom = jnp.sum(weights, axis=-1, keepdims=True)
            out = dot32(weights.astype(bf), qkv[start:extent, vpart])
            if i:
                weights = jnp.exp(far - peak)
                denom += jnp.sum(weights, axis=-1, keepdims=True)
                out += dot32(weights.astype(bf), qkv[:start, vpart])
            out = out / denom
            shifted[i * block + 1 : extent + 1, part] = out
        for index in (2 * i, 2 * i + 1):
            heads_out[index] = shifted[index * crows : (index + 1) * crows, :].astype(bf)

            @pl.when(me_s != index)
            def _(index=index):
                heads_copy(index).start()

    coarse_heads[:, head_cols(me_s)] = heads_out[me_s]
    in_wout.wait()
    in_wup.wait()
    for j in range(seq):

        @pl.when(me_s != j)
        def _(j=j):
            arrived(coarse_heads.at[:, pl.ds(j * own, own)], h_r.at[j])

    sides, ways = 4, 2
    side = fcols // sides

    def partial(t, u, store):
        @pl.loop(0, side // tile)
        def _(i):
            cols = pl.ds(pl.multiple_of(u * side + i * tile, tile), tile)
            wcols = pl.ds(pl.multiple_of(t * fcols + u * side + i * tile, tile), tile)
            store(cols, dot32(coarse_heads[...], wout[:, wcols]))

    r1 = {}
    for sub in range(tp - 1, 0, -1):
        bit = sub & -sub
        lows = [low for low in tp_bits if low < bit]
        for u in range(sides):
            ucols = pl.ds(u * side, side)
            for low in lows:
                r1[sub + low, u].wait_recv()

            def put(cols, value, sub=sub, lows=lows):
                for low in lows:
                    value += recv1[sub + low - 1, :, cols].astype(f32)
                send1[sub - 1, :, cols] = value.astype(bf)

            partial(toggle(me_t, sub), u, put)
            at = (sub - 1) * sides + u
            r1[sub, u] = remote(
                send1.at[sub - 1, :, ucols], recv1.at[sub - 1, :, ucols], r1_s.at[at], r1_r.at[at],
                {"tp": flip(me_t, bit)},
            )
    sent.extend(r1.values())

    def keep(cols, value):
        short_cols[:, cols] += value

    for u in range(sides):
        partial(me_t, u, keep)
    tp_order = sorted(range(1, tp), key=lambda d: abs(2 * d - tp))
    r2 = []
    for u in range(sides):
        ucols = slice(u * side, (u + 1) * side)
        for bit in tp_bits:
            r1[bit, u].wait_recv()
        whole = short_cols[:, ucols]
        for bit in tp_bits:
            whole += recv1[bit - 1, :, ucols].astype(f32)
        top = lax.broadcasted_iota(jnp.int32, whole.shape, 0) == 0
        state[:, ucols] = jnp.where(top & (me_s == 0), 0.0, whole).astype(bf)
        for w in range(ways):
            wcols = slice(w * width // ways, (w + 1) * width // ways)
            product = dot32(state[:, ucols], wup[ucols, wcols])
            if u:
                product += lift[:, wcols]
            lift[:, wcols] = product
            if u == sides - 1:
                for d in tp_order:
                    dest = around(me_t, d, tp)
                    some = pl.ds(pl.multiple_of(dest * pool_rows, pool_rows), pool_rows)
                    at = (d - 1) * ways + w
                    send2[at] = lift[some, wcols].astype(bf)
                    r2.append(
                        remote(
                            send2.at[at], recv2.at[at], r2_s.at[at], r2_r.at[at], {"tp": dest}
                        )
                    )
    sent.extend(r2)
    for w in range(ways):
        wcols = slice(w * width // ways, (w + 1) * width // ways)
        for copy in r2[w * (tp - 1) : (w + 1) * (tp - 1)]:
            copy.wait_recv()
        lifted = lift[pl.ds(pl.multiple_of(me_t * pool_rows, pool_rows), pool_rows), wcols]
        for d in range(1, tp):
            lifted += recv2[(d - 1) * ways + w].astype(f32)
        spread = jnp.broadcast_to(lifted[:, None, :], (pool_rows, SHORT, width // ways))
        spread = spread.reshape(rows, width // ways)
        result[:, wcols] = (fine_state[:, wcols].astype(f32) + spread).astype(bf)
    for index in range(seq):

        @pl.when(me_s != index)
        def _(index=index):
            heads_copy(index).wait_send()

    for copy in sent:
        copy.wait_send()


def before_slot(me_s, tp, total):
    return lax.rem(me_s * tp + total - 1, total)


def head_body(
    tokens,
    fine_gain,
    fine_query,
    fine_keyval,
    fine_out,
    down_weight,
    coarse_gain,
    coarse_query,
    coarse_keyval,
    coarse_out,
    up_weight,
):
    seq, tp = lax.axis_size("seq"), lax.axis_size("tp")
    rows, width = tokens.shape
    depth, local_cols = coarse_query.shape
    own = local_cols // seq
    half = seq // 2
    pool_rows = rows // SHORT
    crows = pool_rows * tp
    count = crows * seq
    bf, f32 = jnp.bfloat16, jnp.float32
    V = pltpu.VMEM
    dma = lambda n: pltpu.SemaphoreType.DMA((n,))
    one = pltpu.SemaphoreType.DMA
    anywhere = pl.BlockSpec(memory_space=pl.ANY)
    vmem = pl.BlockSpec(memory_space=pltpu.VMEM)
    return pl.pallas_call(
        functools.partial(section_kernel, seq, tp),
        out_shape=jax.ShapeDtypeStruct((rows, width), bf),
        in_specs=[anywhere] * 11,
        out_specs=vmem,
        scratch_shapes=[
            V((1, width), f32), V((1, tp * local_cols), f32),
            V(coarse_keyval.shape, bf), V((2, depth, local_cols), bf),
            V((2 * rows, width), bf), V(fine_query.shape, bf), V(fine_keyval.shape, bf),
            V(fine_out.shape, bf), V(down_weight.shape, bf), V((width, seq * depth), bf),
            V((seq * depth, 2 * own), bf), V((half * depth, 2 * own), bf),
            V(coarse_out.shape, bf), V(up_weight.shape, bf),
            V((2 * rows, width), bf), V((rows, width), bf), V((2 * rows, 2 * width), bf),
            V((rows, width), bf), V((rows, width), bf), V((seq * tp, pool_rows, width), bf),
            V((width, 2 * own), f32), V((width, own), f32), V((width, own), bf),
            V((width, own), bf), V((width, 2 * own), bf), V((width, own), bf),
            V((count, 3 * own), bf), V((count, HEAD), f32),
            V((count + 8, own), f32), V((seq, crows, own), bf),
            V((crows, local_cols), bf), V((crows, local_cols), f32), V((crows, width), f32),
            V((tp, 8, crows), f32), V((seq, 8, crows), f32),
            V((tp - 1, crows, local_cols), bf), V((tp - 1, crows, local_cols), bf),
            V((crows, local_cols), bf),
            V((2 * (tp - 1), pool_rows, width // 2), bf), V((2 * (tp - 1), pool_rows, width // 2), bf),
            dma(10), one(()), one(()), dma(2 * (seq - 1)), dma(seq), dma(2 * (half - 1)), dma(half),
            dma(4 * (tp - 1)), dma(4 * (tp - 1)), dma(tp - 1), dma(tp - 1),
            dma(seq - 1), dma(seq - 1), dma(seq - 1), dma(seq - 1),
            dma(tp - 1), dma(tp - 1), dma(seq - 1), dma(seq - 1), dma(4), dma(4),
            dma(seq), dma(seq), dma(4 * (tp - 1)), dma(4 * (tp - 1)), dma(2 * (tp - 1)),
            dma(2 * (tp - 1)),
        ],
        compiler_params=pltpu.CompilerParams(
            collective_id=0, has_side_effects=True, vmem_limit_bytes=54000 * 1024
        ),
    )(*(pltpu.with_memory_space_constraint(x, pltpu.HBM) for x in (
        tokens, fine_gain[None], fine_query, fine_keyval, fine_out, down_weight, coarse_gain[None],
        coarse_query, coarse_keyval, coarse_out, up_weight)))


def chosen(*args):
    seq, tp = lax.axis_size("seq"), lax.axis_size("tp")
    local_heads = args[7].shape[1] // HEAD
    powers = seq & (seq - 1) == 0 and tp & (tp - 1) == 0 and seq > 1 and tp > 1
    square = args[10].shape[0] == args[10].shape[1] == args[7].shape[1]
    paired = seq % tp == 0 and seq > 2 and args[7].shape[0] * (seq // tp) == args[7].shape[1]
    paired = paired and args[0].shape[0] // SHORT * tp == HEAD
    if local_heads % seq == 0 and args[0].shape[0] == WINDOW and powers and square and paired:
        return head_body(*args)
    return body(*args)


def solution(mesh):
    return jax.shard_map(
        chosen,
        mesh=mesh,
        in_specs=(
            P(("seq", "tp"), None),
            P(),
            P(),
            P(),
            P(),
            P(None, "tp"),
            P(),
            P("seq", "tp"),
            P("seq", None, "tp"),
            P("tp", None),
            P("tp", None),
        ),
        out_specs=P(("seq", "tp"), None),
        check_vma=False,
    )
```

```python
import functools
import math

import jax
import jax.numpy as jnp
from jax import lax
from jax.experimental import pallas as pl
from jax.experimental.pallas import tpu as pltpu
from jax.sharding import PartitionSpec as P

HEAD = 128
WINDOW = 256
SHORT = 8


epsilon = 1e-06
big_negative = -1e30


def from_behind(array, axis, by):
    size = lax.axis_size(axis)
    pairs = [(i, i + by) for i in range(size) if 0 <= i + by < size]
    return lax.ppermute(array, axis, pairs)


def normalize(values, scale_gain):
    mean_square = jnp.mean(values * values, axis=-1, keepdims=True)
    return values * lax.rsqrt(mean_square + epsilon) * scale_gain


def online_update(state, query_heads, key_piece, value_piece, query_index):
    running_max, running_sum, accumulate = state
    scale = 1.0 / math.sqrt(HEAD)
    scores = (
        jnp.einsum("qhd,khd->hqk", query_heads, key_piece, preferred_element_type=jnp.float32)
        * scale
    )
    key_index = jnp.arange(key_piece.shape[0], dtype=jnp.int32)
    allowed = key_index[None, :] <= query_index[:, None]
    scores = jnp.where(allowed[None], scores, big_negative)
    new_max = jnp.maximum(running_max, jnp.max(scores, axis=-1))
    terms = jnp.where(allowed[None], jnp.exp(scores - new_max[..., None]), 0.0)
    new_sum = jnp.sum(terms, axis=-1)
    product = jnp.einsum(
        "hqk,khd->hqd", terms.astype(jnp.bfloat16), value_piece, preferred_element_type=jnp.float32
    )
    return (new_max, new_sum, product)


def body(
    tokens,
    fine_gain,
    fine_query,
    fine_keyval,
    fine_out,
    down_weight,
    coarse_gain,
    coarse_query,
    coarse_keyval,
    coarse_out,
    up_weight,
):
    tok_rows = tokens.shape[0]
    width = tokens.shape[1]
    fine_heads = width // HEAD
    scale = 1.0 / math.sqrt(HEAD)
    start_row = lax.axis_index(("seq", "tp")) * tok_rows
    inputs = tokens.astype(jnp.float32)
    normed = normalize(inputs, fine_gain).astype(jnp.bfloat16)
    queries = jnp.dot(normed, fine_query, preferred_element_type=jnp.float32).astype(jnp.bfloat16)
    keyvals = jnp.dot(normed, fine_keyval, preferred_element_type=jnp.float32).astype(jnp.bfloat16)
    earlier = from_behind(keyvals, ("seq", "tp"), 1)
    key_rows = jnp.concatenate([earlier, keyvals], 0)
    span = key_rows.shape[0]
    key_heads = key_rows[:, :width].reshape(span, fine_heads, HEAD)
    value_heads = key_rows[:, width:].reshape(span, fine_heads, HEAD)
    query_heads = queries.reshape(tok_rows, fine_heads, HEAD)
    scores = (
        jnp.einsum("qhd,khd->hqk", query_heads, key_heads, preferred_element_type=jnp.float32)
        * scale
    )
    row_index = jnp.arange(tok_rows, dtype=jnp.int32)[:, None]
    col_index = jnp.arange(span, dtype=jnp.int32)[None, :]
    offset = row_index + WINDOW - col_index
    allowed = (offset >= 0) & (offset < WINDOW) & (start_row - WINDOW + col_index >= 0)
    scores = jnp.where(allowed[None], scores, big_negative)
    peak = jnp.max(scores, axis=-1, keepdims=True)
    terms = jnp.where(allowed[None], jnp.exp(scores - peak), 0.0)
    denom = jnp.sum(terms, axis=-1)
    mixed = jnp.einsum(
        "hqk,khd->qhd", terms.astype(jnp.bfloat16), value_heads, preferred_element_type=jnp.float32
    )
    local = (mixed / jnp.transpose(denom)[..., None]).reshape(tok_rows, width).astype(jnp.bfloat16)
    fine_state = (inputs + jnp.dot(local, fine_out, preferred_element_type=jnp.float32)).astype(
        jnp.bfloat16
    )
    pooled = jnp.mean(
        fine_state.astype(jnp.float32).reshape(tok_rows // SHORT, SHORT, width), axis=1
    ).astype(jnp.bfloat16)
    pooled_all = lax.all_gather(pooled, "tp", axis=0, tiled=True)
    short_cols = jnp.dot(pooled_all, down_weight, preferred_element_type=jnp.float32).astype(
        jnp.bfloat16
    )
    shortened = lax.all_gather(short_cols, "tp", axis=1, tiled=True)
    coarse_normed = normalize(shortened.astype(jnp.float32), coarse_gain).astype(jnp.bfloat16)
    coarse_rows = coarse_normed.shape[0]
    local_cols = coarse_query.shape[1]
    local_heads = local_cols // HEAD
    query_rows = lax.all_gather(coarse_query, "seq", axis=0, tiled=True)
    keyval_rows = lax.all_gather(coarse_keyval, "seq", axis=0, tiled=True)
    count = query_rows.shape[0]
    query_sum = jnp.dot(coarse_normed, query_rows, preferred_element_type=jnp.float32)
    keyval_sum = jnp.dot(
        coarse_normed,
        keyval_rows.reshape(count, 2 * local_cols),
        preferred_element_type=jnp.float32,
    )
    coarse_queries = query_sum.astype(jnp.bfloat16).reshape(coarse_rows, local_heads, HEAD)
    coarse_kv = keyval_sum.astype(jnp.bfloat16).reshape(coarse_rows, 2, local_cols)
    my_first = lax.axis_index("seq") * coarse_rows
    query_index = my_first + jnp.arange(coarse_rows, dtype=jnp.int32)
    initial = (
        jnp.full((local_heads, coarse_rows), big_negative, jnp.float32),
        jnp.zeros((local_heads, coarse_rows), jnp.float32),
        jnp.zeros((local_heads, coarse_rows, HEAD), jnp.float32),
    )
    piece = lax.all_gather(coarse_kv, "seq", axis=0, tiled=True)
    count = piece.shape[0]
    key_piece = piece[:, 0].reshape(count, local_heads, HEAD)
    value_piece = piece[:, 1].reshape(count, local_heads, HEAD)
    final = lax.cond(
        jnp.int32(0) < my_first + coarse_rows,
        lambda: online_update(initial, coarse_queries, key_piece, value_piece, query_index),
        lambda: initial,
    )
    head_out = final[2] / final[1][..., None]
    coarse_heads = (
        jnp.transpose(head_out, (1, 0, 2)).reshape(coarse_rows, local_cols).astype(jnp.bfloat16)
    )
    partials = jnp.dot(coarse_heads, coarse_out, preferred_element_type=jnp.float32)
    attended = lax.psum_scatter(
        partials.astype(jnp.bfloat16), "tp", scatter_dimension=1, tiled=True
    ).astype(jnp.float32)
    coarse_state = (short_cols.astype(jnp.float32) + attended).astype(jnp.bfloat16)
    prior_row = from_behind(coarse_state[coarse_rows - 1 :], "seq", 1)
    delayed = jnp.concatenate([prior_row, coarse_state[: coarse_rows - 1]], 0)
    lifted = lax.psum_scatter(
        jnp.dot(delayed, up_weight, preferred_element_type=jnp.float32).astype(jnp.bfloat16),
        "tp",
        scatter_dimension=0,
        tiled=True,
    ).astype(jnp.float32)
    result = fine_state.astype(jnp.float32) + jnp.repeat(lifted, SHORT, axis=0)
    return result.astype(jnp.bfloat16)


def flip(index, bit):
    return index + bit - 2 * bit * lax.rem(lax.div(index, jnp.int32(bit)), jnp.int32(2))


def bits_of(size):
    out, bit = [], size // 2
    while bit:
        out.append(bit)
        bit //= 2
    return out


def dot32(left, right):
    return jnp.dot(left, right, preferred_element_type=jnp.float32)


def dot_t(left, right):
    return lax.dot_general(
        left, right, (((1,), (1,)), ((), ())), preferred_element_type=jnp.float32
    )


PLAN = (
    (("down", 0), ("qk", 4)),
    (("v", 3), ("v", 1), ("v", 2), ("qk", 6), ("qk", 1)),
    (),
    (("down", 1),),
    (("qk", 7),),
    (("down", 2),),
    (("qk", 5), ("down", 3)),
    (("qk", 2), ("qk", 3)),
    (),
)


def section_kernel(
    seq, tp,
    tokens, fine_gain, fine_query, fine_keyval, fine_out, down_weight, coarse_gain, coarse_query,
    coarse_kv, coarse_out, up_weight,
    result,
    fgain, cgains, kv_raw, kv, both, wq, wkv, wo, down_own, down_g, wqk, wv, wout, wup,
    normed, queries, key_rows, local, fine_state, pooled_all, mqk, mv, pv_out, pv_in, mixed_qk,
    mixed_v, qkv, factors, shifted, heads_out, coarse_heads, short_cols, lift,
    ss_tp, ss_seq, send1, recv1, state, send2, recv2,
    load_sem, halo_s, halo_r, qk_s, qk_r, v_s, v_r, d_s, d_r, pa_s, pa_r, pb_s, pb_r, pc_s, pc_r,
    ssa_s, ssa_r, ssb_s, ssb_r, pv_s, pv_r, h_s, h_r, r1_s, r1_r, r2_s, r2_r,
):
    me_s = lax.axis_index("seq")
    me_t = lax.axis_index("tp")
    rows, width = tokens.shape
    scale = 1.0 / math.sqrt(HEAD)
    total = seq * tp
    lin = me_s * tp + me_t
    after = lax.rem(lin + 1, total)
    before = lax.rem(lin + total - 1, total)
    bf, f32 = jnp.bfloat16, jnp.float32

    def around(index, step, size):
        return lax.rem(index + step, size)

    def toggle(index, mask):
        bit = 1
        while bit <= mask:
            if mask & bit:
                index = flip(index, bit)
            bit *= 2
        return index

    def remote(src, dst, send, recv, device):
        copy = pltpu.make_async_remote_copy(
            src_ref=src, dst_ref=dst, send_sem=send, recv_sem=recv,
            device_id=device, device_id_type=pl.DeviceIdType.MESH,
        )
        copy.start()
        return copy

    def load(src, dst, sem):
        copy = pltpu.make_async_copy(src, dst, sem)
        copy.start()
        return copy

    def arrived(dst, sem):
        pltpu.make_async_copy(dst, dst, sem).wait()

    def linear(index):
        return {"seq": lax.div(index, tp), "tp": lax.rem(index, tp)}

    depth = coarse_query.shape[0]
    own = coarse_query.shape[1] // seq
    fcols = down_own.shape[1]
    half = seq // 2
    zh = lax.div(me_s, half)
    in_half = lax.rem(me_s, half)
    partner = flip(me_s, half)
    pool_rows = rows // SHORT
    crows = pool_rows * tp
    count = crows * seq
    tile = 2 * HEAD

    def head_cols(dest):
        return pl.ds(pl.multiple_of(dest * own, own), own)

    def block_of(source):
        return pl.ds(pl.multiple_of(source * depth, depth), depth)

    barrier = pltpu.get_barrier_semaphore()
    peers = [{"seq": around(me_s, d, seq)} for d in range(1, seq)]
    peers += [{"tp": around(me_t, d, tp)} for d in range(1, tp)]
    peers += [linear(after), linear(before)]
    in_kv = load(coarse_kv, kv_raw, load_sem.at[5])
    in_down = load(down_weight, down_own, load_sem.at[4])
    in_cgain = load(coarse_gain, cgains, load_sem.at[8])
    in_fgain = load(fine_gain, fgain, load_sem.at[9])
    in_tokens = load(tokens, both.at[pl.ds(rows, rows)], load_sem.at[0])
    load(coarse_query.at[:, head_cols(me_s)], wqk.at[block_of(me_s), pl.ds(0, own)], qk_r.at[me_s])
    for peer in peers:
        pl.semaphore_signal(barrier, inc=1, device_id=peer, device_id_type=pl.DeviceIdType.MESH)
    in_kv.wait()
    in_wq = load(fine_query, wq, load_sem.at[2])
    in_wkv = load(fine_keyval, wkv, load_sem.at[1])
    in_wo = load(fine_out, wo, load_sem.at[3])
    step = HEAD
    picks = []
    for k in range(2):
        r = lax.broadcasted_iota(jnp.int32, (step, 2 * step), 0)
        c = lax.broadcasted_iota(jnp.int32, (step, 2 * step), 1)
        picks.append((c == 2 * r + k).astype(bf))

    @pl.loop(0, depth // step, unroll=2)
    def _(i):
        at = pl.ds(pl.multiple_of(i * step, step), step)
        turns = kv_raw[at].reshape(2 * step, kv_raw.shape[2])
        for k in range(2):
            kv[k, at, :] = dot32(picks[k], turns).astype(bf)

    load(kv.at[0, :, head_cols(me_s)], wqk.at[block_of(me_s), pl.ds(own, own)], qk_r.at[me_s])
    for k, head in enumerate((partner, me_s)):
        load(kv.at[1, :, head_cols(head)], wv.at[block_of(in_half), pl.ds(k * own, own)],
             v_r.at[in_half])
    pl.semaphore_wait(barrier, len(peers))
    in_wout = load(coarse_out, wout, load_sem.at[6])
    in_wup = load(up_weight, wup, load_sem.at[7])

    sent = []
    halo = remote(tokens, both.at[pl.ds(0, rows)], halo_s, halo_r, linear(after))

    def send_qk(offsets):
        for n in offsets:
            dest = toggle(me_s, n)
            for k, source in enumerate((coarse_query, kv.at[0])):
                sent.append(
                    remote(
                        source.at[:, head_cols(dest)], wqk.at[block_of(me_s), pl.ds(k * own, own)],
                        qk_s.at[2 * (n - 1) + k], qk_r.at[me_s], {"seq": dest},
                    )
                )

    def send_v(offsets):
        for d in offsets:
            dest = toggle(me_s, d)
            for k, head in enumerate((flip(dest, half), dest)):
                sent.append(
                    remote(
                        kv.at[1, :, head_cols(head)],
                        wv.at[block_of(in_half), pl.ds(k * own, own)],
                        v_s.at[2 * (d - 1) + k], v_r.at[in_half], {"seq": dest},
                    )
                )

    tp_bits = bits_of(tp)
    pieces = 4
    span = width // pieces
    in_down.wait()
    in_cgain.wait()
    cgain = cgains[:, pl.ds(pl.multiple_of(me_t * fcols, fcols), fcols)]

    def slot_cols(slot):
        return pl.ds(pl.multiple_of(slot * fcols, fcols), fcols)

    def down_piece(slot, bit, number, r):
        part = down_g.at[pl.ds(r * span, span), slot_cols(slot)]
        at = number * pieces + r
        return remote(part, part, d_s.at[at], d_r.at[at], {"tp": flip(me_t, bit)})

    direct = {}

    def launch_down(r):
        at = pl.ds(r * span, span)
        down_g[at, slot_cols(me_t)] = (down_own[at, :].astype(f32) * cgain).astype(bf)
        for bit in tp_bits:
            direct[r, bit] = down_piece(me_t, bit, bit - 1, r)

    def forward_down(r):
        direct[r, tp_bits[0]].wait_recv()
        for bit in tp_bits[1:]:
            if bit != tp_bits[1]:
                for copy in later[r]:
                    copy.wait_recv()
            later.setdefault(r, []).extend(
                down_piece(toggle(me_t, sub), bit, bit + sub - 1, r)
                for sub in range(2 * bit, tp, 2 * bit)
            )
            later[r].append(direct[r, bit])

    later = {}

    def finish_down(r):
        for copy in later[r]:
            copy.wait_recv()
        sent.extend(later[r] + [direct[r, tp_bits[0]]])

    plan = PLAN
    if sum(len(stage) for stage in PLAN) != seq - 1 + half - 1 + pieces:
        plan = [[("qk", d) for d in range(1, seq)] + [("v", d) for d in range(1, half)]]
        plan[0] += [("down", r) for r in range(pieces)]

    def issue(stage):
        for kind, d in plan[stage] if stage < len(plan) else ():
            if kind == "qk":
                send_qk([d])
            elif kind == "v":
                send_v([d])
            else:
                launch_down(d)

    issue(0)

    in_fgain.wait()
    gain = fgain[...]

    def norm_rows(first):
        values = both[pl.ds(first, rows), :].astype(f32)
        normed[pl.ds(first, rows), :] = normalize(values, gain).astype(bf)

    in_tokens.wait()
    norm_rows(rows)
    in_wq.wait()

    @pl.loop(0, width // tile)
    def _(i):
        cols = pl.ds(pl.multiple_of(i * tile, tile), tile)
        queries[:, cols] = dot32(normed[rows:, :], wq[:, cols]).astype(bf)

    in_wkv.wait()

    def project_rows(first):
        @pl.loop(0, 2 * width // tile)
        def _(i):
            cols = pl.ds(pl.multiple_of(i * tile, tile), tile)
            key_rows[pl.ds(first, rows), cols] = dot32(
                normed[pl.ds(first, rows), :], wkv[:, cols]
            ).astype(bf)

    project_rows(rows)
    issue(1)
    halo.wait_recv()
    sent.append(halo)
    norm_rows(0)
    project_rows(0)
    issue(2)

    own_side = lax.broadcasted_iota(jnp.int32, (rows, rows), 1) <= lax.broadcasted_iota(
        jnp.int32, (rows, rows), 0
    )
    bias = jnp.where(lin > 0, 0.0, big_negative)

    @pl.loop(0, width // HEAD, unroll=4)
    def _(h):
        cols = pl.ds(pl.multiple_of(h * HEAD, HEAD), HEAD)
        vcols = pl.ds(pl.multiple_of(width + h * HEAD, HEAD), HEAD)
        query = queries[:, cols]
        late = dot_t(query, key_rows[rows:, cols])
        early = dot_t(query, key_rows[:rows, cols]) + bias
        scores = jnp.where(own_side, late, early) * scale
        peak = jnp.max(scores, axis=-1, keepdims=True)
        weights = jnp.exp(scores - peak)
        denom = jnp.sum(weights, axis=-1, keepdims=True)
        late = jnp.where(own_side, weights, 0.0).astype(bf)
        early = jnp.where(own_side, 0.0, weights).astype(bf)
        out = dot32(late, key_rows[rows:, vcols]) + dot32(early, key_rows[:rows, vcols])
        local[:, cols] = (out / denom).astype(bf)

    in_wo.wait()

    @pl.loop(0, width // tile)
    def _(i):
        cols = pl.ds(pl.multiple_of(i * tile, tile), tile)
        value = both[rows:, cols].astype(f32) + dot32(local[...], wo[:, cols])
        value = value.astype(bf)
        fine_state[:, cols] = value
        mean = jnp.mean(value.astype(f32).reshape(pool_rows, SHORT, tile), axis=1)
        pooled_all[lin, :, cols] = mean.astype(bf)

    group = []
    for d in range(1, tp):
        slot = pooled_all.at[lin]
        group.append(remote(slot, slot, pa_s.at[d - 1], pa_r.at[d - 1], {"tp": toggle(me_t, d)}))
    issue(3)
    for copy in group:
        copy.wait_recv()
    sent.extend(group)

    core_bit = tp_bits[-1]
    share = tp // 2
    mine_first = lax.rem(me_t, 2) * share

    def blocks(first_s, offset_t):
        return pooled_all.at[pl.ds(first_s * tp + offset_t, share)]

    seq_bits = bits_of(seq)
    gather = {}

    def spread_block(mask):
        for bit in seq_bits:
            if mask == 0 or bit < (mask & -mask):
                part = blocks(toggle(me_s, mask), mine_first)
                at = (mask | bit) - 1
                gather[at + 1] = remote(
                    part, part, pb_s.at[at], pb_r.at[at], {"seq": flip(me_s, bit)}
                )

    spread_block(0)
    issue(4)

    mine = pooled_all[pl.ds(me_s * tp, tp)].reshape(crows, width)
    square_sum = jnp.zeros((8, crows), f32)
    for u in range(2):
        cols = slice(u * fcols // 2, (u + 1) * fcols // 2)
        wide = dot32(mine, down_own[:, cols]).astype(bf).astype(f32)
        short_cols[pl.ds(0, crows), cols] = wide
        square_sum += lax.dot_general(
            jnp.ones((8, fcols // 2), f32), wide * wide, (((1,), (1,)), ((), ())),
            preferred_element_type=f32, precision=lax.Precision.HIGHEST,
        )
    ss_tp[me_t] = square_sum
    group = []
    for d in range(1, tp):
        slot = ss_tp.at[me_t]
        group.append(remote(slot, slot, ssa_s.at[d - 1], ssa_r.at[d - 1], {"tp": toggle(me_t, d)}))
    issue(5)
    ss_copies = []

    def gather_sums():
        for copy in group:
            copy.wait_recv()
        sent.extend(group)
        whole_sum = ss_tp[0]
        for t in range(1, tp):
            whole_sum += ss_tp[t]
        ss_seq[me_s] = whole_sum
        for d in range(1, seq):
            slot = ss_seq.at[me_s]
            ss_copies.append(
                remote(slot, slot, ssb_s.at[d - 1], ssb_r.at[d - 1], {"seq": toggle(me_s, d)})
            )
        sent.extend(ss_copies)

    half_cols = pl.ds(pl.multiple_of(zh * half * depth, half * depth), half * depth)
    pv_copies = []

    def v_piece(piece):
        finish_down(piece)
        at = slice(piece * span, (piece + 1) * span)
        product = dot32(down_g[at, half_cols], wv[...])
        pv_out[at, :] = product[:, :own].astype(bf)
        mv[at, :] = product[:, own:]
        at = pl.ds(piece * span, span)
        pv_copies.append(
            remote(pv_out.at[at], pv_in.at[at], pv_s.at[piece], pv_r.at[piece], {"seq": partner})
        )

    evens = sorted(range(2, seq, 2), key=lambda m: (bin(m).count("1"), m))
    for at, mask in enumerate(evens):
        gather[mask].wait_recv()
        spread_block(mask)
        if at == max(0, len(evens) - 2):
            gather_sums()
        if at == max(0, len(evens) - 2):
            for hs in range(half):
                arrived(wv.at[pl.ds(hs * depth, depth)], v_r.at[hs])
            for piece in range(pieces // 2):
                forward_down(piece)
            for piece in range(pieces // 2):
                v_piece(piece)
        issue(6 + at)
    for piece in range(pieces // 2, pieces):
        forward_down(piece)
        v_piece(piece)
    sent.extend(pv_copies)
    def add_pair(pair, first, last):
        for j in range(2):
            arrived(wqk.at[block_of(2 * pair + j)], qk_r.at[2 * pair + j])
        both_rows = pl.ds(pl.multiple_of(2 * depth * pair, 2 * depth), 2 * depth)

        @pl.loop(0, pieces)
        def _(i):
            at = pl.ds(pl.multiple_of(i * span, span), span)
            product = dot32(down_g[at, both_rows], wqk[both_rows, :])
            if not first:
                product += mqk[at, :]
            if last:
                mixed_qk[at, :] = product.astype(bf)
            else:
                mqk[at, :] = product

    pair_masks = [0] + list(range(half - 1, 1, -1)) + [1]
    pairs = [toggle(lax.div(me_s, 2), mask) for mask in pair_masks]
    for n, pair in enumerate(pairs[: half // 2]):
        add_pair(pair, n == 0, False)

    for mask in range(1, seq, 2):
        gather[mask].wait_recv()
    sent.extend(gather.values())
    pending = []
    for k in range(seq - 1):
        part = blocks(toggle(me_s, k + 1), mine_first)
        pending.append(
            remote(part, part, pc_s.at[k], pc_r.at[k], {"tp": flip(me_t, core_bit)})
        )
    for pair in pairs[half // 2 : -1]:
        add_pair(pair, False, False)
    for copy in pending:
        copy.wait_recv()
    sent.extend(pending)

    for copy in ss_copies:
        copy.wait_recv()
    sums = jnp.concatenate([ss_seq[s, 0:1, :] for s in range(seq)], 0)
    inverse = lax.rsqrt(sums / (tp * fcols) + epsilon)
    turned = jnp.transpose(jnp.concatenate([inverse] * (crows // seq), 0))
    for s in range(seq):
        factors[s * crows : (s + 1) * crows, :] = jnp.broadcast_to(
            turned[:, s : s + 1], (crows, HEAD)
        )

    earlier = pooled_all[before_slot(me_s, tp, total), pool_rows - 16 :, :]
    for u in range(2):
        cols = slice(u * fcols // 2, (u + 1) * fcols // 2)
        last = dot32(earlier, down_own[:, cols]).astype(bf).astype(f32)[15:16, :]
        last = jnp.where(me_s > 0, last, 0.0)
        rolled = pltpu.roll(short_cols[pl.ds(0, crows), cols], 1, 0)
        top = lax.broadcasted_iota(jnp.int32, rolled.shape, 0) == 0
        short_cols[pl.ds(0, crows), cols] = jnp.where(top, last, rolled)

    add_pair(pairs[-1], False, True)
    block = 2 * crows

    def project(columns, mixed):
        @pl.loop(0, seq // 2)
        def _(i):
            at = pl.ds(pl.multiple_of(i * block, block), block)
            pooled = pooled_all[pl.ds(i * 2 * tp, 2 * tp)].reshape(block, width)
            product = dot32(pooled, mixed[...])
            for c in range(product.shape[1] // HEAD):
                first = columns + c * HEAD
                part = product[:, c * HEAD : (c + 1) * HEAD] * factors[at, :]
                if first < own:
                    part = part * scale
                qkv[at, first : first + HEAD] = part.astype(bf)

    project(0, mixed_qk)

    for copy in pv_copies:
        copy.wait_recv()
    mixed_v[...] = (mv[...] + pv_in[...].astype(f32)).astype(bf)
    project(2 * own, mixed_v)
    shifted[0:1, :] = jnp.zeros((1, own), f32)

    def heads_copy(index):
        return pltpu.make_async_remote_copy(
            src_ref=heads_out.at[index], dst_ref=coarse_heads.at[:, head_cols(me_s)], send_sem=h_s.at[index],
            recv_sem=h_r.at[me_s], device_id={"seq": index}, device_id_type=pl.DeviceIdType.MESH,
        )

    r = lax.broadcasted_iota(jnp.int32, (block, block), 0)
    causal = lax.broadcasted_iota(jnp.int32, (block, block), 1) <= r
    for i in range(seq // 2):
        extent = (i + 1) * block
        start = i * block
        for h in range(own // HEAD):
            part = slice(h * HEAD, (h + 1) * HEAD)
            kpart = slice(own + h * HEAD, own + (h + 1) * HEAD)
            vpart = slice(2 * own + h * HEAD, 2 * own + (h + 1) * HEAD)
            query = qkv[start:extent, part]
            near = jnp.where(causal, dot_t(query, qkv[start:extent, kpart]), big_negative)
            peak = jnp.max(near, axis=-1, keepdims=True)
            if i:
                far = dot_t(query, qkv[:start, kpart])
                peak = jnp.maximum(peak, jnp.max(far, axis=-1, keepdims=True))
            weights = jnp.exp(near - peak)
            denom = jnp.sum(weights, axis=-1, keepdims=True)
            out = dot32(weights.astype(bf), qkv[start:extent, vpart])
            if i:
                weights = jnp.exp(far - peak)
                denom += jnp.sum(weights, axis=-1, keepdims=True)
                out += dot32(weights.astype(bf), qkv[:start, vpart])
            out = out / denom
            shifted[i * block + 1 : extent + 1, part] = out
        for index in (2 * i, 2 * i + 1):
            heads_out[index] = shifted[index * crows : (index + 1) * crows, :].astype(bf)

            @pl.when(me_s != index)
            def _(index=index):
                heads_copy(index).start()

    coarse_heads[:, head_cols(me_s)] = heads_out[me_s]
    in_wout.wait()
    in_wup.wait()
    for j in range(seq):

        @pl.when(me_s != j)
        def _(j=j):
            arrived(coarse_heads.at[:, pl.ds(j * own, own)], h_r.at[j])

    sides, ways = 4, 2
    side = fcols // sides

    def partial(t, u, store):
        @pl.loop(0, side // tile)
        def _(i):
            cols = pl.ds(pl.multiple_of(u * side + i * tile, tile), tile)
            wcols = pl.ds(pl.multiple_of(t * fcols + u * side + i * tile, tile), tile)
            store(cols, dot32(coarse_heads[...], wout[:, wcols]))

    r1 = {}
    for sub in range(tp - 1, 0, -1):
        bit = sub & -sub
        lows = [low for low in tp_bits if low < bit]
        for u in range(sides):
            ucols = pl.ds(u * side, side)
            for low in lows:
                r1[sub + low, u].wait_recv()

            def put(cols, value, sub=sub, lows=lows):
                for low in lows:
                    value += recv1[sub + low - 1, :, cols].astype(f32)
                send1[sub - 1, :, cols] = value.astype(bf)

            partial(toggle(me_t, sub), u, put)
            at = (sub - 1) * sides + u
            r1[sub, u] = remote(
                send1.at[sub - 1, :, ucols], recv1.at[sub - 1, :, ucols], r1_s.at[at], r1_r.at[at],
                {"tp": flip(me_t, bit)},
            )
    sent.extend(r1.values())

    def keep(cols, value):
        short_cols[:, cols] += value

    for u in range(sides):
        partial(me_t, u, keep)
    tp_order = sorted(range(1, tp), key=lambda d: abs(2 * d - tp))
    r2 = []
    for u in range(sides):
        ucols = slice(u * side, (u + 1) * side)
        for bit in tp_bits:
            r1[bit, u].wait_recv()
        whole = short_cols[:, ucols]
        for bit in tp_bits:
            whole += recv1[bit - 1, :, ucols].astype(f32)
        top = lax.broadcasted_iota(jnp.int32, whole.shape, 0) == 0
        state[:, ucols] = jnp.where(top & (me_s == 0), 0.0, whole).astype(bf)
        for w in range(ways):
            wcols = slice(w * width // ways, (w + 1) * width // ways)
            product = dot32(state[:, ucols], wup[ucols, wcols])
            if u:
                product += lift[:, wcols]
            lift[:, wcols] = product
            if u == sides - 1:
                for d in tp_order:
                    dest = around(me_t, d, tp)
                    some = pl.ds(pl.multiple_of(dest * pool_rows, pool_rows), pool_rows)
                    at = (d - 1) * ways + w
                    send2[at] = lift[some, wcols].astype(bf)
                    r2.append(
                        remote(
                            send2.at[at], recv2.at[at], r2_s.at[at], r2_r.at[at], {"tp": dest}
                        )
                    )
    sent.extend(r2)
    for w in range(ways):
        wcols = slice(w * width // ways, (w + 1) * width // ways)
        for copy in r2[w * (tp - 1) : (w + 1) * (tp - 1)]:
            copy.wait_recv()
        lifted = lift[pl.ds(pl.multiple_of(me_t * pool_rows, pool_rows), pool_rows), wcols]
        for d in range(1, tp):
            lifted += recv2[(d - 1) * ways + w].astype(f32)
        spread = jnp.broadcast_to(lifted[:, None, :], (pool_rows, SHORT, width // ways))
        spread = spread.reshape(rows, width // ways)
        result[:, wcols] = (fine_state[:, wcols].astype(f32) + spread).astype(bf)
    for index in range(seq):

        @pl.when(me_s != index)
        def _(index=index):
            heads_copy(index).wait_send()

    for copy in sent:
        copy.wait_send()


def before_slot(me_s, tp, total):
    return lax.rem(me_s * tp + total - 1, total)


def head_body(
    tokens,
    fine_gain,
    fine_query,
    fine_keyval,
    fine_out,
    down_weight,
    coarse_gain,
    coarse_query,
    coarse_keyval,
    coarse_out,
    up_weight,
):
    seq, tp = lax.axis_size("seq"), lax.axis_size("tp")
    rows, width = tokens.shape
    depth, local_cols = coarse_query.shape
    own = local_cols // seq
    half = seq // 2
    pool_rows = rows // SHORT
    crows = pool_rows * tp
    count = crows * seq
    bf, f32 = jnp.bfloat16, jnp.float32
    V = pltpu.VMEM
    dma = lambda n: pltpu.SemaphoreType.DMA((n,))
    one = pltpu.SemaphoreType.DMA
    anywhere = pl.BlockSpec(memory_space=pl.ANY)
    vmem = pl.BlockSpec(memory_space=pltpu.VMEM)
    return pl.pallas_call(
        functools.partial(section_kernel, seq, tp),
        out_shape=jax.ShapeDtypeStruct((rows, width), bf),
        in_specs=[anywhere] * 11,
        out_specs=vmem,
        scratch_shapes=[
            V((1, width), f32), V((1, tp * local_cols), f32),
            V(coarse_keyval.shape, bf), V((2, depth, local_cols), bf),
            V((2 * rows, width), bf), V(fine_query.shape, bf), V(fine_keyval.shape, bf),
            V(fine_out.shape, bf), V(down_weight.shape, bf), V((width, seq * depth), bf),
            V((seq * depth, 2 * own), bf), V((half * depth, 2 * own), bf),
            V(coarse_out.shape, bf), V(up_weight.shape, bf),
            V((2 * rows, width), bf), V((rows, width), bf), V((2 * rows, 2 * width), bf),
            V((rows, width), bf), V((rows, width), bf), V((seq * tp, pool_rows, width), bf),
            V((width, 2 * own), f32), V((width, own), f32), V((width, own), bf),
            V((width, own), bf), V((width, 2 * own), bf), V((width, own), bf),
            V((count, 3 * own), bf), V((count, HEAD), f32),
            V((count + 8, own), f32), V((seq, crows, own), bf),
            V((crows, local_cols), bf), V((crows, local_cols), f32), V((crows, width), f32),
            V((tp, 8, crows), f32), V((seq, 8, crows), f32),
            V((tp - 1, crows, local_cols), bf), V((tp - 1, crows, local_cols), bf),
            V((crows, local_cols), bf),
            V((2 * (tp - 1), pool_rows, width // 2), bf), V((2 * (tp - 1), pool_rows, width // 2), bf),
            dma(10), one(()), one(()), dma(2 * (seq - 1)), dma(seq), dma(2 * (half - 1)), dma(half),
            dma(4 * (tp - 1)), dma(4 * (tp - 1)), dma(tp - 1), dma(tp - 1),
            dma(seq - 1), dma(seq - 1), dma(seq - 1), dma(seq - 1),
            dma(tp - 1), dma(tp - 1), dma(seq - 1), dma(seq - 1), dma(4), dma(4),
            dma(seq), dma(seq), dma(4 * (tp - 1)), dma(4 * (tp - 1)), dma(2 * (tp - 1)),
            dma(2 * (tp - 1)),
        ],
        compiler_params=pltpu.CompilerParams(
            collective_id=0, has_side_effects=True, vmem_limit_bytes=54000 * 1024
        ),
    )(*(pltpu.with_memory_space_constraint(x, pltpu.HBM) for x in (
        tokens, fine_gain[None], fine_query, fine_keyval, fine_out, down_weight, coarse_gain[None],
        coarse_query, coarse_keyval, coarse_out, up_weight)))


def chosen(*args):
    seq, tp = lax.axis_size("seq"), lax.axis_size("tp")
    local_heads = args[7].shape[1] // HEAD
    powers = seq & (seq - 1) == 0 and tp & (tp - 1) == 0 and seq > 1 and tp > 1
    square = args[10].shape[0] == args[10].shape[1] == args[7].shape[1]
    paired = seq % tp == 0 and seq > 2 and args[7].shape[0] * (seq // tp) == args[7].shape[1]
    paired = paired and args[0].shape[0] // SHORT * tp == HEAD
    if local_heads % seq == 0 and args[0].shape[0] == WINDOW and powers and square and paired:
        return head_body(*args)
    return body(*args)


def solution(mesh):
    return jax.shard_map(
        chosen,
        mesh=mesh,
        in_specs=(
            P(("seq", "tp"), None),
            P(),
            P(),
            P(),
            P(),
            P(None, "tp"),
            P(),
            P("seq", "tp"),
            P("seq", None, "tp"),
            P("tp", None),
            P("tp", None),
        ),
        out_specs=P(("seq", "tp"), None),
        check_vma=False,
    )
```

```python
import functools
import math

import jax
import jax.numpy as jnp
from jax import lax
from jax.experimental import pallas as pl
from jax.experimental.pallas import tpu as pltpu
from jax.sharding import PartitionSpec as P

HEAD = 128
WINDOW = 256
SHORT = 8


epsilon = 1e-06
big_negative = -1e30


def from_behind(array, axis, by):
    size = lax.axis_size(axis)
    pairs = [(i, i + by) for i in range(size) if 0 <= i + by < size]
    return lax.ppermute(array, axis, pairs)


def normalize(values, scale_gain):
    mean_square = jnp.mean(values * values, axis=-1, keepdims=True)
    return values * lax.rsqrt(mean_square + epsilon) * scale_gain


def online_update(state, query_heads, key_piece, value_piece, query_index):
    running_max, running_sum, accumulate = state
    scale = 1.0 / math.sqrt(HEAD)
    scores = (
        jnp.einsum("qhd,khd->hqk", query_heads, key_piece, preferred_element_type=jnp.float32)
        * scale
    )
    key_index = jnp.arange(key_piece.shape[0], dtype=jnp.int32)
    allowed = key_index[None, :] <= query_index[:, None]
    scores = jnp.where(allowed[None], scores, big_negative)
    new_max = jnp.maximum(running_max, jnp.max(scores, axis=-1))
    terms = jnp.where(allowed[None], jnp.exp(scores - new_max[..., None]), 0.0)
    new_sum = jnp.sum(terms, axis=-1)
    product = jnp.einsum(
        "hqk,khd->hqd", terms.astype(jnp.bfloat16), value_piece, preferred_element_type=jnp.float32
    )
    return (new_max, new_sum, product)


def body(
    tokens,
    fine_gain,
    fine_query,
    fine_keyval,
    fine_out,
    down_weight,
    coarse_gain,
    coarse_query,
    coarse_keyval,
    coarse_out,
    up_weight,
):
    tok_rows = tokens.shape[0]
    width = tokens.shape[1]
    fine_heads = width // HEAD
    scale = 1.0 / math.sqrt(HEAD)
    start_row = lax.axis_index(("seq", "tp")) * tok_rows
    inputs = tokens.astype(jnp.float32)
    normed = normalize(inputs, fine_gain).astype(jnp.bfloat16)
    queries = jnp.dot(normed, fine_query, preferred_element_type=jnp.float32).astype(jnp.bfloat16)
    keyvals = jnp.dot(normed, fine_keyval, preferred_element_type=jnp.float32).astype(jnp.bfloat16)
    earlier = from_behind(keyvals, ("seq", "tp"), 1)
    key_rows = jnp.concatenate([earlier, keyvals], 0)
    span = key_rows.shape[0]
    key_heads = key_rows[:, :width].reshape(span, fine_heads, HEAD)
    value_heads = key_rows[:, width:].reshape(span, fine_heads, HEAD)
    query_heads = queries.reshape(tok_rows, fine_heads, HEAD)
    scores = (
        jnp.einsum("qhd,khd->hqk", query_heads, key_heads, preferred_element_type=jnp.float32)
        * scale
    )
    row_index = jnp.arange(tok_rows, dtype=jnp.int32)[:, None]
    col_index = jnp.arange(span, dtype=jnp.int32)[None, :]
    offset = row_index + WINDOW - col_index
    allowed = (offset >= 0) & (offset < WINDOW) & (start_row - WINDOW + col_index >= 0)
    scores = jnp.where(allowed[None], scores, big_negative)
    peak = jnp.max(scores, axis=-1, keepdims=True)
    terms = jnp.where(allowed[None], jnp.exp(scores - peak), 0.0)
    denom = jnp.sum(terms, axis=-1)
    mixed = jnp.einsum(
        "hqk,khd->qhd", terms.astype(jnp.bfloat16), value_heads, preferred_element_type=jnp.float32
    )
    local = (mixed / jnp.transpose(denom)[..., None]).reshape(tok_rows, width).astype(jnp.bfloat16)
    fine_state = (inputs + jnp.dot(local, fine_out, preferred_element_type=jnp.float32)).astype(
        jnp.bfloat16
    )
    pooled = jnp.mean(
        fine_state.astype(jnp.float32).reshape(tok_rows // SHORT, SHORT, width), axis=1
    ).astype(jnp.bfloat16)
    pooled_all = lax.all_gather(pooled, "tp", axis=0, tiled=True)
    short_cols = jnp.dot(pooled_all, down_weight, preferred_element_type=jnp.float32).astype(
        jnp.bfloat16
    )
    shortened = lax.all_gather(short_cols, "tp", axis=1, tiled=True)
    coarse_normed = normalize(shortened.astype(jnp.float32), coarse_gain).astype(jnp.bfloat16)
    coarse_rows = coarse_normed.shape[0]
    local_cols = coarse_query.shape[1]
    local_heads = local_cols // HEAD
    query_rows = lax.all_gather(coarse_query, "seq", axis=0, tiled=True)
    keyval_rows = lax.all_gather(coarse_keyval, "seq", axis=0, tiled=True)
    count = query_rows.shape[0]
    query_sum = jnp.dot(coarse_normed, query_rows, preferred_element_type=jnp.float32)
    keyval_sum = jnp.dot(
        coarse_normed,
        keyval_rows.reshape(count, 2 * local_cols),
        preferred_element_type=jnp.float32,
    )
    coarse_queries = query_sum.astype(jnp.bfloat16).reshape(coarse_rows, local_heads, HEAD)
    coarse_kv = keyval_sum.astype(jnp.bfloat16).reshape(coarse_rows, 2, local_cols)
    my_first = lax.axis_index("seq") * coarse_rows
    query_index = my_first + jnp.arange(coarse_rows, dtype=jnp.int32)
    initial = (
        jnp.full((local_heads, coarse_rows), big_negative, jnp.float32),
        jnp.zeros((local_heads, coarse_rows), jnp.float32),
        jnp.zeros((local_heads, coarse_rows, HEAD), jnp.float32),
    )
    piece = lax.all_gather(coarse_kv, "seq", axis=0, tiled=True)
    count = piece.shape[0]
    key_piece = piece[:, 0].reshape(count, local_heads, HEAD)
    value_piece = piece[:, 1].reshape(count, local_heads, HEAD)
    final = lax.cond(
        jnp.int32(0) < my_first + coarse_rows,
        lambda: online_update(initial, coarse_queries, key_piece, value_piece, query_index),
        lambda: initial,
    )
    head_out = final[2] / final[1][..., None]
    coarse_heads = (
        jnp.transpose(head_out, (1, 0, 2)).reshape(coarse_rows, local_cols).astype(jnp.bfloat16)
    )
    partials = jnp.dot(coarse_heads, coarse_out, preferred_element_type=jnp.float32)
    attended = lax.psum_scatter(
        partials.astype(jnp.bfloat16), "tp", scatter_dimension=1, tiled=True
    ).astype(jnp.float32)
    coarse_state = (short_cols.astype(jnp.float32) + attended).astype(jnp.bfloat16)
    prior_row = from_behind(coarse_state[coarse_rows - 1 :], "seq", 1)
    delayed = jnp.concatenate([prior_row, coarse_state[: coarse_rows - 1]], 0)
    lifted = lax.psum_scatter(
        jnp.dot(delayed, up_weight, preferred_element_type=jnp.float32).astype(jnp.bfloat16),
        "tp",
        scatter_dimension=0,
        tiled=True,
    ).astype(jnp.float32)
    result = fine_state.astype(jnp.float32) + jnp.repeat(lifted, SHORT, axis=0)
    return result.astype(jnp.bfloat16)


def flip(index, bit):
    return index + bit - 2 * bit * lax.rem(lax.div(index, jnp.int32(bit)), jnp.int32(2))


def bits_of(size):
    out, bit = [], size // 2
    while bit:
        out.append(bit)
        bit //= 2
    return out


def dot32(left, right):
    return jnp.dot(left, right, preferred_element_type=jnp.float32)


def dot_t(left, right):
    return lax.dot_general(
        left, right, (((1,), (1,)), ((), ())), preferred_element_type=jnp.float32
    )


PLAN = (
    (("qk", 4),),
    (("v", 3), ("v", 1), ("v", 2), ("qk", 6), ("qk", 1)),
    (),
    (("down", 1),),
    (("qk", 7),),
    (("down", 2),),
    (("qk", 5), ("down", 3)),
    (("qk", 2), ("qk", 3)),
    (),
)


def section_kernel(
    seq, tp,
    tokens, fine_gain, fine_query, fine_keyval, fine_out, down_weight, coarse_gain, coarse_query,
    coarse_kv, coarse_out, up_weight,
    result,
    fgain, cgains, kv_raw, kv, both, wq, wkv, wo, down_own, down_g, wqk, wv, wout, wup,
    normed, queries, key_rows, local, fine_state, pooled_all, mqk, mv, pv_out, pv_in, mixed_qk,
    mixed_v, qkv, factors, shifted, heads_out, coarse_heads, short_cols, lift,
    ss_tp, ss_seq, send1, recv1, state, send2, recv2,
    load_sem, halo_s, halo_r, qk_s, qk_r, v_s, v_r, d_s, d_r, pa_s, pa_r, pb_s, pb_r, pc_s, pc_r,
    ssa_s, ssa_r, ssb_s, ssb_r, pv_s, pv_r, h_s, h_r, r1_s, r1_r, r2_s, r2_r,
):
    me_s = lax.axis_index("seq")
    me_t = lax.axis_index("tp")
    rows, width = tokens.shape
    scale = 1.0 / math.sqrt(HEAD)
    total = seq * tp
    lin = me_s * tp + me_t
    after = lax.rem(lin + 1, total)
    before = lax.rem(lin + total - 1, total)
    bf, f32 = jnp.bfloat16, jnp.float32

    def around(index, step, size):
        return lax.rem(index + step, size)

    def toggle(index, mask):
        bit = 1
        while bit <= mask:
            if mask & bit:
                index = flip(index, bit)
            bit *= 2
        return index

    def remote(src, dst, send, recv, device):
        copy = pltpu.make_async_remote_copy(
            src_ref=src, dst_ref=dst, send_sem=send, recv_sem=recv,
            device_id=device, device_id_type=pl.DeviceIdType.MESH,
        )
        copy.start()
        return copy

    def load(src, dst, sem):
        copy = pltpu.make_async_copy(src, dst, sem)
        copy.start()
        return copy

    def arrived(dst, sem):
        pltpu.make_async_copy(dst, dst, sem).wait()

    def linear(index):
        return {"seq": lax.div(index, tp), "tp": lax.rem(index, tp)}

    depth = coarse_query.shape[0]
    own = coarse_query.shape[1] // seq
    fcols = down_own.shape[1]
    half = seq // 2
    zh = lax.div(me_s, half)
    in_half = lax.rem(me_s, half)
    partner = flip(me_s, half)
    pool_rows = rows // SHORT
    crows = pool_rows * tp
    count = crows * seq
    tile = 2 * HEAD

    def head_cols(dest):
        return pl.ds(pl.multiple_of(dest * own, own), own)

    def block_of(source):
        return pl.ds(pl.multiple_of(source * depth, depth), depth)

    barrier = pltpu.get_barrier_semaphore()
    peers = [{"seq": around(me_s, d, seq)} for d in range(1, seq)]
    peers += [{"tp": around(me_t, d, tp)} for d in range(1, tp)]
    peers += [linear(after), linear(before)]
    in_kv = load(coarse_kv, kv_raw, load_sem.at[5])
    in_down = load(down_weight, down_own, load_sem.at[4])
    in_cgain = load(coarse_gain, cgains, load_sem.at[8])
    in_fgain = load(fine_gain, fgain, load_sem.at[9])
    in_tokens = load(tokens, both.at[pl.ds(rows, rows)], load_sem.at[0])
    load(coarse_query.at[:, head_cols(me_s)], wqk.at[block_of(me_s), pl.ds(0, own)], qk_r.at[me_s])
    for peer in peers:
        pl.semaphore_signal(barrier, inc=1, device_id=peer, device_id_type=pl.DeviceIdType.MESH)
    pl.semaphore_wait(barrier, len(peers))
    sent = []
    halo = remote(tokens, both.at[pl.ds(0, rows)], halo_s, halo_r, linear(after))

    def send_qk(offsets):
        for n in offsets:
            dest = toggle(me_s, n)
            for k, source in enumerate((coarse_query, kv.at[0])):
                sent.append(
                    remote(
                        source.at[:, head_cols(dest)], wqk.at[block_of(me_s), pl.ds(k * own, own)],
                        qk_s.at[2 * (n - 1) + k], qk_r.at[me_s], {"seq": dest},
                    )
                )

    def send_v(offsets):
        for d in offsets:
            dest = toggle(me_s, d)
            for k, head in enumerate((flip(dest, half), dest)):
                sent.append(
                    remote(
                        kv.at[1, :, head_cols(head)],
                        wv.at[block_of(in_half), pl.ds(k * own, own)],
                        v_s.at[2 * (d - 1) + k], v_r.at[in_half], {"seq": dest},
                    )
                )

    tp_bits = bits_of(tp)
    pieces = 4
    span = width // pieces
    in_down.wait()
    in_cgain.wait()
    cgain = cgains[:, pl.ds(pl.multiple_of(me_t * fcols, fcols), fcols)]

    def slot_cols(slot):
        return pl.ds(pl.multiple_of(slot * fcols, fcols), fcols)

    def down_piece(slot, bit, number, r):
        part = down_g.at[pl.ds(r * span, span), slot_cols(slot)]
        at = number * pieces + r
        return remote(part, part, d_s.at[at], d_r.at[at], {"tp": flip(me_t, bit)})

    direct = {}

    def launch_down(r):
        at = pl.ds(r * span, span)
        down_g[at, slot_cols(me_t)] = (down_own[at, :].astype(f32) * cgain).astype(bf)
        for bit in tp_bits:
            direct[r, bit] = down_piece(me_t, bit, bit - 1, r)

    def forward_down(r):
        direct[r, tp_bits[0]].wait_recv()
        for bit in tp_bits[1:]:
            if bit != tp_bits[1]:
                for copy in later[r]:
                    copy.wait_recv()
            later.setdefault(r, []).extend(
                down_piece(toggle(me_t, sub), bit, bit + sub - 1, r)
                for sub in range(2 * bit, tp, 2 * bit)
            )
            later[r].append(direct[r, bit])

    later = {}

    def finish_down(r):
        for copy in later[r]:
            copy.wait_recv()
        sent.extend(later[r] + [direct[r, tp_bits[0]]])

    plan = PLAN
    if sum(len(stage) for stage in PLAN) != seq - 1 + half - 1 + pieces - 1:
        plan = [[("qk", d) for d in range(1, seq)] + [("v", d) for d in range(1, half)]]
        plan[0] += [("down", r) for r in range(1, pieces)]

    def issue(stage):
        for kind, d in plan[stage] if stage < len(plan) else ():
            if kind == "qk":
                send_qk([d])
            elif kind == "v":
                send_v([d])
            else:
                launch_down(d)

    launch_down(0)
    in_kv.wait()
    in_wq = load(fine_query, wq, load_sem.at[2])
    in_wkv = load(fine_keyval, wkv, load_sem.at[1])
    in_wo = load(fine_out, wo, load_sem.at[3])
    step = HEAD
    picks = []
    for k in range(2):
        r = lax.broadcasted_iota(jnp.int32, (step, 2 * step), 0)
        c = lax.broadcasted_iota(jnp.int32, (step, 2 * step), 1)
        picks.append((c == 2 * r + k).astype(bf))

    @pl.loop(0, depth // step, unroll=2)
    def _(i):
        at = pl.ds(pl.multiple_of(i * step, step), step)
        turns = kv_raw[at].reshape(2 * step, kv_raw.shape[2])
        for k in range(2):
            kv[k, at, :] = dot32(picks[k], turns).astype(bf)

    load(kv.at[0, :, head_cols(me_s)], wqk.at[block_of(me_s), pl.ds(own, own)], qk_r.at[me_s])
    for k, head in enumerate((partner, me_s)):
        load(kv.at[1, :, head_cols(head)], wv.at[block_of(in_half), pl.ds(k * own, own)],
             v_r.at[in_half])
    in_wout = load(coarse_out, wout, load_sem.at[6])
    in_wup = load(up_weight, wup, load_sem.at[7])
    issue(0)

    in_fgain.wait()
    gain = fgain[...]

    def norm_rows(first):
        values = both[pl.ds(first, rows), :].astype(f32)
        normed[pl.ds(first, rows), :] = normalize(values, gain).astype(bf)

    in_tokens.wait()
    norm_rows(rows)
    in_wq.wait()

    @pl.loop(0, width // tile)
    def _(i):
        cols = pl.ds(pl.multiple_of(i * tile, tile), tile)
        queries[:, cols] = dot32(normed[rows:, :], wq[:, cols]).astype(bf)

    in_wkv.wait()

    def project_rows(first):
        @pl.loop(0, 2 * width // tile)
        def _(i):
            cols = pl.ds(pl.multiple_of(i * tile, tile), tile)
            key_rows[pl.ds(first, rows), cols] = dot32(
                normed[pl.ds(first, rows), :], wkv[:, cols]
            ).astype(bf)

    project_rows(rows)
    issue(1)
    halo.wait_recv()
    sent.append(halo)
    norm_rows(0)
    project_rows(0)
    issue(2)

    own_side = lax.broadcasted_iota(jnp.int32, (rows, rows), 1) <= lax.broadcasted_iota(
        jnp.int32, (rows, rows), 0
    )
    bias = jnp.where(lin > 0, 0.0, big_negative)

    @pl.loop(0, width // HEAD, unroll=4)
    def _(h):
        cols = pl.ds(pl.multiple_of(h * HEAD, HEAD), HEAD)
        vcols = pl.ds(pl.multiple_of(width + h * HEAD, HEAD), HEAD)
        query = queries[:, cols]
        late = dot_t(query, key_rows[rows:, cols])
        early = dot_t(query, key_rows[:rows, cols]) + bias
        scores = jnp.where(own_side, late, early) * scale
        peak = jnp.max(scores, axis=-1, keepdims=True)
        weights = jnp.exp(scores - peak)
        denom = jnp.sum(weights, axis=-1, keepdims=True)
        late = jnp.where(own_side, weights, 0.0).astype(bf)
        early = jnp.where(own_side, 0.0, weights).astype(bf)
        out = dot32(late, key_rows[rows:, vcols]) + dot32(early, key_rows[:rows, vcols])
        local[:, cols] = (out / denom).astype(bf)

    in_wo.wait()

    @pl.loop(0, width // tile)
    def _(i):
        cols = pl.ds(pl.multiple_of(i * tile, tile), tile)
        value = both[rows:, cols].astype(f32) + dot32(local[...], wo[:, cols])
        value = value.astype(bf)
        fine_state[:, cols] = value
        mean = jnp.mean(value.astype(f32).reshape(pool_rows, SHORT, tile), axis=1)
        pooled_all[lin, :, cols] = mean.astype(bf)

    group = []
    for d in range(1, tp):
        slot = pooled_all.at[lin]
        group.append(remote(slot, slot, pa_s.at[d - 1], pa_r.at[d - 1], {"tp": toggle(me_t, d)}))
    issue(3)
    for copy in group:
        copy.wait_recv()
    sent.extend(group)

    core_bit = tp_bits[-1]
    share = tp // 2
    mine_first = lax.rem(me_t, 2) * share

    def blocks(first_s, offset_t):
        return pooled_all.at[pl.ds(first_s * tp + offset_t, share)]

    seq_bits = bits_of(seq)
    gather = {}

    def spread_block(mask):
        for bit in seq_bits:
            if mask == 0 or bit < (mask & -mask):
                part = blocks(toggle(me_s, mask), mine_first)
                at = (mask | bit) - 1
                gather[at + 1] = remote(
                    part, part, pb_s.at[at], pb_r.at[at], {"seq": flip(me_s, bit)}
                )

    spread_block(0)
    issue(4)

    mine = pooled_all[pl.ds(me_s * tp, tp)].reshape(crows, width)
    square_sum = jnp.zeros((8, crows), f32)
    for u in range(2):
        cols = slice(u * fcols // 2, (u + 1) * fcols // 2)
        wide = dot32(mine, down_own[:, cols]).astype(bf).astype(f32)
        short_cols[pl.ds(0, crows), cols] = wide
        square_sum += lax.dot_general(
            jnp.ones((8, fcols // 2), f32), wide * wide, (((1,), (1,)), ((), ())),
            preferred_element_type=f32, precision=lax.Precision.HIGHEST,
        )
    ss_tp[me_t] = square_sum
    group = []
    for d in range(1, tp):
        slot = ss_tp.at[me_t]
        group.append(remote(slot, slot, ssa_s.at[d - 1], ssa_r.at[d - 1], {"tp": toggle(me_t, d)}))
    issue(5)
    ss_copies = []

    def gather_sums():
        for copy in group:
            copy.wait_recv()
        sent.extend(group)
        whole_sum = ss_tp[0]
        for t in range(1, tp):
            whole_sum += ss_tp[t]
        ss_seq[me_s] = whole_sum
        for d in range(1, seq):
            slot = ss_seq.at[me_s]
            ss_copies.append(
                remote(slot, slot, ssb_s.at[d - 1], ssb_r.at[d - 1], {"seq": toggle(me_s, d)})
            )
        sent.extend(ss_copies)

    half_cols = pl.ds(pl.multiple_of(zh * half * depth, half * depth), half * depth)
    pv_copies = []

    def v_piece(piece):
        finish_down(piece)
        at = slice(piece * span, (piece + 1) * span)
        product = dot32(down_g[at, half_cols], wv[...])
        pv_out[at, :] = product[:, :own].astype(bf)
        mv[at, :] = product[:, own:]
        at = pl.ds(piece * span, span)
        pv_copies.append(
            remote(pv_out.at[at], pv_in.at[at], pv_s.at[piece], pv_r.at[piece], {"seq": partner})
        )

    evens = sorted(range(2, seq, 2), key=lambda m: (bin(m).count("1"), m))
    for at, mask in enumerate(evens):
        gather[mask].wait_recv()
        spread_block(mask)
        if at == max(0, len(evens) - 2):
            gather_sums()
        if at == max(0, len(evens) - 2):
            for hs in range(half):
                arrived(wv.at[pl.ds(hs * depth, depth)], v_r.at[hs])
            for piece in range(pieces // 2):
                forward_down(piece)
            for piece in range(pieces // 2):
                v_piece(piece)
        issue(6 + at)
    for piece in range(pieces // 2, pieces):
        forward_down(piece)
        v_piece(piece)
    sent.extend(pv_copies)
    def add_pair(pair, first, last):
        for j in range(2):
            arrived(wqk.at[block_of(2 * pair + j)], qk_r.at[2 * pair + j])
        both_rows = pl.ds(pl.multiple_of(2 * depth * pair, 2 * depth), 2 * depth)

        @pl.loop(0, pieces)
        def _(i):
            at = pl.ds(pl.multiple_of(i * span, span), span)
            product = dot32(down_g[at, both_rows], wqk[both_rows, :])
            if not first:
                product += mqk[at, :]
            if last:
                mixed_qk[at, :] = product.astype(bf)
            else:
                mqk[at, :] = product

    pair_masks = [0] + list(range(half - 1, 1, -1)) + [1]
    pairs = [toggle(lax.div(me_s, 2), mask) for mask in pair_masks]
    for n, pair in enumerate(pairs[: half // 2]):
        add_pair(pair, n == 0, False)

    for mask in range(1, seq, 2):
        gather[mask].wait_recv()
    sent.extend(gather.values())
    pending = []
    for k in range(seq - 1):
        part = blocks(toggle(me_s, k + 1), mine_first)
        pending.append(
            remote(part, part, pc_s.at[k], pc_r.at[k], {"tp": flip(me_t, core_bit)})
        )
    for pair in pairs[half // 2 : -1]:
        add_pair(pair, False, False)
    for copy in pending:
        copy.wait_recv()
    sent.extend(pending)

    for copy in ss_copies:
        copy.wait_recv()
    sums = jnp.concatenate([ss_seq[s, 0:1, :] for s in range(seq)], 0)
    inverse = lax.rsqrt(sums / (tp * fcols) + epsilon)
    turned = jnp.transpose(jnp.concatenate([inverse] * (crows // seq), 0))
    for s in range(seq):
        factors[s * crows : (s + 1) * crows, :] = jnp.broadcast_to(
            turned[:, s : s + 1], (crows, HEAD)
        )

    earlier = pooled_all[before_slot(me_s, tp, total), pool_rows - 16 :, :]
    for u in range(2):
        cols = slice(u * fcols // 2, (u + 1) * fcols // 2)
        last = dot32(earlier, down_own[:, cols]).astype(bf).astype(f32)[15:16, :]
        last = jnp.where(me_s > 0, last, 0.0)
        rolled = pltpu.roll(short_cols[pl.ds(0, crows), cols], 1, 0)
        top = lax.broadcasted_iota(jnp.int32, rolled.shape, 0) == 0
        short_cols[pl.ds(0, crows), cols] = jnp.where(top, last, rolled)

    add_pair(pairs[-1], False, True)
    block = 2 * crows

    def project(columns, mixed):
        @pl.loop(0, seq // 2)
        def _(i):
            at = pl.ds(pl.multiple_of(i * block, block), block)
            pooled = pooled_all[pl.ds(i * 2 * tp, 2 * tp)].reshape(block, width)
            product = dot32(pooled, mixed[...])
            for c in range(product.shape[1] // HEAD):
                first = columns + c * HEAD
                part = product[:, c * HEAD : (c + 1) * HEAD] * factors[at, :]
                if first < own:
                    part = part * scale
                qkv[at, first : first + HEAD] = part.astype(bf)

    project(0, mixed_qk)

    for copy in pv_copies:
        copy.wait_recv()
    mixed_v[...] = (mv[...] + pv_in[...].astype(f32)).astype(bf)
    project(2 * own, mixed_v)
    shifted[0:1, :] = jnp.zeros((1, own), f32)

    def heads_copy(index):
        return pltpu.make_async_remote_copy(
            src_ref=heads_out.at[index], dst_ref=coarse_heads.at[:, head_cols(me_s)], send_sem=h_s.at[index],
            recv_sem=h_r.at[me_s], device_id={"seq": index}, device_id_type=pl.DeviceIdType.MESH,
        )

    r = lax.broadcasted_iota(jnp.int32, (block, block), 0)
    causal = lax.broadcasted_iota(jnp.int32, (block, block), 1) <= r
    for i in range(seq // 2):
        extent = (i + 1) * block
        start = i * block
        for h in range(own // HEAD):
            part = slice(h * HEAD, (h + 1) * HEAD)
            kpart = slice(own + h * HEAD, own + (h + 1) * HEAD)
            vpart = slice(2 * own + h * HEAD, 2 * own + (h + 1) * HEAD)
            query = qkv[start:extent, part]
            near = jnp.where(causal, dot_t(query, qkv[start:extent, kpart]), big_negative)
            peak = jnp.max(near, axis=-1, keepdims=True)
            if i:
                far = dot_t(query, qkv[:start, kpart])
                peak = jnp.maximum(peak, jnp.max(far, axis=-1, keepdims=True))
            weights = jnp.exp(near - peak)
            denom = jnp.sum(weights, axis=-1, keepdims=True)
            out = dot32(weights.astype(bf), qkv[start:extent, vpart])
            if i:
                weights = jnp.exp(far - peak)
                denom += jnp.sum(weights, axis=-1, keepdims=True)
                out += dot32(weights.astype(bf), qkv[:start, vpart])
            out = out / denom
            shifted[i * block + 1 : extent + 1, part] = out
        for index in (2 * i, 2 * i + 1):
            heads_out[index] = shifted[index * crows : (index + 1) * crows, :].astype(bf)

            @pl.when(me_s != index)
            def _(index=index):
                heads_copy(index).start()

    coarse_heads[:, head_cols(me_s)] = heads_out[me_s]
    in_wout.wait()
    in_wup.wait()
    for j in range(seq):

        @pl.when(me_s != j)
        def _(j=j):
            arrived(coarse_heads.at[:, pl.ds(j * own, own)], h_r.at[j])

    sides, ways = 4, 2
    side = fcols // sides

    def partial(t, u, store):
        @pl.loop(0, side // tile)
        def _(i):
            cols = pl.ds(pl.multiple_of(u * side + i * tile, tile), tile)
            wcols = pl.ds(pl.multiple_of(t * fcols + u * side + i * tile, tile), tile)
            store(cols, dot32(coarse_heads[...], wout[:, wcols]))

    r1 = {}
    for sub in range(tp - 1, 0, -1):
        bit = sub & -sub
        lows = [low for low in tp_bits if low < bit]
        for u in range(sides):
            ucols = pl.ds(u * side, side)
            for low in lows:
                r1[sub + low, u].wait_recv()

            def put(cols, value, sub=sub, lows=lows):
                for low in lows:
                    value += recv1[sub + low - 1, :, cols].astype(f32)
                send1[sub - 1, :, cols] = value.astype(bf)

            partial(toggle(me_t, sub), u, put)
            at = (sub - 1) * sides + u
            r1[sub, u] = remote(
                send1.at[sub - 1, :, ucols], recv1.at[sub - 1, :, ucols], r1_s.at[at], r1_r.at[at],
                {"tp": flip(me_t, bit)},
            )
    sent.extend(r1.values())

    def keep(cols, value):
        short_cols[:, cols] += value

    for u in range(sides):
        partial(me_t, u, keep)
    tp_order = sorted(range(1, tp), key=lambda d: abs(2 * d - tp))
    r2 = []
    for u in range(sides):
        ucols = slice(u * side, (u + 1) * side)
        for bit in tp_bits:
            r1[bit, u].wait_recv()
        whole = short_cols[:, ucols]
        for bit in tp_bits:
            whole += recv1[bit - 1, :, ucols].astype(f32)
        top = lax.broadcasted_iota(jnp.int32, whole.shape, 0) == 0
        state[:, ucols] = jnp.where(top & (me_s == 0), 0.0, whole).astype(bf)
        for w in range(ways):
            wcols = slice(w * width // ways, (w + 1) * width // ways)
            product = dot32(state[:, ucols], wup[ucols, wcols])
            if u:
                product += lift[:, wcols]
            lift[:, wcols] = product
            if u == sides - 1:
                for d in tp_order:
                    dest = around(me_t, d, tp)
                    some = pl.ds(pl.multiple_of(dest * pool_rows, pool_rows), pool_rows)
                    at = (d - 1) * ways + w
                    send2[at] = lift[some, wcols].astype(bf)
                    r2.append(
                        remote(
                            send2.at[at], recv2.at[at], r2_s.at[at], r2_r.at[at], {"tp": dest}
                        )
                    )
    sent.extend(r2)
    for w in range(ways):
        wcols = slice(w * width // ways, (w + 1) * width // ways)
        for copy in r2[w * (tp - 1) : (w + 1) * (tp - 1)]:
            copy.wait_recv()
        lifted = lift[pl.ds(pl.multiple_of(me_t * pool_rows, pool_rows), pool_rows), wcols]
        for d in range(1, tp):
            lifted += recv2[(d - 1) * ways + w].astype(f32)
        spread = jnp.broadcast_to(lifted[:, None, :], (pool_rows, SHORT, width // ways))
        spread = spread.reshape(rows, width // ways)
        result[:, wcols] = (fine_state[:, wcols].astype(f32) + spread).astype(bf)
    for index in range(seq):

        @pl.when(me_s != index)
        def _(index=index):
            heads_copy(index).wait_send()

    for copy in sent:
        copy.wait_send()


def before_slot(me_s, tp, total):
    return lax.rem(me_s * tp + total - 1, total)


def head_body(
    tokens,
    fine_gain,
    fine_query,
    fine_keyval,
    fine_out,
    down_weight,
    coarse_gain,
    coarse_query,
    coarse_keyval,
    coarse_out,
    up_weight,
):
    seq, tp = lax.axis_size("seq"), lax.axis_size("tp")
    rows, width = tokens.shape
    depth, local_cols = coarse_query.shape
    own = local_cols // seq
    half = seq // 2
    pool_rows = rows // SHORT
    crows = pool_rows * tp
    count = crows * seq
    bf, f32 = jnp.bfloat16, jnp.float32
    V = pltpu.VMEM
    dma = lambda n: pltpu.SemaphoreType.DMA((n,))
    one = pltpu.SemaphoreType.DMA
    anywhere = pl.BlockSpec(memory_space=pl.ANY)
    vmem = pl.BlockSpec(memory_space=pltpu.VMEM)
    return pl.pallas_call(
        functools.partial(section_kernel, seq, tp),
        out_shape=jax.ShapeDtypeStruct((rows, width), bf),
        in_specs=[anywhere] * 11,
        out_specs=vmem,
        scratch_shapes=[
            V((1, width), f32), V((1, tp * local_cols), f32),
            V(coarse_keyval.shape, bf), V((2, depth, local_cols), bf),
            V((2 * rows, width), bf), V(fine_query.shape, bf), V(fine_keyval.shape, bf),
            V(fine_out.shape, bf), V(down_weight.shape, bf), V((width, seq * depth), bf),
            V((seq * depth, 2 * own), bf), V((half * depth, 2 * own), bf),
            V(coarse_out.shape, bf), V(up_weight.shape, bf),
            V((2 * rows, width), bf), V((rows, width), bf), V((2 * rows, 2 * width), bf),
            V((rows, width), bf), V((rows, width), bf), V((seq * tp, pool_rows, width), bf),
            V((width, 2 * own), f32), V((width, own), f32), V((width, own), bf),
            V((width, own), bf), V((width, 2 * own), bf), V((width, own), bf),
            V((count, 3 * own), bf), V((count, HEAD), f32),
            V((count + 8, own), f32), V((seq, crows, own), bf),
            V((crows, local_cols), bf), V((crows, local_cols), f32), V((crows, width), f32),
            V((tp, 8, crows), f32), V((seq, 8, crows), f32),
            V((tp - 1, crows, local_cols), bf), V((tp - 1, crows, local_cols), bf),
            V((crows, local_cols), bf),
            V((2 * (tp - 1), pool_rows, width // 2), bf), V((2 * (tp - 1), pool_rows, width // 2), bf),
            dma(10), one(()), one(()), dma(2 * (seq - 1)), dma(seq), dma(2 * (half - 1)), dma(half),
            dma(4 * (tp - 1)), dma(4 * (tp - 1)), dma(tp - 1), dma(tp - 1),
            dma(seq - 1), dma(seq - 1), dma(seq - 1), dma(seq - 1),
            dma(tp - 1), dma(tp - 1), dma(seq - 1), dma(seq - 1), dma(4), dma(4),
            dma(seq), dma(seq), dma(4 * (tp - 1)), dma(4 * (tp - 1)), dma(2 * (tp - 1)),
            dma(2 * (tp - 1)),
        ],
        compiler_params=pltpu.CompilerParams(
            collective_id=0, has_side_effects=True, vmem_limit_bytes=54000 * 1024
        ),
    )(*(pltpu.with_memory_space_constraint(x, pltpu.HBM) for x in (
        tokens, fine_gain[None], fine_query, fine_keyval, fine_out, down_weight, coarse_gain[None],
        coarse_query, coarse_keyval, coarse_out, up_weight)))


def chosen(*args):
    seq, tp = lax.axis_size("seq"), lax.axis_size("tp")
    local_heads = args[7].shape[1] // HEAD
    powers = seq & (seq - 1) == 0 and tp & (tp - 1) == 0 and seq > 1 and tp > 1
    square = args[10].shape[0] == args[10].shape[1] == args[7].shape[1]
    paired = seq % tp == 0 and seq > 2 and args[7].shape[0] * (seq // tp) == args[7].shape[1]
    paired = paired and args[0].shape[0] // SHORT * tp == HEAD
    if local_heads % seq == 0 and args[0].shape[0] == WINDOW and powers and square and paired:
        return head_body(*args)
    return body(*args)


def solution(mesh):
    return jax.shard_map(
        chosen,
        mesh=mesh,
        in_specs=(
            P(("seq", "tp"), None),
            P(),
            P(),
            P(),
            P(),
            P(None, "tp"),
            P(),
            P("seq", "tp"),
            P("seq", None, "tp"),
            P("tp", None),
            P("tp", None),
        ),
        out_specs=P(("seq", "tp"), None),
        check_vma=False,
    )
```

```python
import functools
import math

import jax
import jax.numpy as jnp
from jax import lax
from jax.experimental import pallas as pl
from jax.experimental.pallas import tpu as pltpu
from jax.sharding import PartitionSpec as P

HEAD = 128
WINDOW = 256
SHORT = 8


epsilon = 1e-06
big_negative = -1e30


def from_behind(array, axis, by):
    size = lax.axis_size(axis)
    pairs = [(i, i + by) for i in range(size) if 0 <= i + by < size]
    return lax.ppermute(array, axis, pairs)


def normalize(values, scale_gain):
    mean_square = jnp.mean(values * values, axis=-1, keepdims=True)
    return values * lax.rsqrt(mean_square + epsilon) * scale_gain


def online_update(state, query_heads, key_piece, value_piece, query_index):
    running_max, running_sum, accumulate = state
    scale = 1.0 / math.sqrt(HEAD)
    scores = (
        jnp.einsum("qhd,khd->hqk", query_heads, key_piece, preferred_element_type=jnp.float32)
        * scale
    )
    key_index = jnp.arange(key_piece.shape[0], dtype=jnp.int32)
    allowed = key_index[None, :] <= query_index[:, None]
    scores = jnp.where(allowed[None], scores, big_negative)
    new_max = jnp.maximum(running_max, jnp.max(scores, axis=-1))
    terms = jnp.where(allowed[None], jnp.exp(scores - new_max[..., None]), 0.0)
    new_sum = jnp.sum(terms, axis=-1)
    product = jnp.einsum(
        "hqk,khd->hqd", terms.astype(jnp.bfloat16), value_piece, preferred_element_type=jnp.float32
    )
    return (new_max, new_sum, product)


def body(
    tokens,
    fine_gain,
    fine_query,
    fine_keyval,
    fine_out,
    down_weight,
    coarse_gain,
    coarse_query,
    coarse_keyval,
    coarse_out,
    up_weight,
):
    tok_rows = tokens.shape[0]
    width = tokens.shape[1]
    fine_heads = width // HEAD
    scale = 1.0 / math.sqrt(HEAD)
    start_row = lax.axis_index(("seq", "tp")) * tok_rows
    inputs = tokens.astype(jnp.float32)
    normed = normalize(inputs, fine_gain).astype(jnp.bfloat16)
    queries = jnp.dot(normed, fine_query, preferred_element_type=jnp.float32).astype(jnp.bfloat16)
    keyvals = jnp.dot(normed, fine_keyval, preferred_element_type=jnp.float32).astype(jnp.bfloat16)
    earlier = from_behind(keyvals, ("seq", "tp"), 1)
    key_rows = jnp.concatenate([earlier, keyvals], 0)
    span = key_rows.shape[0]
    key_heads = key_rows[:, :width].reshape(span, fine_heads, HEAD)
    value_heads = key_rows[:, width:].reshape(span, fine_heads, HEAD)
    query_heads = queries.reshape(tok_rows, fine_heads, HEAD)
    scores = (
        jnp.einsum("qhd,khd->hqk", query_heads, key_heads, preferred_element_type=jnp.float32)
        * scale
    )
    row_index = jnp.arange(tok_rows, dtype=jnp.int32)[:, None]
    col_index = jnp.arange(span, dtype=jnp.int32)[None, :]
    offset = row_index + WINDOW - col_index
    allowed = (offset >= 0) & (offset < WINDOW) & (start_row - WINDOW + col_index >= 0)
    scores = jnp.where(allowed[None], scores, big_negative)
    peak = jnp.max(scores, axis=-1, keepdims=True)
    terms = jnp.where(allowed[None], jnp.exp(scores - peak), 0.0)
    denom = jnp.sum(terms, axis=-1)
    mixed = jnp.einsum(
        "hqk,khd->qhd", terms.astype(jnp.bfloat16), value_heads, preferred_element_type=jnp.float32
    )
    local = (mixed / jnp.transpose(denom)[..., None]).reshape(tok_rows, width).astype(jnp.bfloat16)
    fine_state = (inputs + jnp.dot(local, fine_out, preferred_element_type=jnp.float32)).astype(
        jnp.bfloat16
    )
    pooled = jnp.mean(
        fine_state.astype(jnp.float32).reshape(tok_rows // SHORT, SHORT, width), axis=1
    ).astype(jnp.bfloat16)
    pooled_all = lax.all_gather(pooled, "tp", axis=0, tiled=True)
    short_cols = jnp.dot(pooled_all, down_weight, preferred_element_type=jnp.float32).astype(
        jnp.bfloat16
    )
    shortened = lax.all_gather(short_cols, "tp", axis=1, tiled=True)
    coarse_normed = normalize(shortened.astype(jnp.float32), coarse_gain).astype(jnp.bfloat16)
    coarse_rows = coarse_normed.shape[0]
    local_cols = coarse_query.shape[1]
    local_heads = local_cols // HEAD
    query_rows = lax.all_gather(coarse_query, "seq", axis=0, tiled=True)
    keyval_rows = lax.all_gather(coarse_keyval, "seq", axis=0, tiled=True)
    count = query_rows.shape[0]
    query_sum = jnp.dot(coarse_normed, query_rows, preferred_element_type=jnp.float32)
    keyval_sum = jnp.dot(
        coarse_normed,
        keyval_rows.reshape(count, 2 * local_cols),
        preferred_element_type=jnp.float32,
    )
    coarse_queries = query_sum.astype(jnp.bfloat16).reshape(coarse_rows, local_heads, HEAD)
    coarse_kv = keyval_sum.astype(jnp.bfloat16).reshape(coarse_rows, 2, local_cols)
    my_first = lax.axis_index("seq") * coarse_rows
    query_index = my_first + jnp.arange(coarse_rows, dtype=jnp.int32)
    initial = (
        jnp.full((local_heads, coarse_rows), big_negative, jnp.float32),
        jnp.zeros((local_heads, coarse_rows), jnp.float32),
        jnp.zeros((local_heads, coarse_rows, HEAD), jnp.float32),
    )
    piece = lax.all_gather(coarse_kv, "seq", axis=0, tiled=True)
    count = piece.shape[0]
    key_piece = piece[:, 0].reshape(count, local_heads, HEAD)
    value_piece = piece[:, 1].reshape(count, local_heads, HEAD)
    final = lax.cond(
        jnp.int32(0) < my_first + coarse_rows,
        lambda: online_update(initial, coarse_queries, key_piece, value_piece, query_index),
        lambda: initial,
    )
    head_out = final[2] / final[1][..., None]
    coarse_heads = (
        jnp.transpose(head_out, (1, 0, 2)).reshape(coarse_rows, local_cols).astype(jnp.bfloat16)
    )
    partials = jnp.dot(coarse_heads, coarse_out, preferred_element_type=jnp.float32)
    attended = lax.psum_scatter(
        partials.astype(jnp.bfloat16), "tp", scatter_dimension=1, tiled=True
    ).astype(jnp.float32)
    coarse_state = (short_cols.astype(jnp.float32) + attended).astype(jnp.bfloat16)
    prior_row = from_behind(coarse_state[coarse_rows - 1 :], "seq", 1)
    delayed = jnp.concatenate([prior_row, coarse_state[: coarse_rows - 1]], 0)
    lifted = lax.psum_scatter(
        jnp.dot(delayed, up_weight, preferred_element_type=jnp.float32).astype(jnp.bfloat16),
        "tp",
        scatter_dimension=0,
        tiled=True,
    ).astype(jnp.float32)
    result = fine_state.astype(jnp.float32) + jnp.repeat(lifted, SHORT, axis=0)
    return result.astype(jnp.bfloat16)


def flip(index, bit):
    return index + bit - 2 * bit * lax.rem(lax.div(index, jnp.int32(bit)), jnp.int32(2))


def bits_of(size):
    out, bit = [], size // 2
    while bit:
        out.append(bit)
        bit //= 2
    return out


def dot32(left, right):
    return jnp.dot(left, right, preferred_element_type=jnp.float32)


def dot_t(left, right):
    return lax.dot_general(
        left, right, (((1,), (1,)), ((), ())), preferred_element_type=jnp.float32
    )


PLAN = (
    (("v", 3),),
    (("v", 1), ("v", 2), ("qk", 6), ("qk", 1)),
    (),
    (("down", 1),),
    (("qk", 7),),
    (("down", 2),),
    (("qk", 5), ("down", 3)),
    (("qk", 2), ("qk", 3)),
    (),
)


def section_kernel(
    seq, tp,
    tokens, fine_gain, fine_query, fine_keyval, fine_out, down_weight, coarse_gain, coarse_query,
    coarse_kv, coarse_out, up_weight,
    result,
    fgain, cgains, kv_raw, kv, both, wq, wkv, wo, down_own, down_g, wqk, wv, wout, wup,
    normed, queries, key_rows, local, fine_state, pooled_all, mqk, mv, pv_out, pv_in, mixed_qk,
    mixed_v, qkv, factors, shifted, heads_out, coarse_heads, short_cols, lift,
    ss_tp, ss_seq, send1, recv1, state, send2, recv2,
    load_sem, halo_s, halo_r, qk_s, qk_r, v_s, v_r, d_s, d_r, pa_s, pa_r, pb_s, pb_r, pc_s, pc_r,
    ssa_s, ssa_r, ssb_s, ssb_r, pv_s, pv_r, h_s, h_r, r1_s, r1_r, r2_s, r2_r,
):
    me_s = lax.axis_index("seq")
    me_t = lax.axis_index("tp")
    rows, width = tokens.shape
    scale = 1.0 / math.sqrt(HEAD)
    total = seq * tp
    lin = me_s * tp + me_t
    after = lax.rem(lin + 1, total)
    before = lax.rem(lin + total - 1, total)
    bf, f32 = jnp.bfloat16, jnp.float32

    def around(index, step, size):
        return lax.rem(index + step, size)

    def toggle(index, mask):
        bit = 1
        while bit <= mask:
            if mask & bit:
                index = flip(index, bit)
            bit *= 2
        return index

    def remote(src, dst, send, recv, device):
        copy = pltpu.make_async_remote_copy(
            src_ref=src, dst_ref=dst, send_sem=send, recv_sem=recv,
            device_id=device, device_id_type=pl.DeviceIdType.MESH,
        )
        copy.start()
        return copy

    def load(src, dst, sem):
        copy = pltpu.make_async_copy(src, dst, sem)
        copy.start()
        return copy

    def arrived(dst, sem):
        pltpu.make_async_copy(dst, dst, sem).wait()

    def linear(index):
        return {"seq": lax.div(index, tp), "tp": lax.rem(index, tp)}

    depth = coarse_query.shape[0]
    own = coarse_query.shape[1] // seq
    fcols = down_own.shape[1]
    half = seq // 2
    zh = lax.div(me_s, half)
    in_half = lax.rem(me_s, half)
    partner = flip(me_s, half)
    pool_rows = rows // SHORT
    crows = pool_rows * tp
    count = crows * seq
    tile = 2 * HEAD

    def head_cols(dest):
        return pl.ds(pl.multiple_of(dest * own, own), own)

    def block_of(source):
        return pl.ds(pl.multiple_of(source * depth, depth), depth)

    barrier = pltpu.get_barrier_semaphore()
    peers = [{"seq": around(me_s, d, seq)} for d in range(1, seq)]
    peers += [{"tp": around(me_t, d, tp)} for d in range(1, tp)]
    peers += [linear(after), linear(before)]
    in_kv = load(coarse_kv, kv_raw, load_sem.at[5])
    in_down = load(down_weight, down_own, load_sem.at[4])
    in_cgain = load(coarse_gain, cgains, load_sem.at[8])
    in_fgain = load(fine_gain, fgain, load_sem.at[9])
    in_tokens = load(tokens, both.at[pl.ds(rows, rows)], load_sem.at[0])
    load(coarse_query.at[:, head_cols(me_s)], wqk.at[block_of(me_s), pl.ds(0, own)], qk_r.at[me_s])
    for peer in peers:
        pl.semaphore_signal(barrier, inc=1, device_id=peer, device_id_type=pl.DeviceIdType.MESH)
    pl.semaphore_wait(barrier, len(peers))
    sent = []
    halo = remote(tokens, both.at[pl.ds(0, rows)], halo_s, halo_r, linear(after))

    def send_qk(offsets, parts=(0, 1)):
        for n in offsets:
            dest = toggle(me_s, n)
            for k in parts:
                source = (coarse_query, kv.at[0])[k]
                sent.append(
                    remote(
                        source.at[:, head_cols(dest)], wqk.at[block_of(me_s), pl.ds(k * own, own)],
                        qk_s.at[2 * (n - 1) + k], qk_r.at[me_s], {"seq": dest},
                    )
                )

    def send_v(offsets):
        for d in offsets:
            dest = toggle(me_s, d)
            for k, head in enumerate((flip(dest, half), dest)):
                sent.append(
                    remote(
                        kv.at[1, :, head_cols(head)],
                        wv.at[block_of(in_half), pl.ds(k * own, own)],
                        v_s.at[2 * (d - 1) + k], v_r.at[in_half], {"seq": dest},
                    )
                )

    tp_bits = bits_of(tp)
    pieces = 4
    span = width // pieces
    in_down.wait()
    in_cgain.wait()
    cgain = cgains[:, pl.ds(pl.multiple_of(me_t * fcols, fcols), fcols)]

    def slot_cols(slot):
        return pl.ds(pl.multiple_of(slot * fcols, fcols), fcols)

    def down_piece(slot, bit, number, r):
        part = down_g.at[pl.ds(r * span, span), slot_cols(slot)]
        at = number * pieces + r
        return remote(part, part, d_s.at[at], d_r.at[at], {"tp": flip(me_t, bit)})

    direct = {}

    def launch_down(r):
        at = pl.ds(r * span, span)
        down_g[at, slot_cols(me_t)] = (down_own[at, :].astype(f32) * cgain).astype(bf)
        for bit in tp_bits:
            direct[r, bit] = down_piece(me_t, bit, bit - 1, r)

    def forward_down(r):
        direct[r, tp_bits[0]].wait_recv()
        for bit in tp_bits[1:]:
            if bit != tp_bits[1]:
                for copy in later[r]:
                    copy.wait_recv()
            later.setdefault(r, []).extend(
                down_piece(toggle(me_t, sub), bit, bit + sub - 1, r)
                for sub in range(2 * bit, tp, 2 * bit)
            )
            later[r].append(direct[r, bit])

    later = {}

    def finish_down(r):
        for copy in later[r]:
            copy.wait_recv()
        sent.extend(later[r] + [direct[r, tp_bits[0]]])

    plan = PLAN
    if sum(len(stage) for stage in PLAN) != seq - 2 + half - 1 + pieces - 1:
        plan = [[("qk", d) for d in range(1, seq) if d != half] + [("v", d) for d in range(1, half)]]
        plan[0] += [("down", r) for r in range(1, pieces)]

    def issue(stage):
        for kind, d in plan[stage] if stage < len(plan) else ():
            if kind == "qk":
                send_qk([d])
            elif kind == "v":
                send_v([d])
            else:
                launch_down(d)

    launch_down(0)
    send_qk([half], (0,))
    in_kv.wait()
    in_wq = load(fine_query, wq, load_sem.at[2])
    in_wkv = load(fine_keyval, wkv, load_sem.at[1])
    in_wo = load(fine_out, wo, load_sem.at[3])
    step = HEAD
    picks = []
    for k in range(2):
        r = lax.broadcasted_iota(jnp.int32, (step, 2 * step), 0)
        c = lax.broadcasted_iota(jnp.int32, (step, 2 * step), 1)
        picks.append((c == 2 * r + k).astype(bf))

    @pl.loop(0, depth // step, unroll=2)
    def _(i):
        at = pl.ds(pl.multiple_of(i * step, step), step)
        turns = kv_raw[at].reshape(2 * step, kv_raw.shape[2])
        for k in range(2):
            kv[k, at, :] = dot32(picks[k], turns).astype(bf)

    load(kv.at[0, :, head_cols(me_s)], wqk.at[block_of(me_s), pl.ds(own, own)], qk_r.at[me_s])
    for k, head in enumerate((partner, me_s)):
        load(kv.at[1, :, head_cols(head)], wv.at[block_of(in_half), pl.ds(k * own, own)],
             v_r.at[in_half])
    in_wout = load(coarse_out, wout, load_sem.at[6])
    in_wup = load(up_weight, wup, load_sem.at[7])
    send_qk([half], (1,))
    issue(0)

    in_fgain.wait()
    gain = fgain[...]

    def norm_rows(first):
        values = both[pl.ds(first, rows), :].astype(f32)
        normed[pl.ds(first, rows), :] = normalize(values, gain).astype(bf)

    in_tokens.wait()
    norm_rows(rows)
    in_wq.wait()

    @pl.loop(0, width // tile)
    def _(i):
        cols = pl.ds(pl.multiple_of(i * tile, tile), tile)
        queries[:, cols] = dot32(normed[rows:, :], wq[:, cols]).astype(bf)

    in_wkv.wait()

    def project_rows(first):
        @pl.loop(0, 2 * width // tile)
        def _(i):
            cols = pl.ds(pl.multiple_of(i * tile, tile), tile)
            key_rows[pl.ds(first, rows), cols] = dot32(
                normed[pl.ds(first, rows), :], wkv[:, cols]
            ).astype(bf)

    project_rows(rows)
    issue(1)
    halo.wait_recv()
    sent.append(halo)
    norm_rows(0)
    project_rows(0)
    issue(2)

    own_side = lax.broadcasted_iota(jnp.int32, (rows, rows), 1) <= lax.broadcasted_iota(
        jnp.int32, (rows, rows), 0
    )
    bias = jnp.where(lin > 0, 0.0, big_negative)

    @pl.loop(0, width // HEAD, unroll=4)
    def _(h):
        cols = pl.ds(pl.multiple_of(h * HEAD, HEAD), HEAD)
        vcols = pl.ds(pl.multiple_of(width + h * HEAD, HEAD), HEAD)
        query = queries[:, cols]
        late = dot_t(query, key_rows[rows:, cols])
        early = dot_t(query, key_rows[:rows, cols]) + bias
        scores = jnp.where(own_side, late, early) * scale
        peak = jnp.max(scores, axis=-1, keepdims=True)
        weights = jnp.exp(scores - peak)
        denom = jnp.sum(weights, axis=-1, keepdims=True)
        late = jnp.where(own_side, weights, 0.0).astype(bf)
        early = jnp.where(own_side, 0.0, weights).astype(bf)
        out = dot32(late, key_rows[rows:, vcols]) + dot32(early, key_rows[:rows, vcols])
        local[:, cols] = (out / denom).astype(bf)

    in_wo.wait()

    @pl.loop(0, width // tile)
    def _(i):
        cols = pl.ds(pl.multiple_of(i * tile, tile), tile)
        value = both[rows:, cols].astype(f32) + dot32(local[...], wo[:, cols])
        value = value.astype(bf)
        fine_state[:, cols] = value
        mean = jnp.mean(value.astype(f32).reshape(pool_rows, SHORT, tile), axis=1)
        pooled_all[lin, :, cols] = mean.astype(bf)

    group = []
    for d in range(1, tp):
        slot = pooled_all.at[lin]
        group.append(remote(slot, slot, pa_s.at[d - 1], pa_r.at[d - 1], {"tp": toggle(me_t, d)}))
    issue(3)
    for copy in group:
        copy.wait_recv()
    sent.extend(group)

    core_bit = tp_bits[-1]
    share = tp // 2
    mine_first = lax.rem(me_t, 2) * share

    def blocks(first_s, offset_t):
        return pooled_all.at[pl.ds(first_s * tp + offset_t, share)]

    seq_bits = bits_of(seq)
    gather = {}

    def spread_block(mask):
        for bit in seq_bits:
            if mask == 0 or bit < (mask & -mask):
                part = blocks(toggle(me_s, mask), mine_first)
                at = (mask | bit) - 1
                gather[at + 1] = remote(
                    part, part, pb_s.at[at], pb_r.at[at], {"seq": flip(me_s, bit)}
                )

    spread_block(0)
    issue(4)

    mine = pooled_all[pl.ds(me_s * tp, tp)].reshape(crows, width)
    square_sum = jnp.zeros((8, crows), f32)
    for u in range(2):
        cols = slice(u * fcols // 2, (u + 1) * fcols // 2)
        wide = dot32(mine, down_own[:, cols]).astype(bf).astype(f32)
        short_cols[pl.ds(0, crows), cols] = wide
        square_sum += lax.dot_general(
            jnp.ones((8, fcols // 2), f32), wide * wide, (((1,), (1,)), ((), ())),
            preferred_element_type=f32, precision=lax.Precision.HIGHEST,
        )
    ss_tp[me_t] = square_sum
    group = []
    for d in range(1, tp):
        slot = ss_tp.at[me_t]
        group.append(remote(slot, slot, ssa_s.at[d - 1], ssa_r.at[d - 1], {"tp": toggle(me_t, d)}))
    issue(5)
    ss_copies = []

    def gather_sums():
        for copy in group:
            copy.wait_recv()
        sent.extend(group)
        whole_sum = ss_tp[0]
        for t in range(1, tp):
            whole_sum += ss_tp[t]
        ss_seq[me_s] = whole_sum
        for d in range(1, seq):
            slot = ss_seq.at[me_s]
            ss_copies.append(
                remote(slot, slot, ssb_s.at[d - 1], ssb_r.at[d - 1], {"seq": toggle(me_s, d)})
            )
        sent.extend(ss_copies)

    half_cols = pl.ds(pl.multiple_of(zh * half * depth, half * depth), half * depth)
    pv_copies = []

    def v_piece(piece):
        finish_down(piece)
        at = slice(piece * span, (piece + 1) * span)
        product = dot32(down_g[at, half_cols], wv[...])
        pv_out[at, :] = product[:, :own].astype(bf)
        mv[at, :] = product[:, own:]
        at = pl.ds(piece * span, span)
        pv_copies.append(
            remote(pv_out.at[at], pv_in.at[at], pv_s.at[piece], pv_r.at[piece], {"seq": partner})
        )

    evens = sorted(range(2, seq, 2), key=lambda m: (bin(m).count("1"), m))
    for at, mask in enumerate(evens):
        gather[mask].wait_recv()
        spread_block(mask)
        if at == max(0, len(evens) - 2):
            gather_sums()
        if at == max(0, len(evens) - 2):
            for hs in range(half):
                arrived(wv.at[pl.ds(hs * depth, depth)], v_r.at[hs])
            for piece in range(pieces // 2):
                forward_down(piece)
            for piece in range(pieces // 2):
                v_piece(piece)
        issue(6 + at)
    for piece in range(pieces // 2, pieces):
        forward_down(piece)
        v_piece(piece)
    sent.extend(pv_copies)
    def add_pair(pair, first, last):
        for j in range(2):
            arrived(wqk.at[block_of(2 * pair + j)], qk_r.at[2 * pair + j])
        both_rows = pl.ds(pl.multiple_of(2 * depth * pair, 2 * depth), 2 * depth)

        @pl.loop(0, pieces)
        def _(i):
            at = pl.ds(pl.multiple_of(i * span, span), span)
            product = dot32(down_g[at, both_rows], wqk[both_rows, :])
            if not first:
                product += mqk[at, :]
            if last:
                mixed_qk[at, :] = product.astype(bf)
            else:
                mqk[at, :] = product

    pair_masks = [0] + list(range(half - 1, 1, -1)) + [1]
    pairs = [toggle(lax.div(me_s, 2), mask) for mask in pair_masks]
    for n, pair in enumerate(pairs[: half // 2]):
        add_pair(pair, n == 0, False)

    for mask in range(1, seq, 2):
        gather[mask].wait_recv()
    sent.extend(gather.values())
    pending = []
    for k in range(seq - 1):
        part = blocks(toggle(me_s, k + 1), mine_first)
        pending.append(
            remote(part, part, pc_s.at[k], pc_r.at[k], {"tp": flip(me_t, core_bit)})
        )
    for pair in pairs[half // 2 : -1]:
        add_pair(pair, False, False)
    for copy in pending:
        copy.wait_recv()
    sent.extend(pending)

    for copy in ss_copies:
        copy.wait_recv()
    sums = jnp.concatenate([ss_seq[s, 0:1, :] for s in range(seq)], 0)
    inverse = lax.rsqrt(sums / (tp * fcols) + epsilon)
    turned = jnp.transpose(jnp.concatenate([inverse] * (crows // seq), 0))
    for s in range(seq):
        factors[s * crows : (s + 1) * crows, :] = jnp.broadcast_to(
            turned[:, s : s + 1], (crows, HEAD)
        )

    earlier = pooled_all[before_slot(me_s, tp, total), pool_rows - 16 :, :]
    for u in range(2):
        cols = slice(u * fcols // 2, (u + 1) * fcols // 2)
        last = dot32(earlier, down_own[:, cols]).astype(bf).astype(f32)[15:16, :]
        last = jnp.where(me_s > 0, last, 0.0)
        rolled = pltpu.roll(short_cols[pl.ds(0, crows), cols], 1, 0)
        top = lax.broadcasted_iota(jnp.int32, rolled.shape, 0) == 0
        short_cols[pl.ds(0, crows), cols] = jnp.where(top, last, rolled)

    add_pair(pairs[-1], False, True)
    block = 2 * crows

    def project(columns, mixed):
        @pl.loop(0, seq // 2)
        def _(i):
            at = pl.ds(pl.multiple_of(i * block, block), block)
            pooled = pooled_all[pl.ds(i * 2 * tp, 2 * tp)].reshape(block, width)
            product = dot32(pooled, mixed[...])
            for c in range(product.shape[1] // HEAD):
                first = columns + c * HEAD
                part = product[:, c * HEAD : (c + 1) * HEAD] * factors[at, :]
                if first < own:
                    part = part * scale
                qkv[at, first : first + HEAD] = part.astype(bf)

    project(0, mixed_qk)

    for copy in pv_copies:
        copy.wait_recv()
    mixed_v[...] = (mv[...] + pv_in[...].astype(f32)).astype(bf)
    project(2 * own, mixed_v)
    shifted[0:1, :] = jnp.zeros((1, own), f32)

    def heads_copy(index):
        return pltpu.make_async_remote_copy(
            src_ref=heads_out.at[index], dst_ref=coarse_heads.at[:, head_cols(me_s)], send_sem=h_s.at[index],
            recv_sem=h_r.at[me_s], device_id={"seq": index}, device_id_type=pl.DeviceIdType.MESH,
        )

    r = lax.broadcasted_iota(jnp.int32, (block, block), 0)
    causal = lax.broadcasted_iota(jnp.int32, (block, block), 1) <= r
    for i in range(seq // 2):
        extent = (i + 1) * block
        start = i * block
        for h in range(own // HEAD):
            part = slice(h * HEAD, (h + 1) * HEAD)
            kpart = slice(own + h * HEAD, own + (h + 1) * HEAD)
            vpart = slice(2 * own + h * HEAD, 2 * own + (h + 1) * HEAD)
            query = qkv[start:extent, part]
            near = jnp.where(causal, dot_t(query, qkv[start:extent, kpart]), big_negative)
            peak = jnp.max(near, axis=-1, keepdims=True)
            if i:
                far = dot_t(query, qkv[:start, kpart])
                peak = jnp.maximum(peak, jnp.max(far, axis=-1, keepdims=True))
            weights = jnp.exp(near - peak)
            denom = jnp.sum(weights, axis=-1, keepdims=True)
            out = dot32(weights.astype(bf), qkv[start:extent, vpart])
            if i:
                weights = jnp.exp(far - peak)
                denom += jnp.sum(weights, axis=-1, keepdims=True)
                out += dot32(weights.astype(bf), qkv[:start, vpart])
            out = out / denom
            shifted[i * block + 1 : extent + 1, part] = out
        for index in (2 * i, 2 * i + 1):
            heads_out[index] = shifted[index * crows : (index + 1) * crows, :].astype(bf)

            @pl.when(me_s != index)
            def _(index=index):
                heads_copy(index).start()

    coarse_heads[:, head_cols(me_s)] = heads_out[me_s]
    in_wout.wait()
    in_wup.wait()
    for j in range(seq):

        @pl.when(me_s != j)
        def _(j=j):
            arrived(coarse_heads.at[:, pl.ds(j * own, own)], h_r.at[j])

    sides, ways = 4, 2
    side = fcols // sides

    def partial(t, u, store):
        @pl.loop(0, side // tile)
        def _(i):
            cols = pl.ds(pl.multiple_of(u * side + i * tile, tile), tile)
            wcols = pl.ds(pl.multiple_of(t * fcols + u * side + i * tile, tile), tile)
            store(cols, dot32(coarse_heads[...], wout[:, wcols]))

    r1 = {}
    for sub in range(tp - 1, 0, -1):
        bit = sub & -sub
        lows = [low for low in tp_bits if low < bit]
        for u in range(sides):
            ucols = pl.ds(u * side, side)
            for low in lows:
                r1[sub + low, u].wait_recv()

            def put(cols, value, sub=sub, lows=lows):
                for low in lows:
                    value += recv1[sub + low - 1, :, cols].astype(f32)
                send1[sub - 1, :, cols] = value.astype(bf)

            partial(toggle(me_t, sub), u, put)
            at = (sub - 1) * sides + u
            r1[sub, u] = remote(
                send1.at[sub - 1, :, ucols], recv1.at[sub - 1, :, ucols], r1_s.at[at], r1_r.at[at],
                {"tp": flip(me_t, bit)},
            )
    sent.extend(r1.values())

    def keep(cols, value):
        short_cols[:, cols] += value

    for u in range(sides):
        partial(me_t, u, keep)
    tp_order = sorted(range(1, tp), key=lambda d: abs(2 * d - tp))
    r2 = []
    for u in range(sides):
        ucols = slice(u * side, (u + 1) * side)
        for bit in tp_bits:
            r1[bit, u].wait_recv()
        whole = short_cols[:, ucols]
        for bit in tp_bits:
            whole += recv1[bit - 1, :, ucols].astype(f32)
        top = lax.broadcasted_iota(jnp.int32, whole.shape, 0) == 0
        state[:, ucols] = jnp.where(top & (me_s == 0), 0.0, whole).astype(bf)
        for w in range(ways):
            wcols = slice(w * width // ways, (w + 1) * width // ways)
            product = dot32(state[:, ucols], wup[ucols, wcols])
            if u:
                product += lift[:, wcols]
            lift[:, wcols] = product
            if u == sides - 1:
                for d in tp_order:
                    dest = around(me_t, d, tp)
                    some = pl.ds(pl.multiple_of(dest * pool_rows, pool_rows), pool_rows)
                    at = (d - 1) * ways + w
                    send2[at] = lift[some, wcols].astype(bf)
                    r2.append(
                        remote(
                            send2.at[at], recv2.at[at], r2_s.at[at], r2_r.at[at], {"tp": dest}
                        )
                    )
    sent.extend(r2)
    for w in range(ways):
        wcols = slice(w * width // ways, (w + 1) * width // ways)
        for copy in r2[w * (tp - 1) : (w + 1) * (tp - 1)]:
            copy.wait_recv()
        lifted = lift[pl.ds(pl.multiple_of(me_t * pool_rows, pool_rows), pool_rows), wcols]
        for d in range(1, tp):
            lifted += recv2[(d - 1) * ways + w].astype(f32)
        spread = jnp.broadcast_to(lifted[:, None, :], (pool_rows, SHORT, width // ways))
        spread = spread.reshape(rows, width // ways)
        result[:, wcols] = (fine_state[:, wcols].astype(f32) + spread).astype(bf)
    for index in range(seq):

        @pl.when(me_s != index)
        def _(index=index):
            heads_copy(index).wait_send()

    for copy in sent:
        copy.wait_send()


def before_slot(me_s, tp, total):
    return lax.rem(me_s * tp + total - 1, total)


def head_body(
    tokens,
    fine_gain,
    fine_query,
    fine_keyval,
    fine_out,
    down_weight,
    coarse_gain,
    coarse_query,
    coarse_keyval,
    coarse_out,
    up_weight,
):
    seq, tp = lax.axis_size("seq"), lax.axis_size("tp")
    rows, width = tokens.shape
    depth, local_cols = coarse_query.shape
    own = local_cols // seq
    half = seq // 2
    pool_rows = rows // SHORT
    crows = pool_rows * tp
    count = crows * seq
    bf, f32 = jnp.bfloat16, jnp.float32
    V = pltpu.VMEM
    dma = lambda n: pltpu.SemaphoreType.DMA((n,))
    one = pltpu.SemaphoreType.DMA
    anywhere = pl.BlockSpec(memory_space=pl.ANY)
    vmem = pl.BlockSpec(memory_space=pltpu.VMEM)
    return pl.pallas_call(
        functools.partial(section_kernel, seq, tp),
        out_shape=jax.ShapeDtypeStruct((rows, width), bf),
        in_specs=[anywhere] * 11,
        out_specs=vmem,
        scratch_shapes=[
            V((1, width), f32), V((1, tp * local_cols), f32),
            V(coarse_keyval.shape, bf), V((2, depth, local_cols), bf),
            V((2 * rows, width), bf), V(fine_query.shape, bf), V(fine_keyval.shape, bf),
            V(fine_out.shape, bf), V(down_weight.shape, bf), V((width, seq * depth), bf),
            V((seq * depth, 2 * own), bf), V((half * depth, 2 * own), bf),
            V(coarse_out.shape, bf), V(up_weight.shape, bf),
            V((2 * rows, width), bf), V((rows, width), bf), V((2 * rows, 2 * width), bf),
            V((rows, width), bf), V((rows, width), bf), V((seq * tp, pool_rows, width), bf),
            V((width, 2 * own), f32), V((width, own), f32), V((width, own), bf),
            V((width, own), bf), V((width, 2 * own), bf), V((width, own), bf),
            V((count, 3 * own), bf), V((count, HEAD), f32),
            V((count + 8, own), f32), V((seq, crows, own), bf),
            V((crows, local_cols), bf), V((crows, local_cols), f32), V((crows, width), f32),
            V((tp, 8, crows), f32), V((seq, 8, crows), f32),
            V((tp - 1, crows, local_cols), bf), V((tp - 1, crows, local_cols), bf),
            V((crows, local_cols), bf),
            V((2 * (tp - 1), pool_rows, width // 2), bf), V((2 * (tp - 1), pool_rows, width // 2), bf),
            dma(10), one(()), one(()), dma(2 * (seq - 1)), dma(seq), dma(2 * (half - 1)), dma(half),
            dma(4 * (tp - 1)), dma(4 * (tp - 1)), dma(tp - 1), dma(tp - 1),
            dma(seq - 1), dma(seq - 1), dma(seq - 1), dma(seq - 1),
            dma(tp - 1), dma(tp - 1), dma(seq - 1), dma(seq - 1), dma(4), dma(4),
            dma(seq), dma(seq), dma(4 * (tp - 1)), dma(4 * (tp - 1)), dma(2 * (tp - 1)),
            dma(2 * (tp - 1)),
        ],
        compiler_params=pltpu.CompilerParams(
            collective_id=0, has_side_effects=True, vmem_limit_bytes=54000 * 1024
        ),
    )(*(pltpu.with_memory_space_constraint(x, pltpu.HBM) for x in (
        tokens, fine_gain[None], fine_query, fine_keyval, fine_out, down_weight, coarse_gain[None],
        coarse_query, coarse_keyval, coarse_out, up_weight)))


def chosen(*args):
    seq, tp = lax.axis_size("seq"), lax.axis_size("tp")
    local_heads = args[7].shape[1] // HEAD
    powers = seq & (seq - 1) == 0 and tp & (tp - 1) == 0 and seq > 1 and tp > 1
    square = args[10].shape[0] == args[10].shape[1] == args[7].shape[1]
    paired = seq % tp == 0 and seq > 2 and args[7].shape[0] * (seq // tp) == args[7].shape[1]
    paired = paired and args[0].shape[0] // SHORT * tp == HEAD
    if local_heads % seq == 0 and args[0].shape[0] == WINDOW and powers and square and paired:
        return head_body(*args)
    return body(*args)


def solution(mesh):
    return jax.shard_map(
        chosen,
        mesh=mesh,
        in_specs=(
            P(("seq", "tp"), None),
            P(),
            P(),
            P(),
            P(),
            P(None, "tp"),
            P(),
            P("seq", "tp"),
            P("seq", None, "tp"),
            P("tp", None),
            P("tp", None),
        ),
        out_specs=P(("seq", "tp"), None),
        check_vma=False,
    )
```
